256 devices in a mesh: chan: 64 (over y, x_lo, z), beam: 4 (over x_hi, core).
Axes of the slice: x: 4 (x_hi: 2, x_lo: 2; x = x_hi * 2 + x_lo), y: 4, z: 8, core: 2. Of those that a mesh axis runs over, the one named last changes fastest.
Arguments:
- signals: bfloat16 [16384, 8192], P('chan', 'beam'), may hold values from -6 to 6
- weights: bfloat16 [3, 2, 512, 16384], P(None, None, 'beam', 'chan'), may hold values from -0.046875 to 0.046875
- bin_group: int32 [2048], replicated, may hold values from 0 to 2
Outputs:
- formed: float32 [2048, 2, 512], P('chan', None, 'beam')
The draws below stay inside these ranges and needn't reach their ends.
All inputs are finite; a program needn't handle non-finite values.
Results may differ from the reference program's by a relative error of at most 0.0042.
Values may be sent and summed in bfloat16 or wider, within the bound.
No kernel may reach another device: no remote copies, remote signals or barrier semaphores. Data moves between devices by JAX's collectives and lax.ppermute only.
A program may use at most 64 MiB of HBM per device.

```python
import math
import jax
import jax.numpy as jnp

SAMPLES = 8192
BEAMS = 512
GROUPS = 3
CHANNELS = 16384
BINS = 2048


def place_ends(array, stream_key, smallest, top_value):
    longest = array.shape.index(max(array.shape))
    spots = []
    for shift in (0, 1):
        where = [jax.random.randint(jax.random.fold_in(stream_key, axis), (), 0, length) for axis, length in enumerate(array.shape)]
        where[longest] = (where[longest] + shift) % array.shape[longest]
        spots.append(tuple(where))
    return array.at[spots[0]].set(smallest).at[spots[1]].set(top_value)


def steps_of(rng, extent, shards, smallest, top_value):
    def one(position, blocks):
        heights = jax.random.uniform(jax.random.fold_in(jax.random.fold_in(rng, 6), position), (blocks,), jnp.float32, smallest / len(shards), top_value / len(shards))
        return jnp.repeat(jnp.exp(heights), extent[position] // blocks).reshape((-1,) + (1,) * (len(extent) - position - 1))

    level = one(*shards[0])
    for cut in shards[1:]:
        level = level * one(*cut)
    return level


def gaussian(stream_key, extent, deviation, bound, shards=(), held_as=jnp.bfloat16):
    array = deviation * jax.random.normal(stream_key, extent, jnp.float32)
    if shards:
        array = array * steps_of(stream_key, extent, shards, -0.22, 0.18)
    return jnp.clip(array, -bound, bound).astype(held_as)


def setup_inputs(seed: int = 0) -> dict:
    keys = jax.random.split(jax.random.key(seed), 4)
    return {
        "signals": gaussian(keys[0], (CHANNELS, SAMPLES), 1.0, 6.0, ((0, 64), (1, 4))),
        "weights": gaussian(keys[1], (GROUPS, 2, BEAMS, CHANNELS), CHANNELS ** -0.5, 0.046875, ((2, 4), (3, 64))),
        "bin_group": place_ends(jax.random.randint(keys[2], (BINS,), 0, GROUPS), jax.random.fold_in(keys[2], 1), 0, GROUPS - 1).astype(jnp.int32),
    }


def reference(signals, weights, bin_group):
    frequency = jnp.arange(1, BINS + 1, dtype=jnp.int32)
    sample_index = jnp.arange(SAMPLES, dtype=jnp.int32)
    phases = frequency[:, None] * sample_index[None, :] % SAMPLES
    angles = 2.0 * math.pi / SAMPLES * phases.astype(jnp.float32)
    twiddle = jnp.stack([jnp.cos(angles), -jnp.sin(angles)], 1).astype(jnp.bfloat16)
    summed = jnp.dot(twiddle.reshape(2 * BINS, SAMPLES), signals.T, preferred_element_type=jnp.float32)
    spectrum = (summed * (1.0 / math.sqrt(SAMPLES))).astype(jnp.bfloat16).reshape(BINS, 2, CHANNELS)
    spec_real = spectrum[:, 0]
    spec_imag = spectrum[:, 1]
    formed = jnp.zeros((BINS, 2, BEAMS), jnp.float32)
    for group_id in range(GROUPS):
        w_real = weights[group_id, 0].T
        w_imag = weights[group_id, 1].T
        real_real = jnp.dot(spec_real, w_real, preferred_element_type=jnp.float32)
        imag_imag = jnp.dot(spec_imag, w_imag, preferred_element_type=jnp.float32)
        imag_real = jnp.dot(spec_imag, w_real, preferred_element_type=jnp.float32)
        real_imag = jnp.dot(spec_real, w_imag, preferred_element_type=jnp.float32)
        chosen = (bin_group == group_id).astype(jnp.float32)[:, None, None]
        formed = formed + chosen * jnp.stack([real_real - imag_imag, imag_real + real_imag], 1)
    return formed
```

```python
import math

import jax
import jax.numpy as jnp
from jax import lax
from jax.experimental import pallas as pl
from jax.experimental.pallas import tpu as pltpu
from jax.sharding import PartitionSpec as P

F32 = jnp.float32
BF16 = jnp.bfloat16

STRIDE = 8
LANES = 128


def unit_root(numer, denom):
    angle = 2.0 * math.pi / denom * (numer % denom).astype(F32)
    return jnp.cos(angle), -jnp.sin(angle)


def transform_tables(samples, time_half):
    inner = samples // STRIDE
    lane = jnp.arange(inner // 2, dtype=jnp.int32)
    k = jnp.arange(32, dtype=jnp.int32)
    row = jnp.arange(32, dtype=jnp.int32)
    coarse = jnp.stack(unit_root(k[:, None] * (32 * lane)[None, :], inner))
    fine = jnp.stack(unit_root((row + 1)[:, None] * lane[None, :], inner))
    fine = fine.reshape(2, 4, 8, -1).transpose(1, 0, 2, 3)
    j = jnp.arange(4, dtype=jnp.int32)
    r = jnp.arange(8, dtype=jnp.int32)
    f1 = (32 * k[None, :, None] + 8 * j[:, None, None] + r[None, None, :] + 1).reshape(4, 256, 1)
    s = jnp.arange(LANES, dtype=jnp.int32)[None, None, :]
    numer = f1 * (s % STRIDE + samples // 2 * time_half)
    angle = 2.0 * math.pi / samples * (numer % samples).astype(F32)
    outer = jnp.where(s < STRIDE, jnp.cos(angle), -jnp.sin(angle)) * (1.0 / math.sqrt(samples))
    return coarse, fine, outer


def dft_kernel(ids_ref, own_ref, other_ref, coarse_ref, fine_ref, outer_ref, out_ref, xs_ref, t_ref, f_ref):
    step = pl.program_id(0)

    @pl.when(step == 0)
    def _():
        core = ids_ref[0]
        n_in = lax.broadcasted_iota(jnp.int32, (1024, 1024), 0)
        n_out = lax.broadcasted_iota(jnp.int32, (1024, 1024), 1)
        source = (n_out % LANES) * STRIDE + n_out // LANES
        perm = jnp.where(n_in == source, 1.0, 0.0).astype(BF16)
        rows = jnp.concatenate(
            [own_ref[:, 0:1024], own_ref[:, 1024:2048], other_ref[:, 0:1024], other_ref[:, 1024:2048]], 0
        )
        split = jnp.dot(rows, perm, preferred_element_type=F32).astype(BF16)
        for part in range(4):
            place = core if part < 2 else 1 - core
            lane0 = pl.multiple_of((place * 2 + part % 2) * LANES, LANES)
            for s in range(STRIDE):
                xs_ref[s * 128 : (s + 1) * 128, pl.ds(lane0, LANES)] = split[
                    part * 128 : (part + 1) * 128, s * 128 : (s + 1) * 128
                ]

    quarter = ids_ref[1 + step]
    fr = fine_ref[quarter, 0]
    fi = fine_ref[quarter, 1]

    def make_rows(pair, carry):
        re, im = [], []
        for h in range(2):
            cr = coarse_ref[0, pl.ds(2 * pair + h, 1), :]
            ci = coarse_ref[1, pl.ds(2 * pair + h, 1), :]
            re.append(cr * fr - ci * fi)
            im.append(cr * fi + ci * fr)
        row0 = pl.multiple_of(pair * 16, 16)
        t_ref[pl.ds(row0, 16), :] = jnp.concatenate(re, 0).astype(BF16)
        t_ref[pl.ds(row0 + 256, 16), :] = jnp.concatenate(im, 0).astype(BF16)
        return carry

    lax.fori_loop(0, 16, make_rows, 0)
    f_ref[...] = lax.dot_general(
        t_ref[...], xs_ref[...], (((1,), (1,)), ((), ())), preferred_element_type=F32
    )

    half = math.sqrt(0.5)

    def combine(chunk, carry):
        row0 = pl.multiple_of(chunk * 16, 16)
        gr, gi = [], []
        outer = outer_ref[quarter, pl.ds(row0, 16), :]
        for s in range(STRIDE):
            a = f_ref[pl.ds(row0, 16), s * 128 : (s + 1) * 128]
            b = f_ref[pl.ds(row0 + 256, 16), s * 128 : (s + 1) * 128]
            wr = outer[:, s : s + 1]
            wi = outer[:, STRIDE + s : STRIDE + s + 1]
            gr.append(wr * a - wi * b)
            gi.append(wr * b + wi * a)
        pr = [gr[s] + gr[s + 4] for s in range(4)]
        pi = [gi[s] + gi[s + 4] for s in range(4)]
        mr = [gr[s] - gr[s + 4] for s in range(4)]
        mi = [gi[s] - gi[s + 4] for s in range(4)]
        low_r = (pr[0] + pr[2]) + (pr[1] + pr[3])
        low_i = (pi[0] + pi[2]) + (pi[1] + pi[3])
        er, ei = mr[0] + mi[2], mi[0] - mr[2]
        dr, di = mr[1] + mi[3], mi[1] - mr[3]
        high_r = er + half * (dr + di)
        high_i = ei + half * (di - dr)
        out_ref[0, pl.ds(row0, 16), :] = low_r.astype(BF16)
        out_ref[0, pl.ds(row0 + 256, 16), :] = high_r.astype(BF16)
        out_ref[0, pl.ds(row0 + 512, 16), :] = low_i.astype(BF16)
        out_ref[0, pl.ds(row0 + 768, 16), :] = high_i.astype(BF16)
        return carry

    lax.fori_loop(0, 16, combine, 0)


def dft(ids, own, other, tables, count):
    return pl.pallas_call(
        dft_kernel,
        grid=(count,),
        in_specs=[
            pl.BlockSpec(memory_space=pltpu.SMEM),
            pl.BlockSpec((128, 2048), lambda i: (0, 0)),
            pl.BlockSpec((128, 2048), lambda i: (0, 0)),
            pl.BlockSpec((2, 32, 512), lambda i: (0, 0, 0)),
            pl.BlockSpec((4, 2, 8, 512), lambda i: (0, 0, 0, 0)),
            pl.BlockSpec((4, 256, 128), lambda i: (0, 0, 0)),
        ],
        out_specs=pl.BlockSpec((1, 1024, 128), lambda i: (i, 0, 0)),
        out_shape=jax.ShapeDtypeStruct((count, 1024, 128), BF16),
        scratch_shapes=[
            pltpu.VMEM((1024, 512), BF16),
            pltpu.VMEM((512, 512), BF16),
            pltpu.VMEM((512, 1024), F32),
        ],
        name="dft",
    )(ids, own, other, *tables)


def form_kernel(ids_ref, spec_ref, onehot_ref, w0_ref, w1_ref, out_ref, l_ref):
    me = ids_ref[0]
    for core in range(2):
        spec = spec_ref[core].astype(F32) + spec_ref[2 + core].astype(F32)
        cols = slice(core * 128, core * 128 + 128)
        spec = spec.astype(BF16)
        sr, si = spec[:512], spec[512:]
        for g in range(3):
            m = onehot_ref[:, g : g + 1].astype(BF16)
            mr, mi = sr * m, si * m
            base = g * 512
            c0 = slice(base + cols.start, base + cols.stop)
            c1 = slice(base + 256 + cols.start, base + 256 + cols.stop)
            l_ref[0:512, c0] = mr
            l_ref[0:512, c1] = -mi
            l_ref[512:1024, c0] = mi
            l_ref[512:1024, c1] = mr
    for sib in range(2):
        acc = jnp.zeros((1024, 256), F32)
        for g in range(3):
            for p in range(2):
                w = jnp.concatenate(
                    [w0_ref[g, p], w1_ref[0, g, p]] if sib == 0 else [w1_ref[1, g, p], w1_ref[2, g, p]], 0
                )
                col = (g * 2 + p) * 256
                acc = acc + lax.dot_general(
                    l_ref[:, col : col + 256], w, (((1,), (1,)), ((), ())), preferred_element_type=F32
                )
        for peer in range(2):
            block = me ^ (sib + 2 * peer)
            part = acc[:, peer * 128 : peer * 128 + 128]
            re = part[:512].reshape(64, 8, 128)
            im = part[512:].reshape(64, 8, 128)
            both = jnp.concatenate([re, im], 1).astype(BF16)
            out_ref[:, pl.ds(block, 1)] = both[:, None]


def form(ids, spec, onehot, w_own, w_rest):
    vm = pl.BlockSpec(memory_space=pltpu.VMEM)
    return pl.pallas_call(
        form_kernel,
        in_specs=[pl.BlockSpec(memory_space=pltpu.SMEM), vm, vm, vm, vm],
        out_specs=vm,
        out_shape=jax.ShapeDtypeStruct((64, 4, 16, 128), BF16),
        scratch_shapes=[pltpu.VMEM((1024, 1536), BF16)],
        name="form",
    )(ids, spec, onehot, w_own, w_rest)


def shards(signals, weights, bin_group):
    samples = signals.shape[1] * lax.axis_size("beam")
    me = lax.axis_index("beam")
    core = me % 2
    swap_core = [(0, 1), (1, 0), (2, 3), (3, 2)]
    swap_half = [(0, 2), (2, 0), (1, 3), (3, 1)]
    halves = signals.reshape(2, 128, -1)
    mine = lax.dynamic_index_in_dim(halves, core, 0, keepdims=False)
    theirs = lax.dynamic_index_in_dim(halves, 1 - core, 0, keepdims=False)
    other = lax.ppermute(theirs, "beam", swap_core)

    w_peer = lax.ppermute(weights, "beam", swap_half)
    w_sib = lax.ppermute(weights, "beam", swap_core)
    w_sib_peer = lax.ppermute(w_peer, "beam", swap_core)
    w_rest = jnp.stack([w_peer, w_sib, w_sib_peer])

    tables = transform_tables(samples, me // 2)
    ids = jnp.stack([core, *[jnp.int32(q) for q in range(4)]])
    partial = dft(ids, mine, other, tables, 4)
    spec = lax.all_to_all(partial, "beam", 0, 0, tiled=True)

    mine_bins = lax.dynamic_index_in_dim(bin_group.reshape(64, 4, 8), me, 1, keepdims=False).reshape(512, 1)
    onehot = (mine_bins == jnp.arange(3, dtype=jnp.int32)[None, :]).astype(F32)
    parts = form(me[None], spec, onehot, weights, w_rest).reshape(256, 16, 128)
    got = lax.all_to_all(parts, ("chan", "beam"), 0, 0, tiled=True)
    summed = jnp.sum(got.reshape(64, 4, 2, 8, 128).astype(F32), axis=0)
    return summed.transpose(0, 2, 1, 3).reshape(32, 2, 128)


def solution(mesh):
    in_specs = (P("chan", "beam"), P(None, None, "beam", "chan"), P())
    out_specs = P("chan", None, "beam")
    return jax.shard_map(shards, mesh=mesh, in_specs=in_specs, out_specs=out_specs, check_vma=False)
```

```python
import math

import jax
import jax.numpy as jnp
from jax import lax
from jax.experimental import pallas as pl
from jax.experimental.pallas import tpu as pltpu
from jax.sharding import Mesh, PartitionSpec as P

F32 = jnp.float32
BF16 = jnp.bfloat16
I32 = jnp.int32

STRIDE = 8
SAMPLES = 8192
LIMIT = 24 * 1024 * 1024


def root(numer, denom):
    angle = 2.0 * math.pi / denom * (numer & (denom - 1)).astype(F32)
    return jnp.cos(angle), -jnp.sin(angle)


def iota(shape, dim):
    return lax.broadcasted_iota(I32, shape, dim)


def deinterleave(x, perm):
    out = []
    rows = jnp.concatenate([x[:, :1024], x[:, 1024:]], 0)
    split = jnp.dot(rows, perm, preferred_element_type=F32).astype(BF16)
    for s in range(STRIDE):
        cols = split[:, s * 128 : (s + 1) * 128]
        out.append(jnp.concatenate([cols[:128], cols[128:]], 1))
    return out


def prep_kernel(ids_ref, own_ref, xs_ref, perm_ref, t_ref, outer_ref):
    core, half, low = ids_ref[0], ids_ref[1], ids_ref[2]
    lane = iota((32, 512), 1)
    part = lane // 128
    u = jnp.where(part < 2, 2 * core + part, 2 * (1 - core) + part - 2)
    m = u * 128 + (lane & 127)
    ar, ai = root(iota((32, 128), 0) * iota((32, 128), 1), 32)
    br, bi = root((iota((32, 512), 0) + 1) * m, 1024)
    s = iota((32, 128), 1) & (STRIDE - 1)
    imag = (iota((32, 128), 1) & STRIDE) != 0
    oar, oai = root(iota((32, 128), 0) * s * 32, SAMPLES)
    obr, obi = root((iota((32, 128), 0) + 1) * (s + SAMPLES // 2 * half), SAMPLES)
    scale = 1.0 / math.sqrt(SAMPLES)
    ob1 = jnp.where(imag, obi, obr) * scale
    ob2 = jnp.where(imag, obr, -obi) * scale
    tile = lambda row: jnp.concatenate([row] * 4, 1)
    for tl in range(2):
        for th in range(2):
            slot = {(0, 1): 0, (1, 0): 1, (1, 1): 2, (0, 0): 3}[(tl, th)]
            swap_h = half if th == 0 else 1 - half
            swap_l = low if tl == 0 else 1 - low
            pick = lambda a: jnp.where(swap_h == 1, a[16:], a[:16])
            fr, fi, o1, o2 = pick(br), pick(bi), pick(ob1), pick(ob2)
            for t in range(16):
                k0 = (t // 8) * 16 + t % 8
                sel = lambda a: jnp.where(swap_l == 1, a[k0 + 8 : k0 + 9], a[k0 : k0 + 1])
                cr, ci = tile(sel(ar)), tile(sel(ai))
                row = slot * 512 + t * 16
                t_ref[row : row + 16, :] = (cr * fr - ci * fi).astype(BF16)
                t_ref[row + 256 : row + 272, :] = (cr * fi + ci * fr).astype(BF16)
                outer_ref[slot, t * 16 : t * 16 + 16, :] = sel(oar) * o1 + sel(oai) * o2
    offset = iota((1024, 128), 0) - STRIDE * iota((1024, 128), 1)
    for s in range(STRIDE):
        perm_ref[:, s * 128 : (s + 1) * 128] = jnp.where(offset == s, 1.0, 0.0).astype(BF16)
    for s, rows in enumerate(deinterleave(own_ref[...], perm_ref[...])):
        xs_ref[s * 128 : (s + 1) * 128, :] = rows


def prep(ids, signals):
    full = lambda *shape: pl.BlockSpec(shape, lambda i, ids: (0,) * len(shape))
    return pl.pallas_call(
        prep_kernel,
        grid_spec=pltpu.PrefetchScalarGridSpec(
            num_scalar_prefetch=1,
            grid=(1,),
            in_specs=[pl.BlockSpec((128, 2048), lambda i, ids: (ids[0], 0))],
            out_specs=[full(1024, 256), full(1024, 1024), full(2048, 512), full(4, 256, 128)],
        ),
        out_shape=[
            jax.ShapeDtypeStruct((1024, 256), BF16),
            jax.ShapeDtypeStruct((1024, 1024), BF16),
            jax.ShapeDtypeStruct((2048, 512), BF16),
            jax.ShapeDtypeStruct((4, 256, 128), F32),
        ],
        compiler_params=pltpu.CompilerParams(vmem_limit_bytes=LIMIT),
        name="prep",
    )(ids, signals)


def combine(f_ref, outer_ref, slot, out_ref, index):
    half = math.sqrt(0.5)

    def step(chunk, carry):
        row0 = pl.multiple_of(chunk * 16, 16)
        gr, gi = [], []
        outer = outer_ref[slot, pl.ds(row0, 16), :]
        for s in range(STRIDE):
            a = f_ref[pl.ds(row0, 16), s * 128 : (s + 1) * 128]
            b = f_ref[pl.ds(row0 + 256, 16), s * 128 : (s + 1) * 128]
            wr = outer[:, s : s + 1]
            wi = outer[:, STRIDE + s : STRIDE + s + 1]
            gr.append(wr * a - wi * b)
            gi.append(wr * b + wi * a)
        pr = [gr[s] + gr[s + 4] for s in range(4)]
        pi = [gi[s] + gi[s + 4] for s in range(4)]
        mr = [gr[s] - gr[s + 4] for s in range(4)]
        mi = [gi[s] - gi[s + 4] for s in range(4)]
        er, ei = mr[0] + mi[2], mi[0] - mr[2]
        dr, di = mr[1] + mi[3], mi[1] - mr[3]
        results = (
            (pr[0] + pr[2]) + (pr[1] + pr[3]),
            er + half * (dr + di),
            (pi[0] + pi[2]) + (pi[1] + pi[3]),
            ei + half * (di - dr),
        )
        for place, value in enumerate(results):
            out_ref[index, pl.ds(row0 + 256 * place, 16), :] = value.astype(out_ref.dtype)
        return carry

    lax.fori_loop(0, 16, step, 0, unroll=4)


def first_kernel(other_ref, own_ref, perm_ref, t_ref, outer_ref, out_ref, xs_ref, f_ref):
    xs_ref[:, 0:256] = own_ref[...]
    for s, rows in enumerate(deinterleave(other_ref[...], perm_ref[...])):
        xs_ref[s * 128 : (s + 1) * 128, 256:512] = rows
    f_ref[...] = lax.dot_general(
        t_ref[0:512, :], xs_ref[...], (((1,), (1,)), ((), ())), preferred_element_type=F32
    )
    combine(f_ref, outer_ref, 0, out_ref, 0)


def next_kernel(slots, xs_ref, t_ref, outer_ref, out_ref, f_ref):
    for index, slot in enumerate(slots):
        buf = f_ref.at[index]
        buf[...] = lax.dot_general(
            t_ref[slot * 512 : slot * 512 + 512, :],
            xs_ref[...],
            (((1,), (1,)), ((), ())),
            preferred_element_type=F32,
        )
        combine(buf, outer_ref, slot, out_ref, index)


VM = pl.BlockSpec(memory_space=pltpu.VMEM)


def dft_first(other, own, perm, table, outer):
    return pl.pallas_call(
        first_kernel,
        in_specs=[VM] * 5,
        out_specs=[VM, VM],
        out_shape=[jax.ShapeDtypeStruct((1, 1024, 128), BF16), jax.ShapeDtypeStruct((1024, 512), BF16)],
        scratch_shapes=[pltpu.VMEM((512, 1024), F32)],
        compiler_params=pltpu.CompilerParams(vmem_limit_bytes=LIMIT),
        name="dft_first",
    )(other, own, perm, table, outer)


def dft_next(xs, table, outer, slots, dtype):
    return pl.pallas_call(
        lambda *refs: next_kernel(slots, *refs),
        in_specs=[VM] * 3,
        out_specs=VM,
        out_shape=jax.ShapeDtypeStruct((len(slots), 1024, 128), dtype),
        scratch_shapes=[pltpu.VMEM((len(slots), 512, 1024), F32)],
        compiler_params=pltpu.CompilerParams(vmem_limit_bytes=LIMIT),
        name="dft_next",
    )(xs, table, outer)


def form_kernel(ids_ref, mine_ref, sib_ref, group_ref, w0_ref, w1_ref, w2_ref, w3_ref, out_ref, l_ref, w_ref):
    core, half = ids_ref[0], ids_ref[1]
    for src, place in ((mine_ref, core), (sib_ref, 1 - core)):
        for xl in range(2):
            lane0 = pl.multiple_of(xl * 256 + place * 128, 128)
            sr, si = src[xl, 0:512, :], src[xl, 512:1024, :]
            l_ref[0:512, pl.ds(lane0, 128)] = sr
            l_ref[0:512, pl.ds(lane0 + 512, 128)] = -si
            l_ref[512:1024, pl.ds(lane0, 128)] = si
            l_ref[512:1024, pl.ds(lane0 + 512, 128)] = sr
    for g in range(3):
        for p in range(2):
            for b, xl, ref in ((0, 0, w0_ref), (0, 1, w1_ref), (1, 0, w2_ref), (1, 1, w3_ref)):
                row, col = g * 256 + b * 128, p * 512 + xl * 256
                w_ref[row : row + 128, col : col + 256] = ref[g, p]
    total = jnp.zeros((2, 512, 256), F32)
    groups = group_ref[...]
    for g in range(3):
        acc = lax.dot_general(
            l_ref[...], w_ref[g * 256 : g * 256 + 256, :], (((1,), (1,)), ((), ())), preferred_element_type=F32
        )
        total = jnp.where((groups == g)[None], acc.reshape(2, 512, 256), total)
    for b in range(2):
        part = total[:, :, b * 128 : b * 128 + 128]
        re = part[0].reshape(4, 8, 16, 128)
        im = part[1].reshape(4, 8, 16, 128)
        both = jnp.concatenate([re, im], 2).astype(BF16)
        out_ref[:, :, pl.ds(half if b == 0 else 1 - half, 1)] = both[:, :, None]


def form(ids, mine, sib, group, weights):
    return pl.pallas_call(
        form_kernel,
        in_specs=[pl.BlockSpec(memory_space=pltpu.SMEM)] + [VM] * 7,
        out_specs=VM,
        out_shape=jax.ShapeDtypeStruct((4, 8, 2, 32, 128), BF16),
        scratch_shapes=[pltpu.VMEM((1024, 1024), BF16), pltpu.VMEM((768, 1024), BF16)],
        compiler_params=pltpu.CompilerParams(vmem_limit_bytes=LIMIT),
        name="form",
    )(ids, mine, sib, group, *weights)


def shards(signals, weights, bin_group):
    half, core, low = lax.axis_index("xhi"), lax.axis_index("core"), lax.axis_index("xlo")
    ring = ("xlo", "xhi", "core")

    def exchange(value, flip):
        return lax.ppermute(value, ring, [(i, i ^ flip) for i in range(8)])

    ids = jnp.stack([core, half, low])
    theirs = lax.dynamic_slice_in_dim(signals, (1 - core) * 128, 128, 0)
    other = exchange(theirs, 1)
    own, perm, table, outer = prep(ids, signals)
    peers = [exchange(weights, flip) for flip in (4, 2, 6)]

    spec0, xs = dft_first(other, own, perm, table, outer)
    got0 = exchange(spec0[0], 2)
    spec12 = dft_next(xs, table, outer, (1, 2), BF16)
    got1 = exchange(spec12[0], 4)
    got2 = exchange(spec12[1], 6)
    spec3 = dft_next(xs, table, outer, (3,), F32)
    same = spec3[0] + got0.astype(F32)
    cross = got1.astype(F32) + got2.astype(F32)
    mine = jnp.stack([same, cross]).astype(BF16)
    sib = exchange(mine, 1)

    owned = lax.dynamic_index_in_dim(bin_group.reshape(4, 2, 8, 2, 16), low, 1, keepdims=False)
    owned = lax.dynamic_index_in_dim(owned, half, 2, keepdims=False).reshape(512, 1)
    parts = form(ids, mine, sib, owned, [weights] + peers).reshape(64, 32, 128)
    got = lax.all_to_all(parts, ("y", "z", "xhi"), 0, 0, tiled=True)
    summed = jnp.sum(got.reshape(32, 2, 2, 16, 128).astype(F32), axis=0)
    return summed.transpose(0, 2, 1, 3).reshape(32, 2, 128)


def solution(mesh):
    fine = Mesh(mesh.devices.reshape(4, 2, 8, 2, 2), ("y", "xlo", "z", "xhi", "core"))
    chan, beam = ("y", "xlo", "z"), ("xhi", "core")
    in_specs = (P(chan, beam), P(None, None, beam, chan), P())
    out_specs = P(chan, None, beam)
    return jax.shard_map(shards, mesh=fine, in_specs=in_specs, out_specs=out_specs, check_vma=False)
```

```python
import math

import jax
import jax.numpy as jnp
from jax import lax
from jax.experimental import pallas as pl
from jax.experimental.pallas import tpu as pltpu
from jax.sharding import Mesh, PartitionSpec as P

F32 = jnp.float32
BF16 = jnp.bfloat16
I32 = jnp.int32

STRIDE = 8
SAMPLES = 8192
LIMIT = 24 * 1024 * 1024


def root(numer, denom):
    angle = 2.0 * math.pi / denom * (numer & (denom - 1)).astype(F32)
    return jnp.cos(angle), -jnp.sin(angle)


def iota(shape, dim):
    return lax.broadcasted_iota(I32, shape, dim)


def deinterleave(x, perm):
    out = []
    rows = jnp.concatenate([x[:, :1024], x[:, 1024:]], 0)
    split = jnp.dot(rows, perm, preferred_element_type=F32).astype(BF16)
    for s in range(STRIDE):
        cols = split[:, s * 128 : (s + 1) * 128]
        out.append(jnp.concatenate([cols[:128], cols[128:]], 1))
    return out


def prep_kernel(ids_ref, own_ref, xs_ref, perm_ref, t_ref, outer_ref):
    core, half, low = ids_ref[0], ids_ref[1], ids_ref[2]
    lane = iota((32, 512), 1)
    part = lane // 128
    u = jnp.where(part < 2, 2 * core + part, 2 * (1 - core) + part - 2)
    m = u * 128 + (lane & 127)
    ar, ai = root(iota((32, 128), 0) * iota((32, 128), 1), 32)
    br, bi = root((iota((32, 512), 0) + 1) * m, 1024)
    s = iota((32, 128), 1) & (STRIDE - 1)
    imag = (iota((32, 128), 1) & STRIDE) != 0
    oar, oai = root(iota((32, 128), 0) * s * 32, SAMPLES)
    obr, obi = root((iota((32, 128), 0) + 1) * (s + SAMPLES // 2 * half), SAMPLES)
    scale = 1.0 / math.sqrt(SAMPLES)
    ob1 = jnp.where(imag, obi, obr) * scale
    ob2 = jnp.where(imag, obr, -obi) * scale
    tile = lambda row: jnp.concatenate([row] * 4, 1)
    for tl in range(2):
        for th in range(2):
            slot = {(0, 1): 0, (1, 0): 1, (1, 1): 2, (0, 0): 3}[(tl, th)]
            swap_h = half if th == 0 else 1 - half
            swap_l = low if tl == 0 else 1 - low
            pick = lambda a: jnp.where(swap_h == 1, a[16:], a[:16])
            fr, fi, o1, o2 = pick(br), pick(bi), pick(ob1), pick(ob2)
            for t in range(16):
                k0 = (t // 8) * 16 + t % 8
                sel = lambda a: jnp.where(swap_l == 1, a[k0 + 8 : k0 + 9], a[k0 : k0 + 1])
                cr, ci = tile(sel(ar)), tile(sel(ai))
                row = slot * 512 + t * 16
                t_ref[row : row + 16, :] = (cr * fr - ci * fi).astype(BF16)
                t_ref[row + 256 : row + 272, :] = (cr * fi + ci * fr).astype(BF16)
                outer_ref[slot, t * 16 : t * 16 + 16, :] = sel(oar) * o1 + sel(oai) * o2
    offset = iota((1024, 128), 0) - STRIDE * iota((1024, 128), 1)
    for s in range(STRIDE):
        perm_ref[:, s * 128 : (s + 1) * 128] = jnp.where(offset == s, 1.0, 0.0).astype(BF16)
    for s, rows in enumerate(deinterleave(own_ref[...], perm_ref[...])):
        xs_ref[s * 128 : (s + 1) * 128, :] = rows


def prep(ids, signals):
    full = lambda *shape: pl.BlockSpec(shape, lambda i, ids: (0,) * len(shape))
    return pl.pallas_call(
        prep_kernel,
        grid_spec=pltpu.PrefetchScalarGridSpec(
            num_scalar_prefetch=1,
            grid=(1,),
            in_specs=[pl.BlockSpec((128, 2048), lambda i, ids: (ids[0], 0))],
            out_specs=[full(1024, 256), full(1024, 1024), full(2048, 512), full(4, 256, 128)],
        ),
        out_shape=[
            jax.ShapeDtypeStruct((1024, 256), BF16),
            jax.ShapeDtypeStruct((1024, 1024), BF16),
            jax.ShapeDtypeStruct((2048, 512), BF16),
            jax.ShapeDtypeStruct((4, 256, 128), F32),
        ],
        compiler_params=pltpu.CompilerParams(vmem_limit_bytes=LIMIT),
        name="prep",
    )(ids, signals)


def combine(f_ref, outer_ref, slot, out_ref):
    half = math.sqrt(0.5)

    def step(chunk, carry):
        row0 = pl.multiple_of(chunk * 16, 16)
        gr, gi = [], []
        outer = outer_ref[slot, pl.ds(row0, 16), :]
        for s in range(STRIDE):
            a = f_ref[pl.ds(row0, 16), s * 128 : (s + 1) * 128]
            b = f_ref[pl.ds(row0 + 256, 16), s * 128 : (s + 1) * 128]
            wr = outer[:, s : s + 1]
            wi = outer[:, STRIDE + s : STRIDE + s + 1]
            gr.append(wr * a - wi * b)
            gi.append(wr * b + wi * a)
        pr = [gr[s] + gr[s + 4] for s in range(4)]
        pi = [gi[s] + gi[s + 4] for s in range(4)]
        mr = [gr[s] - gr[s + 4] for s in range(4)]
        mi = [gi[s] - gi[s + 4] for s in range(4)]
        er, ei = mr[0] + mi[2], mi[0] - mr[2]
        dr, di = mr[1] + mi[3], mi[1] - mr[3]
        results = (
            (pr[0] + pr[2]) + (pr[1] + pr[3]),
            er + half * (dr + di),
            (pi[0] + pi[2]) + (pi[1] + pi[3]),
            ei + half * (di - dr),
        )
        for place, value in enumerate(results):
            out_ref[pl.ds(row0 + 256 * place, 16), :] = value.astype(out_ref.dtype)
        return carry

    lax.fori_loop(0, 16, step, 0, unroll=4)


def first_kernel(other_ref, own_ref, perm_ref, t_ref, outer_ref, out_ref, xs_ref, f_ref):
    xs_ref[:, 0:256] = own_ref[...]
    for s, rows in enumerate(deinterleave(other_ref[...], perm_ref[...])):
        xs_ref[s * 128 : (s + 1) * 128, 256:512] = rows
    f_ref[...] = lax.dot_general(
        t_ref[0:512, :], xs_ref[...], (((1,), (1,)), ((), ())), preferred_element_type=F32
    )
    combine(f_ref, outer_ref, 0, out_ref)


def next_kernel(slots, xs_ref, t_ref, outer_ref, *rest):
    outs, f_ref = rest[:-1], rest[-1]
    for index, slot in enumerate(slots):
        buf = f_ref.at[index]
        buf[...] = lax.dot_general(
            t_ref[slot * 512 : slot * 512 + 512, :],
            xs_ref[...],
            (((1,), (1,)), ((), ())),
            preferred_element_type=F32,
        )
        combine(buf, outer_ref, slot, outs[index])


VM = pl.BlockSpec(memory_space=pltpu.VMEM)


def dft_first(other, own, perm, table, outer):
    return pl.pallas_call(
        first_kernel,
        in_specs=[VM] * 5,
        out_specs=[VM, VM],
        out_shape=[jax.ShapeDtypeStruct((1024, 128), BF16), jax.ShapeDtypeStruct((1024, 512), BF16)],
        scratch_shapes=[pltpu.VMEM((512, 1024), F32)],
        compiler_params=pltpu.CompilerParams(vmem_limit_bytes=LIMIT),
        name="dft_first",
    )(other, own, perm, table, outer)


def dft_next(xs, table, outer, slots, dtype):
    return pl.pallas_call(
        lambda *refs: next_kernel(slots, *refs),
        in_specs=[VM] * 3,
        out_specs=[VM] * len(slots),
        out_shape=[jax.ShapeDtypeStruct((1024, 128), dtype)] * len(slots),
        scratch_shapes=[pltpu.VMEM((len(slots), 512, 1024), F32)],
        compiler_params=pltpu.CompilerParams(vmem_limit_bytes=LIMIT),
    )(xs, table, outer)


def form_kernel(ids_ref, s0_ref, s1_ref, p0_ref, p1_ref, group_ref, w0_ref, w1_ref, w2a_ref, w2b_ref, w3_ref, out_ref, l_ref, w_ref):
    core, half = ids_ref[0], ids_ref[1]
    for srcs, place in (((s0_ref, s1_ref), core), ((p0_ref, p1_ref), 1 - core)):
        for xl in range(2):
            lane0 = pl.multiple_of(xl * 256 + place * 128, 128)
            src = srcs[xl]
            sr, si = src[0:512, :], src[512:1024, :]
            l_ref[0:512, pl.ds(lane0, 128)] = sr
            l_ref[0:512, pl.ds(lane0 + 512, 128)] = -si
            l_ref[512:1024, pl.ds(lane0, 128)] = si
            l_ref[512:1024, pl.ds(lane0 + 512, 128)] = sr
    for g in range(3):
        for p in range(2):
            i = g * 2 + p
            w2 = w2a_ref[i] if i < 3 else w2b_ref[i - 3]
            for b, xl, w in ((0, 0, w0_ref[i]), (0, 1, w1_ref[i]), (1, 0, w2), (1, 1, w3_ref[i])):
                row, col = g * 256 + b * 128, p * 512 + xl * 256
                w_ref[row : row + 128, col : col + 256] = w
    total = jnp.zeros((2, 512, 256), F32)
    groups = group_ref[...]
    for g in range(3):
        acc = lax.dot_general(
            l_ref[...], w_ref[g * 256 : g * 256 + 256, :], (((1,), (1,)), ((), ())), preferred_element_type=F32
        )
        total = jnp.where((groups == g)[None], acc.reshape(2, 512, 256), total)
    for b in range(2):
        part = total[:, :, b * 128 : b * 128 + 128]
        re = part[0].reshape(4, 8, 16, 128)
        im = part[1].reshape(4, 8, 16, 128)
        both = jnp.concatenate([re, im], 2).astype(BF16)
        out_ref[:, :, pl.ds(half if b == 0 else 1 - half, 1)] = both[:, :, None]


def form(ids, spec, group, weights):
    return pl.pallas_call(
        form_kernel,
        in_specs=[pl.BlockSpec(memory_space=pltpu.SMEM)] + [VM] * 10,
        out_specs=VM,
        out_shape=jax.ShapeDtypeStruct((4, 8, 2, 32, 128), BF16),
        scratch_shapes=[pltpu.VMEM((1024, 1024), BF16), pltpu.VMEM((768, 1024), BF16)],
        compiler_params=pltpu.CompilerParams(vmem_limit_bytes=LIMIT),
        name="form",
    )(ids, *spec, group, *weights)


def shards(signals, weights, bin_group):
    half, core, low = lax.axis_index("xhi"), lax.axis_index("core"), lax.axis_index("xlo")
    ring = ("xlo", "xhi", "core")

    def exchange(value, flip):
        return lax.ppermute(value, ring, [(i, i ^ flip) for i in range(8)])

    ids = jnp.stack([core, half, low])
    theirs = lax.dynamic_slice_in_dim(signals, (1 - core) * 128, 128, 0)
    other = exchange(theirs, 1)
    blocks = weights.reshape(6, 128, 256)
    w1 = exchange(blocks, 4)
    w3 = exchange(blocks, 6)
    own, perm, table, outer = prep(ids, pltpu.with_memory_space_constraint(signals, pltpu.HBM))

    spec0, xs = dft_first(other, own, perm, table, outer)
    got0 = exchange(spec0, 2)
    spec1, spec2 = dft_next(xs, table, outer, (1, 2), BF16)
    got1 = exchange(spec1, 4)
    got2 = exchange(spec2, 6)
    w2a = exchange(w1[:3], 6)
    w2b = exchange(w3[3:], 4)
    (spec3,) = dft_next(xs, table, outer, (3,), F32)
    same = (spec3 + got0.astype(F32)).astype(BF16)
    same_sib = exchange(same, 1)
    cross = (got1.astype(F32) + got2.astype(F32)).astype(BF16)
    cross_sib = exchange(cross, 1)

    owned = lax.dynamic_index_in_dim(bin_group.reshape(4, 2, 8, 2, 16), low, 1, keepdims=False)
    owned = lax.dynamic_index_in_dim(owned, half, 2, keepdims=False).reshape(512, 1)
    parts = form(ids, (same, cross, same_sib, cross_sib), owned, (blocks, w1, w2a, w2b, w3))
    got = lax.all_to_all(parts.reshape(64, 32, 128), ("y", "z", "xhi"), 0, 0, tiled=True)
    summed = jnp.sum(got.reshape(32, 2, 2, 16, 128).astype(F32), axis=0)
    return summed.transpose(0, 2, 1, 3).reshape(32, 2, 128)


def solution(mesh):
    fine = Mesh(mesh.devices.reshape(4, 2, 8, 2, 2), ("y", "xlo", "z", "xhi", "core"))
    chan, beam = ("y", "xlo", "z"), ("xhi", "core")
    in_specs = (P(chan, beam), P(None, None, beam, chan), P())
    out_specs = P(chan, None, beam)
    return jax.shard_map(shards, mesh=fine, in_specs=in_specs, out_specs=out_specs, check_vma=False)
```

```python
import math

import jax
import jax.numpy as jnp
from jax import lax
from jax.experimental import pallas as pl
from jax.experimental.pallas import tpu as pltpu
from jax.sharding import Mesh, PartitionSpec as P

F32 = jnp.float32
BF16 = jnp.bfloat16
I32 = jnp.int32

STRIDE = 8
SAMPLES = 8192
LIMIT = 24 * 1024 * 1024


def root(numer, denom):
    angle = 2.0 * math.pi / denom * (numer & (denom - 1)).astype(F32)
    return jnp.cos(angle), -jnp.sin(angle)


def iota(shape, dim):
    return lax.broadcasted_iota(I32, shape, dim)


def deinterleave(x, perm):
    out = []
    rows = jnp.concatenate([x[:, :1024], x[:, 1024:]], 0)
    split = jnp.dot(rows, perm, preferred_element_type=F32).astype(BF16)
    for s in range(STRIDE):
        cols = split[:, s * 128 : (s + 1) * 128]
        out.append(jnp.concatenate([cols[:128], cols[128:]], 1))
    return out


def prep_kernel(ids_ref, own_ref, xs_ref, perm_ref, t_ref, outer_ref):
    core, half = ids_ref[0], ids_ref[1]
    lane = iota((32, 512), 1)
    part = lane // 128
    u = jnp.where(part < 2, 2 * core + part, 2 * (1 - core) + part - 2)
    m = u * 128 + (lane & 127)
    ar, ai = root(iota((32, 128), 0) * iota((32, 128), 1), 32)
    br, bi = root((iota((32, 512), 0) + 1) * m, 1024)
    s = iota((32, 128), 1) & (STRIDE - 1)
    imag = (iota((32, 128), 1) & STRIDE) != 0
    oar, oai = root(iota((32, 128), 0) * s * 32, SAMPLES)
    obr, obi = root((iota((32, 128), 0) + 1) * (s + SAMPLES // 2 * half), SAMPLES)
    scale = 1.0 / math.sqrt(SAMPLES)
    ob1 = jnp.where(imag, obi, obr) * scale
    ob2 = jnp.where(imag, obr, -obi) * scale
    tile = lambda row: jnp.concatenate([row] * 4, 1)
    for slot in range(4):
        side = (1 - half) if slot < 2 else half
        pick = lambda a: jnp.where(side == 1, a[16:], a[:16])
        fr, fi, o1, o2 = pick(br), pick(bi), pick(ob1), pick(ob2)
        for t in range(16):
            k = (slot % 2) * 16 + t
            cr, ci = tile(ar[k : k + 1]), tile(ai[k : k + 1])
            row = slot * 512 + t * 16
            t_ref[row : row + 16, :] = (cr * fr - ci * fi).astype(BF16)
            t_ref[row + 256 : row + 272, :] = (cr * fi + ci * fr).astype(BF16)
            outer_ref[slot, t * 16 : t * 16 + 16, :] = oar[k : k + 1] * o1 + oai[k : k + 1] * o2
    offset = iota((1024, 128), 0) - STRIDE * iota((1024, 128), 1)
    for s in range(STRIDE):
        perm_ref[:, s * 128 : (s + 1) * 128] = jnp.where(offset == s, 1.0, 0.0).astype(BF16)
    for s, rows in enumerate(deinterleave(own_ref[...], perm_ref[...])):
        xs_ref[s * 128 : (s + 1) * 128, :] = rows


def prep(ids, signals):
    full = lambda *shape: pl.BlockSpec(shape, lambda i, ids: (0,) * len(shape))
    return pl.pallas_call(
        prep_kernel,
        grid_spec=pltpu.PrefetchScalarGridSpec(
            num_scalar_prefetch=1,
            grid=(1,),
            in_specs=[pl.BlockSpec((128, 2048), lambda i, ids: (ids[0], 0))],
            out_specs=[full(1024, 256), full(1024, 1024), full(2048, 512), full(4, 256, 128)],
        ),
        out_shape=[
            jax.ShapeDtypeStruct((1024, 256), BF16),
            jax.ShapeDtypeStruct((1024, 1024), BF16),
            jax.ShapeDtypeStruct((2048, 512), BF16),
            jax.ShapeDtypeStruct((4, 256, 128), F32),
        ],
        compiler_params=pltpu.CompilerParams(vmem_limit_bytes=LIMIT),
        name="prep",
    )(ids, signals)


def combine(f_ref, outer_ref, slot, *out_refs):
    half = math.sqrt(0.5)

    def step(chunk, carry):
        row0 = pl.multiple_of(chunk * 16, 16)
        gr, gi = [], []
        outer = outer_ref[slot, pl.ds(row0, 16), :]
        for s in range(STRIDE):
            a = f_ref[pl.ds(row0, 16), s * 128 : (s + 1) * 128]
            b = f_ref[pl.ds(row0 + 256, 16), s * 128 : (s + 1) * 128]
            wr = outer[:, s : s + 1]
            wi = outer[:, STRIDE + s : STRIDE + s + 1]
            gr.append(wr * a - wi * b)
            gi.append(wr * b + wi * a)
        pr = [gr[s] + gr[s + 4] for s in range(4)]
        pi = [gi[s] + gi[s + 4] for s in range(4)]
        mr = [gr[s] - gr[s + 4] for s in range(4)]
        mi = [gi[s] - gi[s + 4] for s in range(4)]
        er, ei = mr[0] + mi[2], mi[0] - mr[2]
        dr, di = mr[1] + mi[3], mi[1] - mr[3]
        results = (
            (pr[0] + pr[2]) + (pr[1] + pr[3]),
            er + half * (dr + di),
            (pi[0] + pi[2]) + (pi[1] + pi[3]),
            ei + half * (di - dr),
        )
        for place, value in enumerate(results):
            for out_ref in out_refs:
                out_ref[pl.ds(row0 + 256 * place, 16), :] = value.astype(out_ref.dtype)
        return carry

    lax.fori_loop(0, 16, step, 0, unroll=4)


def first_kernel(other_ref, own_ref, perm_ref, t_ref, outer_ref, out_ref, xs_ref, f_ref):
    xs_ref[:, 0:256] = own_ref[...]
    for s, rows in enumerate(deinterleave(other_ref[...], perm_ref[...])):
        xs_ref[s * 128 : (s + 1) * 128, 256:512] = rows
    f_ref[...] = lax.dot_general(
        t_ref[0:512, :], xs_ref[...], (((1,), (1,)), ((), ())), preferred_element_type=F32
    )
    combine(f_ref, outer_ref, 0, out_ref)


def spectrum(slot, xs_ref, t_ref, f_ref):
    f_ref[...] = lax.dot_general(
        t_ref[slot * 512 : slot * 512 + 512, :], xs_ref[...], (((1,), (1,)), ((), ())), preferred_element_type=F32
    )


def second_kernel(xs_ref, t_ref, outer_ref, out_ref, f_ref):
    spectrum(1, xs_ref, t_ref, f_ref)
    combine(f_ref, outer_ref, 1, out_ref)


def own_kernel(xs_ref, t_ref, outer_ref, owned_ref, wide_ref, out_ref, f_ref):
    for index in range(2):
        spectrum(2 + index, xs_ref, t_ref, f_ref.at[index])
        combine(f_ref.at[index], outer_ref, 2 + index, wide_ref.at[index], out_ref.at[index])


VM = pl.BlockSpec(memory_space=pltpu.VMEM)


def dft_first(other, own, perm, table, outer):
    return pl.pallas_call(
        first_kernel,
        in_specs=[VM] * 5,
        out_specs=[VM, VM],
        out_shape=[jax.ShapeDtypeStruct((1024, 128), BF16), jax.ShapeDtypeStruct((1024, 512), BF16)],
        scratch_shapes=[pltpu.VMEM((512, 1024), F32)],
        compiler_params=pltpu.CompilerParams(vmem_limit_bytes=LIMIT),
        name="dft_first",
    )(other, own, perm, table, outer)


def dft_second(xs, table, outer):
    return pl.pallas_call(
        second_kernel,
        in_specs=[VM] * 3,
        out_specs=VM,
        out_shape=jax.ShapeDtypeStruct((1024, 128), BF16),
        scratch_shapes=[pltpu.VMEM((512, 1024), F32)],
        compiler_params=pltpu.CompilerParams(vmem_limit_bytes=LIMIT),
        name="dft_second",
    )(xs, table, outer)


def dft_own(xs, table, outer, owned):
    return pl.pallas_call(
        own_kernel,
        in_specs=[VM] * 4,
        out_specs=[VM, VM],
        out_shape=[jax.ShapeDtypeStruct((2, 1024, 128), F32), jax.ShapeDtypeStruct((2, 1024, 128), BF16)],
        scratch_shapes=[pltpu.VMEM((2, 512, 1024), F32)],
        compiler_params=pltpu.CompilerParams(vmem_limit_bytes=LIMIT),
        name="dft_own",
    )(xs, table, outer, owned)


def form_kernel(part, ids_ref, wide_ref, got_ref, sib_ref, sib_got_ref, group_ref, w0_ref, w1_ref, *rest):
    out_ref, l_ref, w_ref = rest[-3:]
    core, half = ids_ref[0], ids_ref[1]
    for mine, theirs, place in ((wide_ref, got_ref, core), (sib_ref, sib_got_ref, 1 - core)):
        lane0 = pl.multiple_of(place * 128, 128)
        both = (mine[part].astype(F32) + theirs[...].astype(F32)).astype(BF16)
        sr, si = both[0:512], both[512:1024]
        l_ref[0:512, pl.ds(lane0, 128)] = sr
        l_ref[0:512, pl.ds(lane0 + 256, 128)] = -si
        l_ref[512:1024, pl.ds(lane0, 128)] = si
        l_ref[512:1024, pl.ds(lane0 + 256, 128)] = sr
    for g in range(3):
        for p in range(2):
            for b, ref in ((0, w0_ref), (1, w1_ref)):
                row, col = g * 256 + b * 128, p * 256
                w_ref[row : row + 128, col : col + 256] = ref[g * 2 + p]
    total = jnp.zeros((2, 512, 256), F32)
    groups = group_ref[part]
    for g in range(3):
        acc = lax.dot_general(
            l_ref[...], w_ref[g * 256 : g * 256 + 256, :], (((1,), (1,)), ((), ())), preferred_element_type=F32
        )
        total = jnp.where((groups == g)[None], acc.reshape(2, 512, 256), total)
    for b in range(2):
        block = total[:, :, b * 128 : b * 128 + 128]
        re = block[0].reshape(2, 2, 8, 16, 128)
        im = block[1].reshape(2, 2, 8, 16, 128)
        pair = jnp.concatenate([re, im], 3).astype(BF16)
        side = half if b == 0 else 1 - half
        for f2 in range(2):
            out_ref[2 * f2 + part, :, pl.ds(side, 1)] = pair[f2][:, None]


def form(part, ids, spec, group, weights, begun=()):
    return pl.pallas_call(
        lambda *refs: form_kernel(part, *refs),
        in_specs=[pl.BlockSpec(memory_space=pltpu.SMEM)] + [VM] * (7 + len(begun)),
        out_specs=VM,
        out_shape=jax.ShapeDtypeStruct((4, 2, 2, 8, 32, 128), BF16),
        input_output_aliases={8: 0} if begun else {},
        scratch_shapes=[pltpu.VMEM((1024, 512), BF16), pltpu.VMEM((768, 512), BF16)],
        compiler_params=pltpu.CompilerParams(vmem_limit_bytes=LIMIT),
        name="form_b" if part else "form_a",
    )(ids, *spec, group, *weights, *begun)


def add_first_kernel(got_ref, out_ref):
    for z in range(8):
        for side in range(2):
            total = got_ref[side, z].astype(F32)
            for src in range(1, 8):
                total = total + got_ref[2 * src + side, z].astype(F32)
            out_ref[z, side] = total


def add_last_kernel(got_ref, out_ref):
    for side in range(2):
        total = got_ref[0, side]
        for src in range(1, 8):
            total = total + got_ref[src, side]
        for p in range(2):
            out_ref[side * 16 : side * 16 + 16, p, :] = total[p * 16 : p * 16 + 16]


def add_first(got):
    return pl.pallas_call(
        add_first_kernel,
        in_specs=[VM],
        out_specs=VM,
        out_shape=jax.ShapeDtypeStruct((8, 2, 32, 128), F32),
        compiler_params=pltpu.CompilerParams(vmem_limit_bytes=LIMIT),
        name="add_first",
    )(got)


def add_last(got):
    return pl.pallas_call(
        add_last_kernel,
        in_specs=[VM],
        out_specs=VM,
        out_shape=jax.ShapeDtypeStruct((32, 2, 128), F32),
        compiler_params=pltpu.CompilerParams(vmem_limit_bytes=LIMIT),
        name="add_last",
    )(got)


def shards(signals, weights, bin_group):
    half, core = lax.axis_index("xhi"), lax.axis_index("core")

    def exchange(value, flip):
        return lax.ppermute(value, ("xhi", "core"), [(i, i ^ flip) for i in range(4)])

    ids = jnp.stack([core, half])
    blocks = weights.reshape(6, 128, 256)
    w_far = exchange(blocks, 2)
    theirs = lax.dynamic_slice_in_dim(signals, (1 - core) * 128, 128, 0)
    other = exchange(theirs, 1)
    own, perm, table, outer = prep(ids, pltpu.with_memory_space_constraint(signals, pltpu.HBM))

    spec0, xs = dft_first(other, own, perm, table, outer)
    got0 = exchange(spec0, 2)
    spec1 = dft_second(xs, table, outer)
    got1 = exchange(spec1, 2)
    owned = lax.dynamic_index_in_dim(bin_group.reshape(2, 2, 16, 2, 16), half, 3, keepdims=False)
    owned = owned.transpose(1, 0, 2, 3).reshape(2, 512, 1)
    wide, narrow = dft_own(xs, table, outer, owned)
    sib = exchange(narrow, 1)
    sib_got0 = exchange(got0, 1)
    sib_got1 = exchange(got1, 1)

    spec_a, spec_b = (wide, got0, sib, sib_got0), (wide, got1, sib, sib_got1)
    begun = form(0, ids, spec_a, owned, (blocks, w_far))
    parts = form(1, ids, spec_b, owned, (blocks, w_far), (begun,))
    got = lax.all_to_all(parts.reshape(16, 8, 32, 128), ("y", "xlo", "xhi"), 0, 0, tiled=True)
    column = add_first(got)
    final = lax.all_to_all(column, "z", 0, 0, tiled=True)
    return add_last(final)


def solution(mesh):
    fine = Mesh(mesh.devices.reshape(4, 2, 8, 2, 2), ("y", "xlo", "z", "xhi", "core"))
    chan, beam = ("y", "xlo", "z"), ("xhi", "core")
    in_specs = (P(chan, beam), P(None, None, beam, chan), P())
    out_specs = P(chan, None, beam)
    return jax.shard_map(shards, mesh=fine, in_specs=in_specs, out_specs=out_specs, check_vma=False)
```

```python
import math

import jax
import jax.numpy as jnp
from jax import lax
from jax.experimental import pallas as pl
from jax.experimental.pallas import tpu as pltpu
from jax.sharding import Mesh, PartitionSpec as P

F32 = jnp.float32
BF16 = jnp.bfloat16
I32 = jnp.int32

STRIDE = 8
SAMPLES = 8192
LIMIT = 24 * 1024 * 1024


def root(numer, denom):
    angle = 2.0 * math.pi / denom * (numer & (denom - 1)).astype(F32)
    return jnp.cos(angle), -jnp.sin(angle)


def iota(shape, dim):
    return lax.broadcasted_iota(I32, shape, dim)


def deinterleave(x, perm):
    out = []
    rows = jnp.concatenate([x[:, :1024], x[:, 1024:]], 0)
    split = jnp.dot(rows, perm, preferred_element_type=F32).astype(BF16)
    for s in range(STRIDE):
        cols = split[:, s * 128 : (s + 1) * 128]
        out.append(jnp.concatenate([cols[:128], cols[128:]], 1))
    return out


def prep_kernel(ids_ref, own_ref, xs_ref, perm_ref, t_ref, outer_ref):
    core, half = ids_ref[0], ids_ref[1]
    lane = iota((32, 512), 1)
    part = lane // 128
    u = jnp.where(part < 2, 2 * core + part, 2 * (1 - core) + part - 2)
    m = u * 128 + (lane & 127)
    ar, ai = root(iota((32, 128), 0) * iota((32, 128), 1), 32)
    br, bi = root((iota((32, 512), 0) + 1) * m, 1024)
    s = iota((32, 128), 1) & (STRIDE - 1)
    imag = (iota((32, 128), 1) & STRIDE) != 0
    oar, oai = root(iota((32, 128), 0) * s * 32, SAMPLES)
    obr, obi = root((iota((32, 128), 0) + 1) * (s + SAMPLES // 2 * half), SAMPLES)
    scale = 1.0 / math.sqrt(SAMPLES)
    ob1 = jnp.where(imag, obi, obr) * scale
    ob2 = jnp.where(imag, obr, -obi) * scale
    tile = lambda row: jnp.concatenate([row] * 4, 1)
    for slot in range(4):
        side = (1 - half) if slot < 2 else half
        pick = lambda a: jnp.where(side == 1, a[16:], a[:16])
        fr, fi, o1, o2 = pick(br), pick(bi), pick(ob1), pick(ob2)
        for t in range(16):
            k = (slot % 2) * 16 + t
            cr, ci = tile(ar[k : k + 1]), tile(ai[k : k + 1])
            row = slot * 512 + t * 16
            t_ref[row : row + 16, :] = (cr * fr - ci * fi).astype(BF16)
            t_ref[row + 256 : row + 272, :] = (cr * fi + ci * fr).astype(BF16)
            outer_ref[slot, t * 16 : t * 16 + 16, :] = oar[k : k + 1] * o1 + oai[k : k + 1] * o2
    offset = iota((1024, 128), 0) - STRIDE * iota((1024, 128), 1)
    for s in range(STRIDE):
        perm_ref[:, s * 128 : (s + 1) * 128] = jnp.where(offset == s, 1.0, 0.0).astype(BF16)
    for s, rows in enumerate(deinterleave(own_ref[...], perm_ref[...])):
        xs_ref[s * 128 : (s + 1) * 128, :] = rows


def prep(ids, signals):
    full = lambda *shape: pl.BlockSpec(shape, lambda i, ids: (0,) * len(shape))
    return pl.pallas_call(
        prep_kernel,
        grid_spec=pltpu.PrefetchScalarGridSpec(
            num_scalar_prefetch=1,
            grid=(1,),
            in_specs=[pl.BlockSpec((128, 2048), lambda i, ids: (ids[0], 0))],
            out_specs=[full(1024, 256), full(1024, 1024), full(2048, 512), full(4, 256, 128)],
        ),
        out_shape=[
            jax.ShapeDtypeStruct((1024, 256), BF16),
            jax.ShapeDtypeStruct((1024, 1024), BF16),
            jax.ShapeDtypeStruct((2048, 512), BF16),
            jax.ShapeDtypeStruct((4, 256, 128), F32),
        ],
        compiler_params=pltpu.CompilerParams(vmem_limit_bytes=LIMIT),
        name="prep",
    )(ids, signals)


def combine(f_ref, outer_ref, slot, *out_refs):
    half = math.sqrt(0.5)

    def step(chunk, carry):
        row0 = pl.multiple_of(chunk * 16, 16)
        gr, gi = [], []
        outer = outer_ref[slot, pl.ds(row0, 16), :]
        for s in range(STRIDE):
            a = f_ref[pl.ds(row0, 16), s * 128 : (s + 1) * 128]
            b = f_ref[pl.ds(row0 + 256, 16), s * 128 : (s + 1) * 128]
            wr = outer[:, s : s + 1]
            wi = outer[:, STRIDE + s : STRIDE + s + 1]
            gr.append(wr * a - wi * b)
            gi.append(wr * b + wi * a)
        pr = [gr[s] + gr[s + 4] for s in range(4)]
        pi = [gi[s] + gi[s + 4] for s in range(4)]
        mr = [gr[s] - gr[s + 4] for s in range(4)]
        mi = [gi[s] - gi[s + 4] for s in range(4)]
        er, ei = mr[0] + mi[2], mi[0] - mr[2]
        dr, di = mr[1] + mi[3], mi[1] - mr[3]
        results = (
            (pr[0] + pr[2]) + (pr[1] + pr[3]),
            er + half * (dr + di),
            (pi[0] + pi[2]) + (pi[1] + pi[3]),
            ei + half * (di - dr),
        )
        for place, value in enumerate(results):
            for out_ref in out_refs:
                out_ref[pl.ds(row0 + 256 * place, 16), :] = value.astype(out_ref.dtype)
        return carry

    lax.fori_loop(0, 16, step, 0, unroll=4)


def first_kernel(ids_ref, other_ref, own_ref, perm_ref, t_ref, outer_ref, out_ref, xs_ref, f_ref):
    xs_ref[:, 0:256] = own_ref[...]
    other = other_ref[pl.ds(pl.multiple_of(ids_ref[0] * 128, 128), 128), :]
    for s, rows in enumerate(deinterleave(other, perm_ref[...])):
        xs_ref[s * 128 : (s + 1) * 128, 256:512] = rows
    f_ref[...] = lax.dot_general(
        t_ref[0:512, :], xs_ref[...], (((1,), (1,)), ((), ())), preferred_element_type=F32
    )
    combine(f_ref, outer_ref, 0, out_ref)


def spectrum(slot, xs_ref, t_ref, f_ref):
    f_ref[...] = lax.dot_general(
        t_ref[slot * 512 : slot * 512 + 512, :], xs_ref[...], (((1,), (1,)), ((), ())), preferred_element_type=F32
    )


def second_kernel(xs_ref, t_ref, outer_ref, out_ref, f_ref):
    spectrum(1, xs_ref, t_ref, f_ref)
    combine(f_ref, outer_ref, 1, out_ref)


def own_kernel(xs_ref, t_ref, outer_ref, owned_ref, wide_ref, out_ref, f_ref):
    for index in range(2):
        spectrum(2 + index, xs_ref, t_ref, f_ref.at[index])
        combine(f_ref.at[index], outer_ref, 2 + index, wide_ref.at[index], out_ref.at[index])


VM = pl.BlockSpec(memory_space=pltpu.VMEM)


def dft_first(ids, other, own, perm, table, outer):
    return pl.pallas_call(
        first_kernel,
        in_specs=[pl.BlockSpec(memory_space=pltpu.SMEM)] + [VM] * 5,
        out_specs=[VM, VM],
        out_shape=[jax.ShapeDtypeStruct((1024, 128), BF16), jax.ShapeDtypeStruct((1024, 512), BF16)],
        scratch_shapes=[pltpu.VMEM((512, 1024), F32)],
        compiler_params=pltpu.CompilerParams(vmem_limit_bytes=LIMIT),
        name="dft_first",
    )(ids, other, own, perm, table, outer)


def dft_second(xs, table, outer):
    return pl.pallas_call(
        second_kernel,
        in_specs=[VM] * 3,
        out_specs=VM,
        out_shape=jax.ShapeDtypeStruct((1024, 128), BF16),
        scratch_shapes=[pltpu.VMEM((512, 1024), F32)],
        compiler_params=pltpu.CompilerParams(vmem_limit_bytes=LIMIT),
        name="dft_second",
    )(xs, table, outer)


def dft_own(xs, table, outer, owned):
    return pl.pallas_call(
        own_kernel,
        in_specs=[VM] * 4,
        out_specs=[VM, VM],
        out_shape=[jax.ShapeDtypeStruct((2, 1024, 128), F32), jax.ShapeDtypeStruct((2, 1024, 128), BF16)],
        scratch_shapes=[pltpu.VMEM((2, 512, 1024), F32)],
        compiler_params=pltpu.CompilerParams(vmem_limit_bytes=LIMIT),
        name="dft_own",
    )(xs, table, outer, owned)


def form_kernel(part, ids_ref, wide_ref, got_ref, sib_ref, sib_got_ref, group_ref, w0_ref, w1_ref, *rest):
    out_ref, l_ref, w_ref = rest[-3:]
    core, half = ids_ref[0], ids_ref[1]
    for mine, theirs, place in ((wide_ref, got_ref, core), (sib_ref, sib_got_ref, 1 - core)):
        lane0 = pl.multiple_of(place * 128, 128)
        both = (mine[part].astype(F32) + theirs[...].astype(F32)).astype(BF16)
        sr, si = both[0:512], both[512:1024]
        l_ref[0:512, pl.ds(lane0, 128)] = sr
        l_ref[0:512, pl.ds(lane0 + 256, 128)] = -si
        l_ref[512:1024, pl.ds(lane0, 128)] = si
        l_ref[512:1024, pl.ds(lane0 + 256, 128)] = sr
    for g in range(3):
        for p in range(2):
            for b, ref in ((0, w0_ref), (1, w1_ref)):
                row, col = g * 256 + b * 128, p * 256
                w_ref[row : row + 128, col : col + 256] = ref[g * 2 + p]
    total = jnp.zeros((2, 512, 256), F32)
    groups = group_ref[part]
    for g in range(3):
        acc = lax.dot_general(
            l_ref[...], w_ref[g * 256 : g * 256 + 256, :], (((1,), (1,)), ((), ())), preferred_element_type=F32
        )
        total = jnp.where((groups == g)[None], acc.reshape(2, 512, 256), total)
    for b in range(2):
        block = total[:, :, b * 128 : b * 128 + 128]
        re = block[0].reshape(2, 2, 8, 16, 128)
        im = block[1].reshape(2, 2, 8, 16, 128)
        pair = jnp.concatenate([re, im], 3).astype(BF16)
        side = half if b == 0 else 1 - half
        for f2 in range(2):
            out_ref[2 * f2 + part, :, :, pl.ds(side, 1)] = pair[f2][:, :, None]


def form(part, ids, spec, group, weights, begun=()):
    return pl.pallas_call(
        lambda *refs: form_kernel(part, *refs),
        in_specs=[pl.BlockSpec(memory_space=pltpu.SMEM)] + [VM] * (7 + len(begun)),
        out_specs=VM,
        out_shape=jax.ShapeDtypeStruct((4, 2, 8, 2, 32, 128), BF16),
        input_output_aliases={8: 0} if begun else {},
        scratch_shapes=[pltpu.VMEM((1024, 512), BF16), pltpu.VMEM((768, 512), BF16)],
        compiler_params=pltpu.CompilerParams(vmem_limit_bytes=LIMIT),
        name="form_b" if part else "form_a",
    )(ids, *spec, group, *weights, *begun)


def add_kernel(got_ref, out_ref):
    for side in range(2):
        parts = [got_ref[2 * src + side].astype(F32) for src in range(4)]
        for src in range(4, 64):
            parts[src % 4] = parts[src % 4] + got_ref[2 * src + side].astype(F32)
        total = (parts[0] + parts[1]) + (parts[2] + parts[3])
        for p in range(2):
            out_ref[side * 16 : side * 16 + 16, p, :] = total[p * 16 : p * 16 + 16]


def add(got):
    return pl.pallas_call(
        add_kernel,
        in_specs=[VM],
        out_specs=VM,
        out_shape=jax.ShapeDtypeStruct((32, 2, 128), F32),
        compiler_params=pltpu.CompilerParams(vmem_limit_bytes=LIMIT),
        name="add",
    )(got)


def shards(signals, weights, bin_group):
    half, core = lax.axis_index("xhi"), lax.axis_index("core")

    def exchange(value, flip):
        return lax.ppermute(value, ("xhi", "core"), [(i, i ^ flip) for i in range(4)])

    ids = jnp.stack([core, half])
    blocks = weights.reshape(6, 128, 256)
    w_far = exchange(blocks, 2)
    other = exchange(signals, 1)
    own, perm, table, outer = prep(ids, pltpu.with_memory_space_constraint(signals, pltpu.HBM))

    spec0, xs = dft_first(ids, other, own, perm, table, outer)
    got0 = exchange(spec0, 2)
    spec1 = dft_second(xs, table, outer)
    got1 = exchange(spec1, 2)
    owned = lax.dynamic_index_in_dim(bin_group.reshape(2, 2, 16, 2, 16), half, 3, keepdims=False)
    owned = owned.transpose(1, 0, 2, 3).reshape(2, 512, 1)
    wide, narrow = dft_own(xs, table, outer, owned)
    sib = exchange(narrow, 1)
    sib_got0 = exchange(got0, 1)
    sib_got1 = exchange(got1, 1)

    spec_a, spec_b = (wide, got0, sib, sib_got0), (wide, got1, sib, sib_got1)
    begun = form(0, ids, spec_a, owned, (blocks, w_far))
    parts = form(1, ids, spec_b, owned, (blocks, w_far), (begun,))
    got = lax.all_to_all(parts.reshape(128, 32, 128), ("y", "xlo", "z", "xhi"), 0, 0, tiled=True)
    return add(got)


def solution(mesh):
    fine = Mesh(mesh.devices.reshape(4, 2, 8, 2, 2), ("y", "xlo", "z", "xhi", "core"))
    chan, beam = ("y", "xlo", "z"), ("xhi", "core")
    in_specs = (P(chan, beam), P(None, None, beam, chan), P())
    out_specs = P(chan, None, beam)
    return jax.shard_map(shards, mesh=fine, in_specs=in_specs, out_specs=out_specs, check_vma=False)
```

```python
import math

import jax
import jax.numpy as jnp
from jax import lax
from jax.experimental import pallas as pl
from jax.experimental.pallas import tpu as pltpu
from jax.sharding import Mesh, PartitionSpec as P

F32 = jnp.float32
BF16 = jnp.bfloat16
I32 = jnp.int32

STRIDE = 8
SAMPLES = 8192
LIMIT = 16 * 1024 * 1024


def root(numer, denom):
    angle = 2.0 * math.pi / denom * (numer & (denom - 1)).astype(F32)
    return jnp.cos(angle), -jnp.sin(angle)


def iota(shape, dim):
    return lax.broadcasted_iota(I32, shape, dim)


def deinterleave(x, perm):
    out = []
    rows = jnp.concatenate([x[:, :1024], x[:, 1024:]], 0)
    split = jnp.dot(rows, perm, preferred_element_type=F32).astype(BF16)
    for s in range(STRIDE):
        cols = split[:, s * 128 : (s + 1) * 128]
        out.append(jnp.concatenate([cols[:128], cols[128:]], 1))
    return out


def prep_kernel(ids_ref, own_ref, xs_ref, perm_ref, t_ref, outer_ref):
    core, half, low = ids_ref[0], ids_ref[1], ids_ref[2]
    lane = iota((32, 512), 1)
    part = lane // 128
    u = jnp.where(part < 2, 2 * core + part, 2 * (1 - core) + part - 2)
    m = u * 128 + (lane & 127)
    ar, ai = root(iota((32, 128), 0) * iota((32, 128), 1), 32)
    br, bi = root((iota((32, 512), 0) + 1) * m, 1024)
    s = iota((32, 128), 1) & (STRIDE - 1)
    imag = (iota((32, 128), 1) & STRIDE) != 0
    oar, oai = root(iota((32, 128), 0) * s * 32, SAMPLES)
    obr, obi = root((iota((32, 128), 0) + 1) * (s + SAMPLES // 2 * half), SAMPLES)
    scale = 1.0 / math.sqrt(SAMPLES)
    ob1 = jnp.where(imag, obi, obr) * scale
    ob2 = jnp.where(imag, obr, -obi) * scale
    tile = lambda row: jnp.concatenate([row] * 4, 1)
    for tl in range(2):
        for th in range(2):
            slot = {(0, 1): 0, (1, 0): 1, (1, 1): 2, (0, 0): 3}[(tl, th)]
            swap_h = half if th == 0 else 1 - half
            swap_l = low if tl == 0 else 1 - low
            pick = lambda a: jnp.where(swap_h == 1, a[16:], a[:16])
            fr, fi, o1, o2 = pick(br), pick(bi), pick(ob1), pick(ob2)
            for t in range(16):
                k0 = (t // 8) * 16 + t % 8
                sel = lambda a: jnp.where(swap_l == 1, a[k0 + 8 : k0 + 9], a[k0 : k0 + 1])
                cr, ci = tile(sel(ar)), tile(sel(ai))
                row = slot * 512 + t * 16
                t_ref[row : row + 16, :] = (cr * fr - ci * fi).astype(BF16)
                t_ref[row + 256 : row + 272, :] = (cr * fi + ci * fr).astype(BF16)
                outer_ref[slot, t * 16 : t * 16 + 16, :] = sel(oar) * o1 + sel(oai) * o2
    offset = iota((1024, 128), 0) - STRIDE * iota((1024, 128), 1)
    for s in range(STRIDE):
        perm_ref[:, s * 128 : (s + 1) * 128] = jnp.where(offset == s, 1.0, 0.0).astype(BF16)
    for s, rows in enumerate(deinterleave(own_ref[...], perm_ref[...])):
        xs_ref[s * 128 : (s + 1) * 128, :] = rows


def prep(ids, signals):
    full = lambda *shape: pl.BlockSpec(shape, lambda i, ids: (0,) * len(shape))
    return pl.pallas_call(
        prep_kernel,
        grid_spec=pltpu.PrefetchScalarGridSpec(
            num_scalar_prefetch=1,
            grid=(1,),
            in_specs=[pl.BlockSpec((128, 2048), lambda i, ids: (ids[0], 0))],
            out_specs=[full(1024, 256), full(1024, 1024), full(2048, 512), full(4, 256, 128)],
        ),
        out_shape=[
            jax.ShapeDtypeStruct((1024, 256), BF16),
            jax.ShapeDtypeStruct((1024, 1024), BF16),
            jax.ShapeDtypeStruct((2048, 512), BF16),
            jax.ShapeDtypeStruct((4, 256, 128), F32),
        ],
        compiler_params=pltpu.CompilerParams(vmem_limit_bytes=LIMIT),
        name="prep",
    )(ids, signals)


def combine(f_ref, outer_ref, slot, out_ref):
    half = math.sqrt(0.5)

    def step(chunk, carry):
        row0 = pl.multiple_of(chunk * 16, 16)
        gr, gi = [], []
        outer = outer_ref[slot, pl.ds(row0, 16), :]
        for s in range(STRIDE):
            a = f_ref[pl.ds(row0, 16), s * 128 : (s + 1) * 128]
            b = f_ref[pl.ds(row0 + 256, 16), s * 128 : (s + 1) * 128]
            wr = outer[:, s : s + 1]
            wi = outer[:, STRIDE + s : STRIDE + s + 1]
            gr.append(wr * a - wi * b)
            gi.append(wr * b + wi * a)
        pr = [gr[s] + gr[s + 4] for s in range(4)]
        pi = [gi[s] + gi[s + 4] for s in range(4)]
        mr = [gr[s] - gr[s + 4] for s in range(4)]
        mi = [gi[s] - gi[s + 4] for s in range(4)]
        er, ei = mr[0] + mi[2], mi[0] - mr[2]
        dr, di = mr[1] + mi[3], mi[1] - mr[3]
        results = (
            (pr[0] + pr[2]) + (pr[1] + pr[3]),
            er + half * (dr + di),
            (pi[0] + pi[2]) + (pi[1] + pi[3]),
            ei + half * (di - dr),
        )
        for place, value in enumerate(results):
            out_ref[pl.ds(row0 + 256 * place, 16), :] = value.astype(out_ref.dtype)
        return carry

    lax.fori_loop(0, 16, step, 0, unroll=4)


def first_kernel(ids_ref, other_ref, own_ref, perm_ref, t_ref, outer_ref, out_ref, xs_ref, f_ref):
    xs_ref[:, 0:256] = own_ref[...]
    other = other_ref[pl.ds(pl.multiple_of(ids_ref[0] * 128, 128), 128), :]
    for s, rows in enumerate(deinterleave(other, perm_ref[...])):
        xs_ref[s * 128 : (s + 1) * 128, 256:512] = rows
    f_ref[...] = lax.dot_general(
        t_ref[0:512, :], xs_ref[...], (((1,), (1,)), ((), ())), preferred_element_type=F32
    )
    combine(f_ref, outer_ref, 0, out_ref)


def next_kernel(slots, xs_ref, t_ref, outer_ref, *rest):
    outs, f_ref = rest[:-1], rest[-1]
    for index, slot in enumerate(slots):
        buf = f_ref.at[index]
        buf[...] = lax.dot_general(
            t_ref[slot * 512 : slot * 512 + 512, :],
            xs_ref[...],
            (((1,), (1,)), ((), ())),
            preferred_element_type=F32,
        )
        combine(buf, outer_ref, slot, outs[index])


VM = pl.BlockSpec(memory_space=pltpu.VMEM)


def dft_first(ids, other, own, perm, table, outer):
    return pl.pallas_call(
        first_kernel,
        in_specs=[pl.BlockSpec(memory_space=pltpu.SMEM)] + [VM] * 5,
        out_specs=[VM, VM],
        out_shape=[jax.ShapeDtypeStruct((1024, 128), BF16), jax.ShapeDtypeStruct((1024, 512), BF16)],
        scratch_shapes=[pltpu.VMEM((512, 1024), F32)],
        compiler_params=pltpu.CompilerParams(vmem_limit_bytes=LIMIT),
        name="dft_first",
    )(ids, other, own, perm, table, outer)


def last_kernel(ids_ref, xs_ref, t_ref, outer_ref, bins_ref, out_ref, group_ref, f_ref):
    next_kernel((3,), xs_ref, t_ref, outer_ref, out_ref, f_ref)
    half, low = ids_ref[1], ids_ref[2]
    row = iota((512, 128), 0)
    block = row // 128 * 16 + low * 8 + row // 16 % 8
    place = block % 4 * 32 + half * 16 + row % 16
    line = jnp.where(iota((512, 128), 1) == block // 4, 1.0, 0.0).astype(BF16)[:, :16]
    lines = jnp.dot(line, bins_ref[...].astype(F32).astype(BF16), preferred_element_type=F32)
    chosen = jnp.where(iota((512, 128), 1) == place, lines, 0.0)
    group_ref[...] = jnp.broadcast_to(jnp.sum(chosen, axis=1, keepdims=True), (512, 128))


def dft_last(ids, xs, table, outer, bins):
    return pl.pallas_call(
        last_kernel,
        in_specs=[pl.BlockSpec(memory_space=pltpu.SMEM)] + [VM] * 4,
        out_specs=[VM, VM],
        out_shape=[jax.ShapeDtypeStruct((1024, 128), F32), jax.ShapeDtypeStruct((512, 128), F32)],
        scratch_shapes=[pltpu.VMEM((1, 512, 1024), F32)],
        compiler_params=pltpu.CompilerParams(vmem_limit_bytes=LIMIT),
        name="dft_last",
    )(ids, xs, table, outer, bins)


def dft_next(xs, table, outer, slots, dtype):
    return pl.pallas_call(
        lambda *refs: next_kernel(slots, *refs),
        in_specs=[VM] * 3,
        out_specs=[VM] * len(slots),
        out_shape=[jax.ShapeDtypeStruct((1024, 128), dtype)] * len(slots),
        scratch_shapes=[pltpu.VMEM((len(slots), 512, 1024), F32)],
        compiler_params=pltpu.CompilerParams(vmem_limit_bytes=LIMIT),
    )(xs, table, outer)


def form_beams(side, l_ref, w_ref, group_ref, out_ref):
    acc = lax.dot_general(l_ref[...], w_ref[...], (((1,), (1,)), ((), ())), preferred_element_type=F32)
    acc = acc.reshape(2, 512, 384)
    group = group_ref[...][None]
    total = jnp.where(group == 0, acc[:, :, 0:128], jnp.where(group == 1, acc[:, :, 128:256], acc[:, :, 256:384]))
    re = total[0].reshape(4, 8, 16, 128)
    im = total[1].reshape(4, 8, 16, 128)
    out_ref[:, :, pl.ds(side, 1)] = jnp.concatenate([re, im], 2).astype(BF16)[:, :, None]


def near_kernel(ids_ref, s0_ref, s1_ref, p0_ref, p1_ref, group_ref, w0_ref, w1_ref, out_ref, l_ref, w_ref):
    core, half = ids_ref[0], ids_ref[1]
    for srcs, place in (((s0_ref, s1_ref), core), ((p0_ref, p1_ref), 1 - core)):
        for xl in range(2):
            lane0 = pl.multiple_of(xl * 256 + place * 128, 128)
            src = srcs[xl]
            sr, si = src[0:512, :], src[512:1024, :]
            l_ref[0:512, pl.ds(lane0, 128)] = sr
            l_ref[0:512, pl.ds(lane0 + 512, 128)] = -si
            l_ref[512:1024, pl.ds(lane0, 128)] = si
            l_ref[512:1024, pl.ds(lane0 + 512, 128)] = sr
    for i in range(6):
        row, col = i // 2 * 128, i % 2 * 512
        w_ref[row : row + 128, col : col + 256] = w0_ref[i]
        w_ref[row : row + 128, col + 256 : col + 512] = w1_ref[i]
    form_beams(half, l_ref, w_ref, group_ref, out_ref)


def far_kernel(ids_ref, l_ref, group_ref, w2a_ref, w2b_ref, w3_ref, begun_ref, out_ref, w_ref):
    for i in range(6):
        row, col = i // 2 * 128, i % 2 * 512
        w_ref[row : row + 128, col : col + 256] = w2a_ref[i] if i < 3 else w2b_ref[i - 3]
        w_ref[row : row + 128, col + 256 : col + 512] = w3_ref[i]
    form_beams(1 - ids_ref[1], l_ref, w_ref, group_ref, out_ref)


PARTS = jax.ShapeDtypeStruct((4, 8, 2, 32, 128), BF16)


def form_near(ids, spec, group, weights):
    return pl.pallas_call(
        near_kernel,
        in_specs=[pl.BlockSpec(memory_space=pltpu.SMEM)] + [VM] * 7,
        out_specs=[VM, VM],
        out_shape=[PARTS, jax.ShapeDtypeStruct((1024, 1024), BF16)],
        scratch_shapes=[pltpu.VMEM((384, 1024), BF16)],
        compiler_params=pltpu.CompilerParams(vmem_limit_bytes=LIMIT),
        name="form_near",
    )(ids, *spec, group, *weights)


def form_far(ids, lhs, group, weights, begun):
    return pl.pallas_call(
        far_kernel,
        in_specs=[pl.BlockSpec(memory_space=pltpu.SMEM)] + [VM] * 6,
        out_specs=VM,
        out_shape=PARTS,
        input_output_aliases={6: 0},
        scratch_shapes=[pltpu.VMEM((384, 1024), BF16)],
        compiler_params=pltpu.CompilerParams(vmem_limit_bytes=LIMIT),
        name="form_far",
    )(ids, lhs, group, *weights, begun)


def add_kernel(got_ref, out_ref):
    for side in range(2):
        parts = [got_ref[2 * src + side].astype(F32) for src in range(4)]
        for src in range(4, 32):
            parts[src % 4] = parts[src % 4] + got_ref[2 * src + side].astype(F32)
        total = (parts[0] + parts[1]) + (parts[2] + parts[3])
        for p in range(2):
            out_ref[side * 16 : side * 16 + 16, p, :] = total[p * 16 : p * 16 + 16]


def add(got):
    return pl.pallas_call(
        add_kernel,
        in_specs=[VM],
        out_specs=VM,
        out_shape=jax.ShapeDtypeStruct((32, 2, 128), F32),
        compiler_params=pltpu.CompilerParams(vmem_limit_bytes=LIMIT),
        name="add",
    )(got)


def shards(signals, weights, bin_group):
    half, core, low = lax.axis_index("xhi"), lax.axis_index("core"), lax.axis_index("xlo")
    ring = ("xlo", "xhi", "core")

    def exchange(value, flip):
        return lax.ppermute(value, ring, [(i, i ^ flip) for i in range(8)])

    ids = jnp.stack([core, half, low])
    blocks = weights.reshape(6, 128, 256)
    w1 = exchange(blocks, 4)
    w3 = exchange(blocks, 6)
    other = exchange(signals, 1)
    own, perm, table, outer = prep(ids, pltpu.with_memory_space_constraint(signals, pltpu.HBM))

    spec0, xs = dft_first(ids, other, own, perm, table, outer)
    got0 = exchange(spec0, 2)
    spec1, spec2 = dft_next(xs, table, outer, (1, 2), BF16)
    got1 = exchange(spec1, 4)
    got2 = exchange(spec2, 6)
    w2a = exchange(w1[:3], 6)
    w2b = exchange(w3[3:], 4)
    spec3, owned = dft_last(ids, xs, table, outer, bin_group.reshape(16, 128))
    same = (spec3 + got0.astype(F32)).astype(BF16)
    same_sib = exchange(same, 1)
    cross = (got1.astype(F32) + got2.astype(F32)).astype(BF16)
    cross_sib = exchange(cross, 1)

    begun, lhs = form_near(ids, (same, cross, same_sib, cross_sib), owned, (blocks, w1))
    parts = form_far(ids, lhs, owned, (w2a, w2b, w3), begun)
    got = lax.all_to_all(parts.reshape(64, 32, 128), ("y", "z", "xhi"), 0, 0, tiled=True)
    return add(got)


def solution(mesh):
    fine = Mesh(mesh.devices.reshape(4, 2, 8, 2, 2), ("y", "xlo", "z", "xhi", "core"))
    chan, beam = ("y", "xlo", "z"), ("xhi", "core")
    in_specs = (P(chan, beam), P(None, None, beam, chan), P())
    out_specs = P(chan, None, beam)
    return jax.shard_map(shards, mesh=fine, in_specs=in_specs, out_specs=out_specs, check_vma=False)
```

```python
import math

import jax
import jax.numpy as jnp
from jax import lax
from jax.experimental import pallas as pl
from jax.experimental.pallas import tpu as pltpu
from jax.sharding import Mesh, PartitionSpec as P

F32 = jnp.float32
BF16 = jnp.bfloat16
I32 = jnp.int32

STRIDE = 8
SAMPLES = 8192
LIMIT = 16 * 1024 * 1024
UNROLL = 16


def root(numer, denom):
    angle = 2.0 * math.pi / denom * (numer & (denom - 1)).astype(F32)
    return jnp.cos(angle), -jnp.sin(angle)


def iota(shape, dim):
    return lax.broadcasted_iota(I32, shape, dim)


def deinterleave(x, perm):
    out = []
    rows = jnp.concatenate([x[:, :1024], x[:, 1024:]], 0)
    split = jnp.dot(rows, perm, preferred_element_type=F32).astype(BF16)
    for s in range(STRIDE):
        cols = split[:, s * 128 : (s + 1) * 128]
        out.append(jnp.concatenate([cols[:128], cols[128:]], 1))
    return out


def eighth(q):
    q = q & 7
    half = math.sqrt(0.5)
    odd = (q & 1) != 0
    re = jnp.where(odd, half, jnp.where((q & 2) != 0, 0.0, 1.0))
    re = jnp.where((q > 2) & (q < 6), -re, re)
    im = jnp.where(odd, half, jnp.where((q & 2) != 0, 1.0, 0.0))
    im = jnp.where(q < 4, -im, im)
    return re, im


def owner(ids_ref, slot):
    half, low = ids_ref[1], ids_ref[2]
    return (1 - half if slot in (0, 2) else half), (1 - low if slot in (1, 2) else low)


def block_of(t, low):
    return t // 8 * 16 + low * 8 + t % 8


def make_twiddles(ids_ref, slot, coarse_ref, fine_ref, t_ref, row0):
    half, low = owner(ids_ref, slot)
    first = pl.multiple_of(half * 16, 16)
    fr = fine_ref[0, pl.ds(first, 16), :]
    fi = fine_ref[1, pl.ds(first, 16), :]
    for t in range(16):
        k = block_of(t, low)
        cr = jnp.concatenate([coarse_ref[0, pl.ds(k, 1), :]] * 4, 1)
        ci = jnp.concatenate([coarse_ref[1, pl.ds(k, 1), :]] * 4, 1)
        row = row0 + t * 16
        t_ref[row : row + 16, :] = (cr * fr - ci * fi).astype(BF16)
        t_ref[row + 256 : row + 272, :] = (cr * fi + ci * fr).astype(BF16)


def prep_kernel(ids_ref, own_ref, xs_ref, perm_ref, t_ref, coarse_ref, fine_ref, outer_ref):
    core, half = ids_ref[0], ids_ref[1]
    row, lane = iota((32, 128), 0), iota((32, 128), 1)
    coarse_ref[0], coarse_ref[1] = root(row * lane, 32)
    br, bi = root((row + 1) * lane, 1024)
    for part in range(4):
        u = 2 * core + part if part < 2 else 2 * (1 - core) + part - 2
        er, ei = eighth((row + 1) * u)
        cols = slice(part * 128, part * 128 + 128)
        fine_ref[0, :, cols] = br * er - bi * ei
        fine_ref[1, :, cols] = br * ei + bi * er
    outer_ref[0], outer_ref[1] = root(row * 32, SAMPLES)
    outer_ref[2], outer_ref[3] = root(row + 1, SAMPLES)
    scale = 1.0 / math.sqrt(SAMPLES)
    outer_ref[4] = jnp.where((((row + 1) * half) & 1) != 0, -scale, scale)
    make_twiddles(ids_ref, 0, coarse_ref, fine_ref, t_ref, 0)
    same = jnp.where(iota((1024, 128), 0) // STRIDE == iota((1024, 128), 1), 1.0, 0.0).astype(BF16)
    phase = iota((16, 128), 0) & (STRIDE - 1)
    for s in range(STRIDE):
        keep = jnp.where(phase == s, 1.0, 0.0).astype(BF16)
        perm_ref[:, s * 128 : (s + 1) * 128] = (same.reshape(64, 16, 128) * keep[None]).reshape(1024, 128)
    for s, rows in enumerate(deinterleave(own_ref[...], perm_ref[...])):
        xs_ref[s * 128 : (s + 1) * 128, :] = rows


def prep(ids, signals):
    full = lambda *shape: pl.BlockSpec(shape, lambda i, ids: (0,) * len(shape))
    return pl.pallas_call(
        prep_kernel,
        grid_spec=pltpu.PrefetchScalarGridSpec(
            num_scalar_prefetch=1,
            grid=(1,),
            in_specs=[pl.BlockSpec((128, 2048), lambda i, ids: (ids[0], 0))],
            out_specs=[
                full(1024, 256),
                full(1024, 1024),
                full(512, 512),
                full(2, 32, 128),
                full(2, 32, 512),
                full(5, 32, 128),
            ],
        ),
        out_shape=[
            jax.ShapeDtypeStruct((1024, 256), BF16),
            jax.ShapeDtypeStruct((1024, 1024), BF16),
            jax.ShapeDtypeStruct((512, 512), BF16),
            jax.ShapeDtypeStruct((2, 32, 128), F32),
            jax.ShapeDtypeStruct((2, 32, 512), F32),
            jax.ShapeDtypeStruct((5, 32, 128), F32),
        ],
        compiler_params=pltpu.CompilerParams(vmem_limit_bytes=LIMIT),
        name="prep",
    )(ids, signals)


def times(w, x):
    return w[0] * x[0] - w[1] * x[1], w[0] * x[1] + w[1] * x[0]


def plus(x, y):
    return x[0] + y[0], x[1] + y[1]


def minus(x, y):
    return x[0] - y[0], x[1] - y[1]


def turned(x, y):
    return x[0] + y[1], x[1] - y[0]


def combine(ids_ref, slot, f_ref, outer_ref, out_ref, add_ref=None):
    half, low = owner(ids_ref, slot)
    first = pl.multiple_of(half * 16, 16)
    fine = outer_ref[2, pl.ds(first, 16), :], outer_ref[3, pl.ds(first, 16), :]
    scale = outer_ref[4, pl.ds(first, 16), :]
    eighth_root = math.sqrt(0.5)

    def step(t, carry):
        row0 = pl.multiple_of(t * 16, 16)
        k = block_of(t, low)
        w = times((outer_ref[0, pl.ds(k, 1), :], outer_ref[1, pl.ds(k, 1), :]), fine)
        w2 = times(w, w)
        w4 = times(w2, w2)
        wt = eighth_root * (w[0] + w[1]), eighth_root * (w[1] - w[0])
        term = lambda s: (
            f_ref[pl.ds(row0, 16), s * 128 : (s + 1) * 128],
            f_ref[pl.ds(row0 + 256, 16), s * 128 : (s + 1) * 128],
        )
        sums = []
        for s in range(2):
            near, far = term(s), times(w4, term(s + 4))
            up, down = plus(near, far), minus(near, far)
            near, far = term(s + 2), times(w4, term(s + 6))
            sums.append(
                (plus(up, times(w2, plus(near, far))), turned(down, times(w2, minus(near, far))))
            )
        low_bin = plus(sums[0][0], times(w, sums[1][0]))
        high_bin = plus(sums[0][1], times(wt, sums[1][1]))
        for place, value in enumerate((low_bin[0], high_bin[0], low_bin[1], high_bin[1])):
            rows = pl.ds(row0 + 256 * place, 16)
            value = value * scale
            if add_ref is not None:
                value = value + add_ref[rows, :].astype(F32)
            out_ref[rows, :] = value.astype(out_ref.dtype)
        return carry

    lax.fori_loop(0, 16, step, 0, unroll=UNROLL)


def spectrum(t_ref, row0, xs_ref, f_ref):
    f_ref[...] = lax.dot_general(
        t_ref[row0 : row0 + 512, :], xs_ref[...], (((1,), (1,)), ((), ())), preferred_element_type=F32
    )


def first_kernel(
    ids_ref, other_ref, own_ref, perm_ref, t_ref, coarse_ref, fine_ref, outer_ref, out_ref, xs_ref, rest_ref, f_ref
):
    xs_ref[:, 0:256] = own_ref[...]
    other = other_ref[pl.ds(pl.multiple_of(ids_ref[0] * 128, 128), 128), :]
    for s, rows in enumerate(deinterleave(other, perm_ref[...])):
        xs_ref[s * 128 : (s + 1) * 128, 256:512] = rows
    for slot in (1, 2, 3):
        make_twiddles(ids_ref, slot, coarse_ref, fine_ref, rest_ref, (slot - 1) * 512)
    spectrum(t_ref, 0, xs_ref, f_ref)
    combine(ids_ref, 0, f_ref, outer_ref, out_ref)


def next_kernel(ids_ref, xs_ref, rest_ref, outer_ref, out1_ref, out2_ref, f_ref):
    for index, out_ref in enumerate((out1_ref, out2_ref)):
        spectrum(rest_ref, index * 512, xs_ref, f_ref.at[index])
        combine(ids_ref, 1 + index, f_ref.at[index], outer_ref, out_ref)


def last_kernel(ids_ref, xs_ref, rest_ref, outer_ref, got_ref, bins_ref, out_ref, group_ref, f_ref):
    spectrum(rest_ref, 1024, xs_ref, f_ref)
    half, low = ids_ref[1], ids_ref[2]
    row, lane = iota((512, 128), 0), iota((512, 128), 1)
    line = jnp.where(lane == (row // 128 * 4 + low * 2 + row // 64 % 2), 1.0, 0.0).astype(BF16)[:, :16]
    lines = jnp.dot(line, bins_ref[...].astype(F32).astype(BF16), preferred_element_type=F32)
    place = row // 16 % 4 * 32 + half * 16 + row % 16
    chosen = jnp.where(lane == place, lines, 0.0).astype(BF16)
    group_ref[...] = jnp.dot(chosen, jnp.ones((128, 128), BF16), preferred_element_type=F32)
    combine(ids_ref, 3, f_ref, outer_ref, out_ref, got_ref)


VM = pl.BlockSpec(memory_space=pltpu.VMEM)


SM = pl.BlockSpec(memory_space=pltpu.SMEM)
PIECE = jax.ShapeDtypeStruct((1024, 128), BF16)


def call(kernel, count, out_shape, scratch):
    outs = len(out_shape) if isinstance(out_shape, list) else 0
    return pl.pallas_call(
        kernel,
        in_specs=[SM] + [VM] * count,
        out_specs=[VM] * outs if outs else VM,
        out_shape=out_shape,
        scratch_shapes=scratch,
        compiler_params=pltpu.CompilerParams(vmem_limit_bytes=LIMIT),
    )


def dft_first(*args):
    outs = [PIECE, jax.ShapeDtypeStruct((1024, 512), BF16), jax.ShapeDtypeStruct((1536, 512), BF16)]
    return call(first_kernel, 7, outs, [pltpu.VMEM((512, 1024), F32)])(*args)


def dft_next(*args):
    return call(next_kernel, 3, [PIECE, PIECE], [pltpu.VMEM((2, 512, 1024), F32)])(*args)


def dft_last(*args):
    outs = [PIECE, jax.ShapeDtypeStruct((512, 128), F32)]
    return call(last_kernel, 5, outs, [pltpu.VMEM((512, 1024), F32)])(*args)


def form_kernel(
    ids_ref, s0_ref, s1_ref, p0_ref, p1_ref, group_ref, w0_ref, w1_ref, w2a_ref, w2b_ref, w3_ref, out_ref, l_ref, w_ref
):
    core, half = ids_ref[0], ids_ref[1]
    for srcs, place in (((s0_ref, s1_ref), core), ((p0_ref, p1_ref), 1 - core)):
        for xl in range(2):
            lane0 = pl.multiple_of(xl * 256 + place * 128, 128)
            for r in range(0, 512, 64):
                sr, si = srcs[xl][r : r + 64, :], srcs[xl][512 + r : 576 + r, :]
                l_ref[r : r + 64, pl.ds(lane0, 128)] = sr
                l_ref[r : r + 64, pl.ds(lane0 + 512, 128)] = -si
                l_ref[512 + r : 576 + r, pl.ds(lane0, 128)] = si
                l_ref[512 + r : 576 + r, pl.ds(lane0 + 512, 128)] = sr
    for g in range(3):
        for p in range(2):
            i = g * 2 + p
            w2 = w2a_ref[i] if i < 3 else w2b_ref[i - 3]
            for b, xl, w in ((0, 0, w0_ref[i]), (0, 1, w1_ref[i]), (1, 0, w2), (1, 1, w3_ref[i])):
                row, col = g * 256 + b * 128, p * 512 + xl * 256
                w_ref[row : row + 128, col : col + 256] = w
    total = jnp.zeros((2, 512, 256), F32)
    group = group_ref[...]
    group = jnp.concatenate([group, group], 1)[None]
    for g in range(3):
        acc = lax.dot_general(
            l_ref[...], w_ref[g * 256 : g * 256 + 256, :], (((1,), (1,)), ((), ())), preferred_element_type=F32
        )
        total = jnp.where(group == g, acc.reshape(2, 512, 256), total)
    for b in range(2):
        part = total[:, :, b * 128 : b * 128 + 128]
        re = part[0].reshape(4, 8, 16, 128)
        im = part[1].reshape(4, 8, 16, 128)
        both = jnp.concatenate([re, im], 2).astype(BF16)
        out_ref[:, :, pl.ds(half if b == 0 else 1 - half, 1)] = both[:, :, None]


def form(*args):
    scratch = [pltpu.VMEM((1024, 1024), BF16), pltpu.VMEM((768, 1024), BF16)]
    return call(form_kernel, 10, jax.ShapeDtypeStruct((4, 8, 2, 32, 128), BF16), scratch)(*args)


def add_kernel(got_ref, out_ref):
    for side in range(2):
        parts = [got_ref[2 * src + side].astype(F32) for src in range(4)]
        for src in range(4, 32):
            parts[src % 4] = parts[src % 4] + got_ref[2 * src + side].astype(F32)
        total = (parts[0] + parts[1]) + (parts[2] + parts[3])
        for p in range(2):
            out_ref[side * 16 : side * 16 + 16, p, :] = total[p * 16 : p * 16 + 16]


def add(got):
    return pl.pallas_call(
        add_kernel,
        in_specs=[VM],
        out_specs=VM,
        out_shape=jax.ShapeDtypeStruct((32, 2, 128), F32),
        compiler_params=pltpu.CompilerParams(vmem_limit_bytes=LIMIT),
        name="add",
    )(got)


def shards(signals, weights, bin_group):
    half, core, low = lax.axis_index("xhi"), lax.axis_index("core"), lax.axis_index("xlo")
    ring = ("xlo", "xhi", "core")

    def exchange(value, flip):
        return lax.ppermute(value, ring, [(i, i ^ flip) for i in range(8)])

    ids = jnp.stack([core, half, low])
    blocks = weights.reshape(6, 128, 256)
    w1 = exchange(blocks, 4)
    w3 = exchange(blocks, 6)
    other = exchange(signals, 1)
    own, perm, table, coarse, fine, outer = prep(ids, pltpu.with_memory_space_constraint(signals, pltpu.HBM))

    spec0, xs, rest = dft_first(ids, other, own, perm, table, coarse, fine, outer)
    got0 = exchange(spec0, 2)
    spec1, spec2 = dft_next(ids, xs, rest, outer)
    got1 = exchange(spec1, 4)
    got2 = exchange(spec2, 6)
    w2a = exchange(w1[:3], 6)
    w2b = exchange(w3[3:], 4)
    same, group = dft_last(ids, xs, rest, outer, got0, bin_group.reshape(16, 128))
    same_sib = exchange(same, 1)
    cross = (got1.astype(F32) + got2.astype(F32)).astype(BF16)
    cross_sib = exchange(cross, 1)
    parts = form(ids, same, cross, same_sib, cross_sib, group, blocks, w1, w2a, w2b, w3)
    got = lax.all_to_all(parts.reshape(64, 32, 128), ("y", "z", "xhi"), 0, 0, tiled=True)
    return add(got)


def solution(mesh):
    fine = Mesh(mesh.devices.reshape(4, 2, 8, 2, 2), ("y", "xlo", "z", "xhi", "core"))
    chan, beam = ("y", "xlo", "z"), ("xhi", "core")
    in_specs = (P(chan, beam), P(None, None, beam, chan), P())
    out_specs = P(chan, None, beam)
    return jax.shard_map(shards, mesh=fine, in_specs=in_specs, out_specs=out_specs, check_vma=False)
```

```python
import math

import jax
import jax.numpy as jnp
from jax import lax
from jax.experimental import pallas as pl
from jax.experimental.pallas import tpu as pltpu
from jax.sharding import Mesh, PartitionSpec as P

F32 = jnp.float32
BF16 = jnp.bfloat16
I32 = jnp.int32

STRIDE = 8
SAMPLES = 8192
LIMIT = 16 * 1024 * 1024
UNROLL = 16


def root(numer, denom):
    angle = 2.0 * math.pi / denom * (numer & (denom - 1)).astype(F32)
    return jnp.cos(angle), -jnp.sin(angle)


def iota(shape, dim):
    return lax.broadcasted_iota(I32, shape, dim)


def deinterleave(x, perm):
    out = []
    rows = jnp.concatenate([x[:, :1024], x[:, 1024:]], 0)
    split = jnp.dot(rows, perm, preferred_element_type=F32).astype(BF16)
    for s in range(STRIDE):
        cols = split[:, s * 128 : (s + 1) * 128]
        out.append(jnp.concatenate([cols[:128], cols[128:]], 1))
    return out


def eighth(q):
    q = q & 7
    half = math.sqrt(0.5)
    odd = (q & 1) != 0
    re = jnp.where(odd, half, jnp.where((q & 2) != 0, 0.0, 1.0))
    re = jnp.where((q > 2) & (q < 6), -re, re)
    im = jnp.where(odd, half, jnp.where((q & 2) != 0, 1.0, 0.0))
    im = jnp.where(q < 4, -im, im)
    return re, im


def owner(ids_ref, slot):
    half, low = ids_ref[1], ids_ref[2]
    return (1 - half if slot in (0, 2) else half), (1 - low if slot in (1, 2) else low)


def block_of(t, low):
    return t // 8 * 16 + low * 8 + t % 8


def make_twiddles(ids_ref, slot, coarse_ref, fine_ref, t_ref, row0):
    half, low = owner(ids_ref, slot)
    first = pl.multiple_of(half * 16, 16)
    fr = fine_ref[0, pl.ds(first, 16), :]
    fi = fine_ref[1, pl.ds(first, 16), :]
    for t in range(16):
        k = block_of(t, low)
        cr = jnp.concatenate([coarse_ref[0, pl.ds(k, 1), :]] * 4, 1)
        ci = jnp.concatenate([coarse_ref[1, pl.ds(k, 1), :]] * 4, 1)
        row = row0 + t * 16
        t_ref[row : row + 16, :] = (cr * fr - ci * fi).astype(BF16)
        t_ref[row + 256 : row + 272, :] = (cr * fi + ci * fr).astype(BF16)


def prep_kernel(ids_ref, own_ref, xs_ref, perm_ref, t_ref, coarse_ref, fine_ref, outer_ref):
    core, half = ids_ref[0], ids_ref[1]
    row, lane = iota((32, 128), 0), iota((32, 128), 1)
    coarse_ref[0], coarse_ref[1] = root(row * lane, 32)
    br, bi = root((row + 1) * lane, 1024)
    for part in range(4):
        u = 2 * core + part if part < 2 else 2 * (1 - core) + part - 2
        er, ei = eighth((row + 1) * u)
        cols = slice(part * 128, part * 128 + 128)
        fine_ref[0, :, cols] = br * er - bi * ei
        fine_ref[1, :, cols] = br * ei + bi * er
    outer_ref[0], outer_ref[1] = root(row * 32, SAMPLES)
    outer_ref[2], outer_ref[3] = root(row + 1, SAMPLES)
    scale = 1.0 / math.sqrt(SAMPLES)
    outer_ref[4] = jnp.where((((row + 1) * half) & 1) != 0, -scale, scale)
    make_twiddles(ids_ref, 0, coarse_ref, fine_ref, t_ref, 0)
    same = jnp.where(iota((1024, 128), 0) // STRIDE == iota((1024, 128), 1), 1.0, 0.0).astype(BF16)
    phase = iota((16, 128), 0) & (STRIDE - 1)
    for s in range(STRIDE):
        keep = jnp.where(phase == s, 1.0, 0.0).astype(BF16)
        perm_ref[:, s * 128 : (s + 1) * 128] = (same.reshape(64, 16, 128) * keep[None]).reshape(1024, 128)
    for s, rows in enumerate(deinterleave(own_ref[...], perm_ref[...])):
        xs_ref[s * 128 : (s + 1) * 128, :] = rows


def prep(ids, signals):
    full = lambda *shape: pl.BlockSpec(shape, lambda i, ids: (0,) * len(shape))
    return pl.pallas_call(
        prep_kernel,
        grid_spec=pltpu.PrefetchScalarGridSpec(
            num_scalar_prefetch=1,
            grid=(1,),
            in_specs=[pl.BlockSpec((128, 2048), lambda i, ids: (ids[0], 0))],
            out_specs=[
                full(1024, 256),
                full(1024, 1024),
                full(512, 512),
                full(2, 32, 128),
                full(2, 32, 512),
                full(5, 32, 128),
            ],
        ),
        out_shape=[
            jax.ShapeDtypeStruct((1024, 256), BF16),
            jax.ShapeDtypeStruct((1024, 1024), BF16),
            jax.ShapeDtypeStruct((512, 512), BF16),
            jax.ShapeDtypeStruct((2, 32, 128), F32),
            jax.ShapeDtypeStruct((2, 32, 512), F32),
            jax.ShapeDtypeStruct((5, 32, 128), F32),
        ],
        compiler_params=pltpu.CompilerParams(vmem_limit_bytes=LIMIT),
        name="prep",
    )(ids, signals)


def times(w, x):
    return w[0] * x[0] - w[1] * x[1], w[0] * x[1] + w[1] * x[0]


def plus(x, y):
    return x[0] + y[0], x[1] + y[1]


def minus(x, y):
    return x[0] - y[0], x[1] - y[1]


def turned(x, y):
    return x[0] + y[1], x[1] - y[0]


def combine(ids_ref, slot, f_ref, outer_ref, out_ref):
    half, low = owner(ids_ref, slot)
    first = pl.multiple_of(half * 16, 16)
    fine = outer_ref[2, pl.ds(first, 16), :], outer_ref[3, pl.ds(first, 16), :]
    scale = outer_ref[4, pl.ds(first, 16), :]
    eighth_root = math.sqrt(0.5)

    def step(t, carry):
        row0 = pl.multiple_of(t * 16, 16)
        k = block_of(t, low)
        w = times((outer_ref[0, pl.ds(k, 1), :], outer_ref[1, pl.ds(k, 1), :]), fine)
        w2 = times(w, w)
        w4 = times(w2, w2)
        wt = eighth_root * (w[0] + w[1]), eighth_root * (w[1] - w[0])
        term = lambda s: (
            f_ref[pl.ds(row0, 16), s * 128 : (s + 1) * 128],
            f_ref[pl.ds(row0 + 256, 16), s * 128 : (s + 1) * 128],
        )
        sums = []
        for s in range(2):
            near, far = term(s), times(w4, term(s + 4))
            up, down = plus(near, far), minus(near, far)
            near, far = term(s + 2), times(w4, term(s + 6))
            sums.append(
                (plus(up, times(w2, plus(near, far))), turned(down, times(w2, minus(near, far))))
            )
        low_bin = plus(sums[0][0], times(w, sums[1][0]))
        high_bin = plus(sums[0][1], times(wt, sums[1][1]))
        for place, value in enumerate((low_bin[0], high_bin[0], low_bin[1], high_bin[1])):
            rows = pl.ds(row0 + 256 * place, 16)
            out_ref[rows, :] = (value * scale).astype(out_ref.dtype)
        return carry

    lax.fori_loop(0, 16, step, 0, unroll=UNROLL)


def spectrum(t_ref, row0, xs_ref, f_ref):
    f_ref[...] = lax.dot_general(
        t_ref[row0 : row0 + 512, :], xs_ref[...], (((1,), (1,)), ((), ())), preferred_element_type=F32
    )


def first_kernel(
    ids_ref, other_ref, own_ref, perm_ref, t_ref, coarse_ref, fine_ref, outer_ref, out_ref, xs_ref, rest_ref, f_ref
):
    xs_ref[:, 0:256] = own_ref[...]
    other = other_ref[pl.ds(pl.multiple_of(ids_ref[0] * 128, 128), 128), :]
    for s, rows in enumerate(deinterleave(other, perm_ref[...])):
        xs_ref[s * 128 : (s + 1) * 128, 256:512] = rows
    for slot in (1, 2, 3):
        make_twiddles(ids_ref, slot, coarse_ref, fine_ref, rest_ref, (slot - 1) * 512)
    spectrum(t_ref, 0, xs_ref, f_ref)
    combine(ids_ref, 0, f_ref, outer_ref, out_ref)


def next_kernel(ids_ref, xs_ref, rest_ref, outer_ref, out1_ref, out2_ref, f_ref):
    for index, out_ref in enumerate((out1_ref, out2_ref)):
        spectrum(rest_ref, index * 512, xs_ref, f_ref.at[index])
        combine(ids_ref, 1 + index, f_ref.at[index], outer_ref, out_ref)


def last_kernel(ids_ref, xs_ref, rest_ref, outer_ref, bins_ref, out_ref, group_ref, f_ref):
    spectrum(rest_ref, 1024, xs_ref, f_ref)
    half, low = ids_ref[1], ids_ref[2]
    row, lane = iota((512, 128), 0), iota((512, 128), 1)
    line = jnp.where(lane == (row // 128 * 4 + low * 2 + row // 64 % 2), 1.0, 0.0).astype(BF16)[:, :16]
    lines = jnp.dot(line, bins_ref[...].astype(F32).astype(BF16), preferred_element_type=F32)
    place = row // 16 % 4 * 32 + half * 16 + row % 16
    chosen = jnp.where(lane == place, lines, 0.0).astype(BF16)
    group_ref[...] = jnp.dot(chosen, jnp.ones((128, 128), BF16), preferred_element_type=F32)
    combine(ids_ref, 3, f_ref, outer_ref, out_ref)


VM = pl.BlockSpec(memory_space=pltpu.VMEM)


SM = pl.BlockSpec(memory_space=pltpu.SMEM)
PIECE = jax.ShapeDtypeStruct((1024, 128), BF16)


def call(kernel, count, out_shape, scratch, alias={}):
    outs = len(out_shape) if isinstance(out_shape, list) else 0
    return pl.pallas_call(
        kernel,
        in_specs=[SM] + [VM] * count,
        out_specs=[VM] * outs if outs else VM,
        out_shape=out_shape,
        scratch_shapes=scratch,
        input_output_aliases=alias,
        compiler_params=pltpu.CompilerParams(vmem_limit_bytes=LIMIT),
    )


def dft_first(*args):
    outs = [PIECE, jax.ShapeDtypeStruct((1024, 512), BF16), jax.ShapeDtypeStruct((1536, 512), BF16)]
    return call(first_kernel, 7, outs, [pltpu.VMEM((512, 1024), F32)])(*args)


def dft_next(*args):
    return call(next_kernel, 3, [PIECE, PIECE], [pltpu.VMEM((2, 512, 1024), F32)])(*args)


def dft_last(*args):
    outs = [jax.ShapeDtypeStruct((1024, 128), F32), jax.ShapeDtypeStruct((512, 128), F32)]
    return call(last_kernel, 4, outs, [pltpu.VMEM((512, 1024), F32)])(*args)


def form_beams(side, l_ref, w_ref, group_ref, out_ref):
    acc = lax.dot_general(l_ref[...], w_ref[...], (((1,), (1,)), ((), ())), preferred_element_type=F32)
    acc = acc.reshape(2, 512, 384)
    group = group_ref[...][None]
    total = jnp.where(group == 0, acc[:, :, 0:128], jnp.where(group == 1, acc[:, :, 128:256], acc[:, :, 256:384]))
    re = total[0].reshape(4, 8, 16, 128)
    im = total[1].reshape(4, 8, 16, 128)
    out_ref[:, :, pl.ds(side, 1)] = jnp.concatenate([re, im], 2).astype(BF16)[:, :, None]


def near_kernel(ids_ref, s0_ref, s1_ref, p0_ref, p1_ref, group_ref, w0_ref, w1_ref, out_ref, l_ref, w_ref):
    core, half = ids_ref[0], ids_ref[1]
    for srcs, place in (((s0_ref, s1_ref), core), ((p0_ref, p1_ref), 1 - core)):
        for xl in range(2):
            lane0 = pl.multiple_of(xl * 256 + place * 128, 128)
            for r in range(0, 512, 64):
                sr, si = srcs[xl][r : r + 64, :], srcs[xl][512 + r : 576 + r, :]
                l_ref[r : r + 64, pl.ds(lane0, 128)] = sr
                l_ref[r : r + 64, pl.ds(lane0 + 512, 128)] = -si
                l_ref[512 + r : 576 + r, pl.ds(lane0, 128)] = si
                l_ref[512 + r : 576 + r, pl.ds(lane0 + 512, 128)] = sr
    for i in range(6):
        row, col = i // 2 * 128, i % 2 * 512
        w_ref[row : row + 128, col : col + 256] = w0_ref[i]
        w_ref[row : row + 128, col + 256 : col + 512] = w1_ref[i]
    form_beams(half, l_ref, w_ref, group_ref, out_ref)


def far_kernel(ids_ref, l_ref, group_ref, w2a_ref, w2b_ref, w3_ref, begun_ref, out_ref, w_ref):
    for i in range(6):
        row, col = i // 2 * 128, i % 2 * 512
        w_ref[row : row + 128, col : col + 256] = w2a_ref[i] if i < 3 else w2b_ref[i - 3]
        w_ref[row : row + 128, col + 256 : col + 512] = w3_ref[i]
    form_beams(1 - ids_ref[1], l_ref, w_ref, group_ref, out_ref)


PARTS = jax.ShapeDtypeStruct((4, 8, 2, 32, 128), BF16)


def form_near(*args):
    outs = [PARTS, jax.ShapeDtypeStruct((1024, 1024), BF16)]
    return call(near_kernel, 7, outs, [pltpu.VMEM((384, 1024), BF16)])(*args)


def form_far(*args):
    return call(far_kernel, 6, PARTS, [pltpu.VMEM((384, 1024), BF16)], {6: 0})(*args)


def add_kernel(got_ref, out_ref):
    for side in range(2):
        parts = [got_ref[2 * src + side].astype(F32) for src in range(4)]
        for src in range(4, 32):
            parts[src % 4] = parts[src % 4] + got_ref[2 * src + side].astype(F32)
        total = (parts[0] + parts[1]) + (parts[2] + parts[3])
        for p in range(2):
            out_ref[side * 16 : side * 16 + 16, p, :] = total[p * 16 : p * 16 + 16]


def add(got):
    return pl.pallas_call(
        add_kernel,
        in_specs=[VM],
        out_specs=VM,
        out_shape=jax.ShapeDtypeStruct((32, 2, 128), F32),
        compiler_params=pltpu.CompilerParams(vmem_limit_bytes=LIMIT),
        name="add",
    )(got)


def shards(signals, weights, bin_group):
    half, core, low = lax.axis_index("xhi"), lax.axis_index("core"), lax.axis_index("xlo")
    ring = ("xlo", "xhi", "core")

    def exchange(value, flip):
        return lax.ppermute(value, ring, [(i, i ^ flip) for i in range(8)])

    ids = jnp.stack([core, half, low])
    blocks = weights.reshape(6, 128, 256)
    w1 = exchange(blocks, 4)
    w3 = exchange(blocks, 6)
    other = exchange(signals, 1)
    own, perm, table, coarse, fine, outer = prep(ids, pltpu.with_memory_space_constraint(signals, pltpu.HBM))

    spec0, xs, rest = dft_first(ids, other, own, perm, table, coarse, fine, outer)
    got0 = exchange(spec0, 2)
    spec1, spec2 = dft_next(ids, xs, rest, outer)
    got1 = exchange(spec1, 4)
    got2 = exchange(spec2, 6)
    mine, group = dft_last(ids, xs, rest, outer, bin_group.reshape(16, 128))
    w2a = exchange(w1[:3], 6)
    w2b = exchange(w3[3:], 4)
    same = (mine + got0.astype(F32)).astype(BF16)
    same_sib = exchange(same, 1)
    cross = (got1.astype(F32) + got2.astype(F32)).astype(BF16)
    cross_sib = exchange(cross, 1)
    begun, lhs = form_near(ids, same, cross, same_sib, cross_sib, group, blocks, w1)
    parts = form_far(ids, lhs, group, w2a, w2b, w3, begun)
    got = lax.all_to_all(parts.reshape(64, 32, 128), ("y", "z", "xhi"), 0, 0, tiled=True)
    return add(got)


def solution(mesh):
    fine = Mesh(mesh.devices.reshape(4, 2, 8, 2, 2), ("y", "xlo", "z", "xhi", "core"))
    chan, beam = ("y", "xlo", "z"), ("xhi", "core")
    in_specs = (P(chan, beam), P(None, None, beam, chan), P())
    out_specs = P(chan, None, beam)
    return jax.shard_map(shards, mesh=fine, in_specs=in_specs, out_specs=out_specs, check_vma=False)
```

```python
import math

import jax
import jax.numpy as jnp
from jax import lax
from jax.experimental import pallas as pl
from jax.experimental.pallas import tpu as pltpu
from jax.sharding import Mesh, PartitionSpec as P

F32 = jnp.float32
BF16 = jnp.bfloat16
I32 = jnp.int32

STRIDE = 8
SAMPLES = 8192
LIMIT = 16 * 1024 * 1024
UNROLL = 16


def root(numer, denom):
    angle = 2.0 * math.pi / denom * (numer & (denom - 1)).astype(F32)
    return jnp.cos(angle), -jnp.sin(angle)


def iota(shape, dim):
    return lax.broadcasted_iota(I32, shape, dim)


def deinterleave(x, perm):
    out = []
    rows = jnp.concatenate([x[:, :1024], x[:, 1024:]], 0)
    split = jnp.dot(rows, perm, preferred_element_type=F32).astype(BF16)
    for s in range(STRIDE):
        cols = split[:, s * 128 : (s + 1) * 128]
        out.append(jnp.concatenate([cols[:128], cols[128:]], 1))
    return out


def eighth(q):
    q = q & 7
    half = math.sqrt(0.5)
    odd = (q & 1) != 0
    re = jnp.where(odd, half, jnp.where((q & 2) != 0, 0.0, 1.0))
    re = jnp.where((q > 2) & (q < 6), -re, re)
    im = jnp.where(odd, half, jnp.where((q & 2) != 0, 1.0, 0.0))
    im = jnp.where(q < 4, -im, im)
    return re, im


def owner(ids_ref, slot):
    half, low = ids_ref[1], ids_ref[2]
    return (1 - half if slot in (0, 2) else half), (1 - low if slot in (1, 2) else low)


def block_of(t, low):
    return t // 8 * 16 + low * 8 + t % 8


def make_twiddles(ids_ref, slot, coarse_ref, fine_ref, t_ref, row0):
    half, low = owner(ids_ref, slot)
    first = pl.multiple_of(half * 16, 16)
    fr = fine_ref[0, pl.ds(first, 16), :]
    fi = fine_ref[1, pl.ds(first, 16), :]
    for t in range(16):
        k = block_of(t, low)
        cr = jnp.concatenate([coarse_ref[0, pl.ds(k, 1), :]] * 4, 1)
        ci = jnp.concatenate([coarse_ref[1, pl.ds(k, 1), :]] * 4, 1)
        row = row0 + t * 16
        t_ref[row : row + 16, :] = (cr * fr - ci * fi).astype(BF16)
        t_ref[row + 256 : row + 272, :] = (cr * fi + ci * fr).astype(BF16)


def prep_kernel(ids_ref, own_ref, xs_ref, perm_ref, t_ref, coarse_ref, fine_ref, outer_ref):
    core, half = ids_ref[0], ids_ref[1]
    row, lane = iota((32, 128), 0), iota((32, 128), 1)
    coarse_ref[0], coarse_ref[1] = root(row * lane, 32)
    br, bi = root((row + 1) * lane, 1024)
    for part in range(4):
        u = 2 * core + part if part < 2 else 2 * (1 - core) + part - 2
        er, ei = eighth((row + 1) * u)
        cols = slice(part * 128, part * 128 + 128)
        fine_ref[0, :, cols] = br * er - bi * ei
        fine_ref[1, :, cols] = br * ei + bi * er
    outer_ref[0], outer_ref[1] = root(row * 32, SAMPLES)
    outer_ref[2], outer_ref[3] = root(row + 1, SAMPLES)
    scale = 1.0 / math.sqrt(SAMPLES)
    outer_ref[4] = jnp.where((((row + 1) * half) & 1) != 0, -scale, scale)
    make_twiddles(ids_ref, 0, coarse_ref, fine_ref, t_ref, 0)
    same = jnp.where(iota((1024, 128), 0) // STRIDE == iota((1024, 128), 1), 1.0, 0.0).astype(BF16)
    phase = iota((16, 128), 0) & (STRIDE - 1)
    for s in range(STRIDE):
        keep = jnp.where(phase == s, 1.0, 0.0).astype(BF16)
        perm_ref[:, s * 128 : (s + 1) * 128] = (same.reshape(64, 16, 128) * keep[None]).reshape(1024, 128)
    for s, rows in enumerate(deinterleave(own_ref[...], perm_ref[...])):
        xs_ref[s * 128 : (s + 1) * 128, :] = rows


def prep(ids, signals):
    full = lambda *shape: pl.BlockSpec(shape, lambda i, ids: (0,) * len(shape))
    return pl.pallas_call(
        prep_kernel,
        grid_spec=pltpu.PrefetchScalarGridSpec(
            num_scalar_prefetch=1,
            grid=(1,),
            in_specs=[pl.BlockSpec((128, 2048), lambda i, ids: (ids[0], 0))],
            out_specs=[
                full(1024, 256),
                full(1024, 1024),
                full(512, 512),
                full(2, 32, 128),
                full(2, 32, 512),
                full(5, 32, 128),
            ],
        ),
        out_shape=[
            jax.ShapeDtypeStruct((1024, 256), BF16),
            jax.ShapeDtypeStruct((1024, 1024), BF16),
            jax.ShapeDtypeStruct((512, 512), BF16),
            jax.ShapeDtypeStruct((2, 32, 128), F32),
            jax.ShapeDtypeStruct((2, 32, 512), F32),
            jax.ShapeDtypeStruct((5, 32, 128), F32),
        ],
        compiler_params=pltpu.CompilerParams(vmem_limit_bytes=LIMIT),
        name="prep",
    )(ids, signals)


def times(w, x):
    return w[0] * x[0] - w[1] * x[1], w[0] * x[1] + w[1] * x[0]


def plus(x, y):
    return x[0] + y[0], x[1] + y[1]


def minus(x, y):
    return x[0] - y[0], x[1] - y[1]


def turned(x, y):
    return x[0] + y[1], x[1] - y[0]


def combine(ids_ref, slot, f_ref, outer_ref, out_ref):
    half, low = owner(ids_ref, slot)
    first = pl.multiple_of(half * 16, 16)
    fine = outer_ref[2, pl.ds(first, 16), :], outer_ref[3, pl.ds(first, 16), :]
    scale = outer_ref[4, pl.ds(first, 16), :]
    eighth_root = math.sqrt(0.5)

    def step(t, carry):
        row0 = pl.multiple_of(t * 16, 16)
        k = block_of(t, low)
        w = times((outer_ref[0, pl.ds(k, 1), :], outer_ref[1, pl.ds(k, 1), :]), fine)
        w2 = times(w, w)
        w4 = times(w2, w2)
        wt = eighth_root * (w[0] + w[1]), eighth_root * (w[1] - w[0])
        term = lambda s: (
            f_ref[pl.ds(row0, 16), s * 128 : (s + 1) * 128],
            f_ref[pl.ds(row0 + 256, 16), s * 128 : (s + 1) * 128],
        )
        sums = []
        for s in range(2):
            near, far = term(s), times(w4, term(s + 4))
            up, down = plus(near, far), minus(near, far)
            near, far = term(s + 2), times(w4, term(s + 6))
            sums.append(
                (plus(up, times(w2, plus(near, far))), turned(down, times(w2, minus(near, far))))
            )
        low_bin = plus(sums[0][0], times(w, sums[1][0]))
        high_bin = plus(sums[0][1], times(wt, sums[1][1]))
        for place, value in enumerate((low_bin[0], high_bin[0], low_bin[1], high_bin[1])):
            rows = pl.ds(row0 + 256 * place, 16)
            out_ref[rows, :] = (value * scale).astype(out_ref.dtype)
        return carry

    lax.fori_loop(0, 16, step, 0, unroll=UNROLL)


def spectrum(t_ref, row0, xs_ref, f_ref):
    f_ref[...] = lax.dot_general(
        t_ref[row0 : row0 + 512, :], xs_ref[...], (((1,), (1,)), ((), ())), preferred_element_type=F32
    )


def first_kernel(
    ids_ref, other_ref, own_ref, perm_ref, t_ref, coarse_ref, fine_ref, outer_ref, out_ref, xs_ref, rest_ref, f_ref
):
    xs_ref[:, 0:256] = own_ref[...]
    other = other_ref[pl.ds(pl.multiple_of(ids_ref[0] * 128, 128), 128), :]
    for s, rows in enumerate(deinterleave(other, perm_ref[...])):
        xs_ref[s * 128 : (s + 1) * 128, 256:512] = rows
    for slot in (1, 2, 3):
        make_twiddles(ids_ref, slot, coarse_ref, fine_ref, rest_ref, (slot - 1) * 512)
    spectrum(t_ref, 0, xs_ref, f_ref)
    combine(ids_ref, 0, f_ref, outer_ref, out_ref)


def next_kernel(ids_ref, xs_ref, rest_ref, outer_ref, out1_ref, out2_ref, f_ref):
    for index, out_ref in enumerate((out1_ref, out2_ref)):
        spectrum(rest_ref, index * 512, xs_ref, f_ref.at[index])
        combine(ids_ref, 1 + index, f_ref.at[index], outer_ref, out_ref)


def last_kernel(ids_ref, xs_ref, rest_ref, outer_ref, bins_ref, out_ref, group_ref, f_ref):
    spectrum(rest_ref, 1024, xs_ref, f_ref)
    half, low = ids_ref[1], ids_ref[2]
    row, lane = iota((512, 128), 0), iota((512, 128), 1)
    line = jnp.where(lane == (row // 128 * 4 + low * 2 + row // 64 % 2), 1.0, 0.0).astype(BF16)[:, :16]
    lines = jnp.dot(line, bins_ref[...].astype(F32).astype(BF16), preferred_element_type=F32)
    place = row // 16 % 4 * 32 + half * 16 + row % 16
    chosen = jnp.where(lane == place, lines, 0.0).astype(BF16)
    group_ref[...] = jnp.dot(chosen, jnp.ones((128, 128), BF16), preferred_element_type=F32)
    combine(ids_ref, 3, f_ref, outer_ref, out_ref)


VM = pl.BlockSpec(memory_space=pltpu.VMEM)


SM = pl.BlockSpec(memory_space=pltpu.SMEM)
PIECE = jax.ShapeDtypeStruct((1024, 128), BF16)


def call(kernel, count, out_shape, scratch, alias={}):
    outs = len(out_shape) if isinstance(out_shape, list) else 0
    return pl.pallas_call(
        kernel,
        in_specs=[SM] + [VM] * count,
        out_specs=[VM] * outs if outs else VM,
        out_shape=out_shape,
        scratch_shapes=scratch,
        input_output_aliases=alias,
        compiler_params=pltpu.CompilerParams(vmem_limit_bytes=LIMIT),
    )


def dft_first(*args):
    outs = [PIECE, jax.ShapeDtypeStruct((1024, 512), BF16), jax.ShapeDtypeStruct((1536, 512), BF16)]
    return call(first_kernel, 7, outs, [pltpu.VMEM((512, 1024), F32)])(*args)


def dft_next(*args):
    return call(next_kernel, 3, [PIECE, PIECE], [pltpu.VMEM((2, 512, 1024), F32)])(*args)


def dft_last(*args):
    outs = [jax.ShapeDtypeStruct((1024, 128), F32), jax.ShapeDtypeStruct((512, 128), F32)]
    return call(last_kernel, 4, outs, [pltpu.VMEM((512, 1024), F32)])(*args)


def product(lhs, weights):
    return lax.dot_general(lhs, weights, (((1,), (1,)), ((), ())), preferred_element_type=F32)


def store_beams(side, acc, group_ref, out_ref):
    acc = acc.reshape(2, 512, 384)
    group = group_ref[...][None]
    total = jnp.where(group == 0, acc[:, :, 0:128], jnp.where(group == 1, acc[:, :, 128:256], acc[:, :, 256:384]))
    re = total[0].reshape(4, 8, 16, 128)
    im = total[1].reshape(4, 8, 16, 128)
    both = jnp.concatenate([re, im], 2).astype(BF16)
    for y in range(4):
        out_ref[:, pl.ds(side, 1), y] = both[y][:, None]


def place_rows(l_ref, xl, src):
    for r in range(0, 512, 64):
        sr, si = src[r : r + 64, :], src[512 + r : 576 + r, :]
        c0, c1 = slice(xl * 256, xl * 256 + 128), slice(xl * 256 + 128, xl * 256 + 256)
        l_ref[r : r + 64, c0] = sr
        l_ref[r : r + 64, c1] = -si
        l_ref[512 + r : 576 + r, c0] = si
        l_ref[512 + r : 576 + r, c1] = sr


def place_weights(core, w_ref, col, blocks):
    for which in range(2):
        lane0 = pl.multiple_of((core if which == 0 else 1 - core) * 128, 128)
        for i in range(6):
            row, at = i // 2 * 128, col + i % 2 * 128
            w_ref[which, row : row + 128, at : at + 128] = blocks[i][:, pl.ds(lane0, 128)]


def pack_kernel(ids_ref, w0_ref, w1_ref, w3_ref, near_ref, side_ref):
    place_weights(ids_ref[0], near_ref, 0, [w0_ref.at[i] for i in range(6)])
    place_weights(ids_ref[0], near_ref, 256, [w1_ref.at[i] for i in range(6)])
    place_weights(ids_ref[0], side_ref, 0, [w3_ref.at[i] for i in range(6)])


def own_kernel(ids_ref, same_ref, cross_ref, near_ref, l_ref, acc_ref):
    place_rows(l_ref, 0, same_ref)
    place_rows(l_ref, 1, cross_ref)
    acc_ref[...] = product(l_ref[...], near_ref[0])


def sib_kernel(ids_ref, same_ref, cross_ref, near_ref, side_ref, own_ref, acc_ref, group_ref, out_ref, l_ref, far_ref):
    place_rows(l_ref, 0, same_ref)
    place_rows(l_ref, 1, cross_ref)
    store_beams(ids_ref[1], acc_ref[...] + product(l_ref[...], near_ref[1]), group_ref, out_ref)
    far_ref[...] = product(own_ref[:, 256:512], side_ref[0]) + product(l_ref[:, 256:512], side_ref[1])


def far_kernel(ids_ref, own_ref, sib_ref, acc_ref, group_ref, w2a_ref, w2b_ref, begun_ref, out_ref, w_ref):
    place_weights(ids_ref[0], w_ref, 0, [w2a_ref.at[i] for i in range(3)] + [w2b_ref.at[i] for i in range(3)])
    acc = acc_ref[...] + product(own_ref[:, 0:256], w_ref[0]) + product(sib_ref[:, 0:256], w_ref[1])
    store_beams(1 - ids_ref[1], acc, group_ref, out_ref)


PARTS = jax.ShapeDtypeStruct((8, 2, 4, 32, 128), BF16)
ROWS = jax.ShapeDtypeStruct((1024, 512), BF16)
SUMS = jax.ShapeDtypeStruct((1024, 384), F32)


def pack(*args):
    outs = [jax.ShapeDtypeStruct((2, 384, 512), BF16), jax.ShapeDtypeStruct((2, 384, 256), BF16)]
    return call(pack_kernel, 3, outs, [])(*args)


def form_own(*args):
    return call(own_kernel, 3, [ROWS, SUMS], [])(*args)


def form_sib(*args):
    return call(sib_kernel, 7, [PARTS, ROWS, SUMS], [])(*args)


def form_far(*args):
    return call(far_kernel, 7, PARTS, [pltpu.VMEM((2, 384, 256), BF16)], {7: 0})(*args)


def add_kernel(got_ref, out_ref):
    for side in range(2):
        sources = [(z * 2 + side) * 4 + y for z in range(8) for y in range(4)]
        parts = [got_ref[src].astype(F32) for src in sources[:4]]
        for place, src in enumerate(sources[4:]):
            parts[place % 4] = parts[place % 4] + got_ref[src].astype(F32)
        total = (parts[0] + parts[1]) + (parts[2] + parts[3])
        for p in range(2):
            out_ref[side * 16 : side * 16 + 16, p, :] = total[p * 16 : p * 16 + 16]


def add(got):
    return pl.pallas_call(
        add_kernel,
        in_specs=[VM],
        out_specs=VM,
        out_shape=jax.ShapeDtypeStruct((32, 2, 128), F32),
        compiler_params=pltpu.CompilerParams(vmem_limit_bytes=LIMIT),
        name="add",
    )(got)


def shards(signals, weights, bin_group):
    half, core, low = lax.axis_index("xhi"), lax.axis_index("core"), lax.axis_index("xlo")
    ring = ("xlo", "xhi", "core")

    def exchange(value, flip):
        return lax.ppermute(value, ring, [(i, i ^ flip) for i in range(8)])

    ids = jnp.stack([core, half, low])
    blocks = weights.reshape(6, 128, 256)
    w1 = exchange(blocks, 4)
    w3 = exchange(blocks, 6)
    other = exchange(signals, 1)
    own, perm, table, coarse, fine, outer = prep(ids, pltpu.with_memory_space_constraint(signals, pltpu.HBM))

    spec0, xs, rest = dft_first(ids, other, own, perm, table, coarse, fine, outer)
    got0 = exchange(spec0, 2)
    spec1, spec2 = dft_next(ids, xs, rest, outer)
    got1 = exchange(spec1, 4)
    got2 = exchange(spec2, 6)
    mine, group = dft_last(ids, xs, rest, outer, bin_group.reshape(16, 128))
    same = (mine + got0.astype(F32)).astype(BF16)
    same_sib = exchange(same, 1)
    w2a = exchange(w1[:3], 6)
    w2b = exchange(w3[3:], 4)
    near, side = pack(ids, blocks, w1, w3)
    cross = (got1.astype(F32) + got2.astype(F32)).astype(BF16)
    cross_sib = exchange(cross, 1)
    lhs, acc = form_own(ids, same, cross, near)
    begun, lhs_sib, acc_far = form_sib(ids, same_sib, cross_sib, near, side, lhs, acc, group)
    parts = form_far(ids, lhs, lhs_sib, acc_far, group, w2a, w2b, begun)
    got = lax.all_to_all(parts.reshape(64, 32, 128), ("z", "xhi", "y"), 0, 0, tiled=True)
    return add(got)


def solution(mesh):
    fine = Mesh(mesh.devices.reshape(4, 2, 8, 2, 2), ("y", "xlo", "z", "xhi", "core"))
    chan, beam = ("y", "xlo", "z"), ("xhi", "core")
    in_specs = (P(chan, beam), P(None, None, beam, chan), P())
    out_specs = P(chan, None, beam)
    return jax.shard_map(shards, mesh=fine, in_specs=in_specs, out_specs=out_specs, check_vma=False)
```

```python
import math

import jax
import jax.numpy as jnp
from jax import lax
from jax.experimental import pallas as pl
from jax.experimental.pallas import tpu as pltpu
from jax.sharding import Mesh, PartitionSpec as P

F32 = jnp.float32
BF16 = jnp.bfloat16
I32 = jnp.int32

STRIDE = 8
SAMPLES = 8192
LIMIT = 16 * 1024 * 1024
UNROLL = 16


def root(numer, denom):
    angle = 2.0 * math.pi / denom * (numer & (denom - 1)).astype(F32)
    return jnp.cos(angle), -jnp.sin(angle)


def iota(shape, dim):
    return lax.broadcasted_iota(I32, shape, dim)


def deinterleave(x, perm):
    out = []
    rows = jnp.concatenate([x[:, :1024], x[:, 1024:]], 0)
    split = jnp.dot(rows, perm, preferred_element_type=F32).astype(BF16)
    for s in range(STRIDE):
        cols = split[:, s * 128 : (s + 1) * 128]
        out.append(jnp.concatenate([cols[:128], cols[128:]], 1))
    return out


def eighth(q):
    q = q & 7
    half = math.sqrt(0.5)
    odd = (q & 1) != 0
    re = jnp.where(odd, half, jnp.where((q & 2) != 0, 0.0, 1.0))
    re = jnp.where((q > 2) & (q < 6), -re, re)
    im = jnp.where(odd, half, jnp.where((q & 2) != 0, 1.0, 0.0))
    im = jnp.where(q < 4, -im, im)
    return re, im


def owner(ids_ref, slot):
    half, low = ids_ref[1], ids_ref[2]
    return (1 - half if slot in (0, 2) else half), (1 - low if slot in (1, 2) else low)


def block_of(t, low):
    return t // 8 * 16 + low * 8 + t % 8


def make_twiddles(ids_ref, slot, coarse_ref, fine_ref, t_ref, row0):
    half, low = owner(ids_ref, slot)
    first = pl.multiple_of(half * 16, 16)
    fr = fine_ref[0, pl.ds(first, 16), :]
    fi = fine_ref[1, pl.ds(first, 16), :]
    for t in range(16):
        k = block_of(t, low)
        cr = jnp.concatenate([coarse_ref[0, pl.ds(k, 1), :]] * 4, 1)
        ci = jnp.concatenate([coarse_ref[1, pl.ds(k, 1), :]] * 4, 1)
        row = row0 + t * 16
        t_ref[row : row + 16, :] = (cr * fr - ci * fi).astype(BF16)
        t_ref[row + 256 : row + 272, :] = (cr * fi + ci * fr).astype(BF16)


def prep_kernel(ids_ref, own_ref, xs_ref, perm_ref, t_ref, coarse_ref, fine_ref, outer_ref):
    core, half = ids_ref[0], ids_ref[1]
    row, lane = iota((32, 128), 0), iota((32, 128), 1)
    coarse_ref[0], coarse_ref[1] = root(row * lane, 32)
    br, bi = root((row + 1) * lane, 1024)
    for part in range(4):
        u = 2 * core + part if part < 2 else 2 * (1 - core) + part - 2
        er, ei = eighth((row + 1) * u)
        cols = slice(part * 128, part * 128 + 128)
        fine_ref[0, :, cols] = br * er - bi * ei
        fine_ref[1, :, cols] = br * ei + bi * er
    outer_ref[0], outer_ref[1] = root(row * 32, SAMPLES)
    outer_ref[2], outer_ref[3] = root(row + 1, SAMPLES)
    scale = 1.0 / math.sqrt(SAMPLES)
    outer_ref[4] = jnp.where((((row + 1) * half) & 1) != 0, -scale, scale)
    make_twiddles(ids_ref, 0, coarse_ref, fine_ref, t_ref, 0)
    same = jnp.where(iota((1024, 128), 0) // STRIDE == iota((1024, 128), 1), 1.0, 0.0).astype(BF16)
    phase = iota((16, 128), 0) & (STRIDE - 1)
    for s in range(STRIDE):
        keep = jnp.where(phase == s, 1.0, 0.0).astype(BF16)
        perm_ref[:, s * 128 : (s + 1) * 128] = (same.reshape(64, 16, 128) * keep[None]).reshape(1024, 128)
    for s, rows in enumerate(deinterleave(own_ref[...], perm_ref[...])):
        xs_ref[s * 128 : (s + 1) * 128, :] = rows


def prep(ids, signals):
    full = lambda *shape: pl.BlockSpec(shape, lambda i, ids: (0,) * len(shape))
    return pl.pallas_call(
        prep_kernel,
        grid_spec=pltpu.PrefetchScalarGridSpec(
            num_scalar_prefetch=1,
            grid=(1,),
            in_specs=[pl.BlockSpec((128, 2048), lambda i, ids: (ids[0], 0))],
            out_specs=[
                full(1024, 256),
                full(1024, 1024),
                full(512, 512),
                full(2, 32, 128),
                full(2, 32, 512),
                full(5, 32, 128),
            ],
        ),
        out_shape=[
            jax.ShapeDtypeStruct((1024, 256), BF16),
            jax.ShapeDtypeStruct((1024, 1024), BF16),
            jax.ShapeDtypeStruct((512, 512), BF16),
            jax.ShapeDtypeStruct((2, 32, 128), F32),
            jax.ShapeDtypeStruct((2, 32, 512), F32),
            jax.ShapeDtypeStruct((5, 32, 128), F32),
        ],
        compiler_params=pltpu.CompilerParams(vmem_limit_bytes=LIMIT),
        name="prep",
    )(ids, signals)


def times(w, x):
    return w[0] * x[0] - w[1] * x[1], w[0] * x[1] + w[1] * x[0]


def plus(x, y):
    return x[0] + y[0], x[1] + y[1]


def minus(x, y):
    return x[0] - y[0], x[1] - y[1]


def turned(x, y):
    return x[0] + y[1], x[1] - y[0]


def combine(ids_ref, slot, f_ref, outer_ref, out_ref):
    half, low = owner(ids_ref, slot)
    first = pl.multiple_of(half * 16, 16)
    fine = outer_ref[2, pl.ds(first, 16), :], outer_ref[3, pl.ds(first, 16), :]
    scale = outer_ref[4, pl.ds(first, 16), :]
    eighth_root = math.sqrt(0.5)

    def step(t, carry):
        row0 = pl.multiple_of(t * 16, 16)
        k = block_of(t, low)
        w = times((outer_ref[0, pl.ds(k, 1), :], outer_ref[1, pl.ds(k, 1), :]), fine)
        w2 = times(w, w)
        w4 = times(w2, w2)
        wt = eighth_root * (w[0] + w[1]), eighth_root * (w[1] - w[0])
        term = lambda s: (
            f_ref[pl.ds(row0, 16), s * 128 : (s + 1) * 128],
            f_ref[pl.ds(row0 + 256, 16), s * 128 : (s + 1) * 128],
        )
        sums = []
        for s in range(2):
            near, far = term(s), times(w4, term(s + 4))
            up, down = plus(near, far), minus(near, far)
            near, far = term(s + 2), times(w4, term(s + 6))
            sums.append(
                (plus(up, times(w2, plus(near, far))), turned(down, times(w2, minus(near, far))))
            )
        low_bin = plus(sums[0][0], times(w, sums[1][0]))
        high_bin = plus(sums[0][1], times(wt, sums[1][1]))
        for place, value in enumerate((low_bin[0], high_bin[0], low_bin[1], high_bin[1])):
            rows = pl.ds(row0 + 256 * place, 16)
            out_ref[rows, :] = (value * scale).astype(out_ref.dtype)
        return carry

    lax.fori_loop(0, 16, step, 0, unroll=UNROLL)


def spectrum(t_ref, row0, xs_ref, f_ref):
    f_ref[...] = lax.dot_general(
        t_ref[row0 : row0 + 512, :], xs_ref[...], (((1,), (1,)), ((), ())), preferred_element_type=F32
    )


def first_kernel(
    ids_ref, other_ref, own_ref, perm_ref, t_ref, coarse_ref, fine_ref, outer_ref, out_ref, xs_ref, rest_ref, f_ref
):
    xs_ref[:, 0:256] = own_ref[...]
    other = other_ref[pl.ds(pl.multiple_of(ids_ref[0] * 128, 128), 128), :]
    for s, rows in enumerate(deinterleave(other, perm_ref[...])):
        xs_ref[s * 128 : (s + 1) * 128, 256:512] = rows
    for slot in (1, 2, 3):
        make_twiddles(ids_ref, slot, coarse_ref, fine_ref, rest_ref, (slot - 1) * 512)
    spectrum(t_ref, 0, xs_ref, f_ref)
    combine(ids_ref, 0, f_ref, outer_ref, out_ref)


def next_kernel(ids_ref, xs_ref, rest_ref, outer_ref, out1_ref, out2_ref, f_ref):
    for index, out_ref in enumerate((out1_ref, out2_ref)):
        spectrum(rest_ref, index * 512, xs_ref, f_ref.at[index])
        combine(ids_ref, 1 + index, f_ref.at[index], outer_ref, out_ref)


def last_kernel(ids_ref, xs_ref, rest_ref, outer_ref, bins_ref, out_ref, group_ref, f_ref):
    spectrum(rest_ref, 1024, xs_ref, f_ref)
    half, low = ids_ref[1], ids_ref[2]
    row, lane = iota((512, 128), 0), iota((512, 128), 1)
    line = jnp.where(lane == (row // 128 * 4 + low * 2 + row // 64 % 2), 1.0, 0.0).astype(BF16)[:, :16]
    lines = jnp.dot(line, bins_ref[...].astype(F32).astype(BF16), preferred_element_type=F32)
    place = row // 16 % 4 * 32 + half * 16 + row % 16
    chosen = jnp.where(lane == place, lines, 0.0).astype(BF16)
    group_ref[...] = jnp.dot(chosen, jnp.ones((128, 128), BF16), preferred_element_type=F32)
    combine(ids_ref, 3, f_ref, outer_ref, out_ref)


VM = pl.BlockSpec(memory_space=pltpu.VMEM)


SM = pl.BlockSpec(memory_space=pltpu.SMEM)
PIECE = jax.ShapeDtypeStruct((1024, 128), BF16)


def call(kernel, count, out_shape, scratch, alias={}):
    outs = len(out_shape) if isinstance(out_shape, list) else 0
    return pl.pallas_call(
        kernel,
        in_specs=[SM] + [VM] * count,
        out_specs=[VM] * outs if outs else VM,
        out_shape=out_shape,
        scratch_shapes=scratch,
        input_output_aliases=alias,
        compiler_params=pltpu.CompilerParams(vmem_limit_bytes=LIMIT),
    )


def dft_first(*args):
    outs = [PIECE, jax.ShapeDtypeStruct((1024, 512), BF16), jax.ShapeDtypeStruct((1536, 512), BF16)]
    return call(first_kernel, 7, outs, [pltpu.VMEM((512, 1024), F32)])(*args)


def dft_next(*args):
    return call(next_kernel, 3, [PIECE, PIECE], [pltpu.VMEM((2, 512, 1024), F32)])(*args)


def dft_last(*args):
    outs = [jax.ShapeDtypeStruct((1024, 128), F32), jax.ShapeDtypeStruct((512, 128), F32)]
    return call(last_kernel, 4, outs, [pltpu.VMEM((512, 1024), F32)])(*args)


def product(lhs, weights):
    return lax.dot_general(lhs, weights, (((1,), (1,)), ((), ())), preferred_element_type=F32)


def store_beams(side, acc, group_ref, out_ref):
    acc = acc.reshape(2, 512, 384)
    group = group_ref[...][None]
    total = jnp.where(group == 0, acc[:, :, 0:128], jnp.where(group == 1, acc[:, :, 128:256], acc[:, :, 256:384]))
    re = total[0].reshape(4, 8, 16, 128)
    im = total[1].reshape(4, 8, 16, 128)
    both = jnp.concatenate([re, im], 2).astype(BF16)
    for y in range(4):
        out_ref[:, pl.ds(side, 1), y] = both[y][:, None]


def place_rows(l_ref, xl, src):
    for r in range(0, 512, 64):
        sr, si = src[r : r + 64, :], src[512 + r : 576 + r, :]
        c0, c1 = slice(xl * 256, xl * 256 + 128), slice(xl * 256 + 128, xl * 256 + 256)
        l_ref[r : r + 64, c0] = sr
        l_ref[r : r + 64, c1] = -si
        l_ref[512 + r : 576 + r, c0] = si
        l_ref[512 + r : 576 + r, c1] = sr


def place_weights(core, w_ref, col, blocks):
    for which in range(2):
        lane0 = pl.multiple_of((core if which == 0 else 1 - core) * 128, 128)
        for i in range(6):
            row, at = i // 2 * 128, col + i % 2 * 128
            w_ref[which, row : row + 128, at : at + 128] = blocks[i][:, pl.ds(lane0, 128)]


def pack_near_kernel(ids_ref, w0_ref, w1_ref, p0_ref, p1_ref):
    place_weights(ids_ref[0], p0_ref, 0, [w0_ref.at[i] for i in range(6)])
    place_weights(ids_ref[0], p1_ref, 0, [w1_ref.at[i] for i in range(6)])


def pack_side_kernel(ids_ref, w3_ref, p3_ref):
    place_weights(ids_ref[0], p3_ref, 0, [w3_ref.at[i] for i in range(6)])


def half_sums(which, l_ref, p0_ref, p1_ref, p3_ref):
    both = product(l_ref[:, 256:512], jnp.concatenate([p1_ref[which], p3_ref[which]], 0))
    return product(l_ref[:, 0:256], p0_ref[which]) + both[:, 0:384], both[:, 384:768]


def own_kernel(ids_ref, same_ref, cross_ref, p0_ref, p1_ref, p3_ref, l_ref, near_ref, far_ref):
    place_rows(l_ref, 0, same_ref)
    place_rows(l_ref, 1, cross_ref)
    near_ref[...], far_ref[...] = half_sums(0, l_ref, p0_ref, p1_ref, p3_ref)


def sib_kernel(
    ids_ref, same_ref, cross_ref, p0_ref, p1_ref, p3_ref, near_ref, begun_ref, group_ref, out_ref, l_ref, far_ref
):
    place_rows(l_ref, 0, same_ref)
    place_rows(l_ref, 1, cross_ref)
    near, far = half_sums(1, l_ref, p0_ref, p1_ref, p3_ref)
    store_beams(ids_ref[1], near_ref[...] + near, group_ref, out_ref)
    far_ref[...] = begun_ref[...] + far


def far_kernel(ids_ref, own_ref, sib_ref, acc_ref, group_ref, w2a_ref, w2b_ref, begun_ref, out_ref, w_ref):
    place_weights(ids_ref[0], w_ref, 0, [w2a_ref.at[i] for i in range(3)] + [w2b_ref.at[i] for i in range(3)])
    acc = acc_ref[...] + product(own_ref[:, 0:256], w_ref[0]) + product(sib_ref[:, 0:256], w_ref[1])
    store_beams(1 - ids_ref[1], acc, group_ref, out_ref)


PARTS = jax.ShapeDtypeStruct((8, 2, 4, 32, 128), BF16)
ROWS = jax.ShapeDtypeStruct((1024, 512), BF16)
SUMS = jax.ShapeDtypeStruct((1024, 384), F32)


PACKED = jax.ShapeDtypeStruct((2, 384, 256), BF16)


def pack_near(*args):
    return call(pack_near_kernel, 2, [PACKED, PACKED], [])(*args)


def pack_side(*args):
    return call(pack_side_kernel, 1, PACKED, [])(*args)


def form_own(*args):
    return call(own_kernel, 5, [ROWS, SUMS, SUMS], [])(*args)


def form_sib(*args):
    return call(sib_kernel, 8, [PARTS, ROWS, SUMS], [])(*args)


def form_far(*args):
    return call(far_kernel, 7, PARTS, [pltpu.VMEM((2, 384, 256), BF16)], {7: 0})(*args)


def add_kernel(got_ref, out_ref):
    for side in range(2):
        sources = [(z * 2 + side) * 4 + y for z in range(8) for y in range(4)]
        parts = [got_ref[src].astype(F32) for src in sources[:4]]
        for place, src in enumerate(sources[4:]):
            parts[place % 4] = parts[place % 4] + got_ref[src].astype(F32)
        total = (parts[0] + parts[1]) + (parts[2] + parts[3])
        for p in range(2):
            out_ref[side * 16 : side * 16 + 16, p, :] = total[p * 16 : p * 16 + 16]


def add(got):
    return pl.pallas_call(
        add_kernel,
        in_specs=[VM],
        out_specs=VM,
        out_shape=jax.ShapeDtypeStruct((32, 2, 128), F32),
        compiler_params=pltpu.CompilerParams(vmem_limit_bytes=LIMIT),
        name="add",
    )(got)


def shards(signals, weights, bin_group):
    half, core, low = lax.axis_index("xhi"), lax.axis_index("core"), lax.axis_index("xlo")
    ring = ("xlo", "xhi", "core")

    def exchange(value, flip):
        return lax.ppermute(value, ring, [(i, i ^ flip) for i in range(8)])

    ids = jnp.stack([core, half, low])
    blocks = weights.reshape(6, 128, 256)
    w1 = exchange(blocks, 4)
    w3 = exchange(blocks, 6)
    other = exchange(signals, 1)
    own, perm, table, coarse, fine, outer = prep(ids, pltpu.with_memory_space_constraint(signals, pltpu.HBM))

    spec0, xs, rest = dft_first(ids, other, own, perm, table, coarse, fine, outer)
    got0 = exchange(spec0, 2)
    spec1, spec2 = dft_next(ids, xs, rest, outer)
    got1 = exchange(spec1, 4)
    got2 = exchange(spec2, 6)
    mine, group = dft_last(ids, xs, rest, outer, bin_group.reshape(16, 128))
    same = (mine + got0.astype(F32)).astype(BF16)
    same_sib = exchange(same, 1)
    p0, p1 = pack_near(ids, blocks, w1)
    w2a = exchange(w1[:3], 6)
    w2b = exchange(w3[3:], 4)
    p3 = pack_side(ids, w3)
    cross = (got1.astype(F32) + got2.astype(F32)).astype(BF16)
    cross_sib = exchange(cross, 1)
    lhs, near, far = form_own(ids, same, cross, p0, p1, p3)
    begun, lhs_sib, acc_far = form_sib(ids, same_sib, cross_sib, p0, p1, p3, near, far, group)
    parts = form_far(ids, lhs, lhs_sib, acc_far, group, w2a, w2b, begun)
    got = lax.all_to_all(parts.reshape(64, 32, 128), ("z", "xhi", "y"), 0, 0, tiled=True)
    return add(got)


def solution(mesh):
    fine = Mesh(mesh.devices.reshape(4, 2, 8, 2, 2), ("y", "xlo", "z", "xhi", "core"))
    chan, beam = ("y", "xlo", "z"), ("xhi", "core")
    in_specs = (P(chan, beam), P(None, None, beam, chan), P())
    out_specs = P(chan, None, beam)
    return jax.shard_map(shards, mesh=fine, in_specs=in_specs, out_specs=out_specs, check_vma=False)
```

```python
import math

import jax
import jax.numpy as jnp
from jax import lax
from jax.experimental import pallas as pl
from jax.experimental.pallas import tpu as pltpu
from jax.sharding import Mesh, PartitionSpec as P

F32 = jnp.float32
BF16 = jnp.bfloat16
I32 = jnp.int32

STRIDE = 8
SAMPLES = 8192
LIMIT = 16 * 1024 * 1024
UNROLL = 16


def root(numer, denom):
    angle = 2.0 * math.pi / denom * (numer & (denom - 1)).astype(F32)
    return jnp.cos(angle), -jnp.sin(angle)


def iota(shape, dim):
    return lax.broadcasted_iota(I32, shape, dim)


def deinterleave(x, perm):
    out = []
    rows = jnp.concatenate([x[:, :1024], x[:, 1024:]], 0)
    split = jnp.dot(rows, perm, preferred_element_type=F32).astype(BF16)
    for s in range(STRIDE):
        cols = split[:, s * 128 : (s + 1) * 128]
        out.append(jnp.concatenate([cols[:128], cols[128:]], 1))
    return out


def eighth(q):
    q = q & 7
    half = math.sqrt(0.5)
    odd = (q & 1) != 0
    re = jnp.where(odd, half, jnp.where((q & 2) != 0, 0.0, 1.0))
    re = jnp.where((q > 2) & (q < 6), -re, re)
    im = jnp.where(odd, half, jnp.where((q & 2) != 0, 1.0, 0.0))
    im = jnp.where(q < 4, -im, im)
    return re, im


def owner(ids_ref, slot):
    half, low = ids_ref[1], ids_ref[2]
    return (1 - half if slot in (0, 2) else half), (1 - low if slot in (1, 2) else low)


def block_of(t, low):
    return t // 8 * 16 + low * 8 + t % 8


def make_twiddles(ids_ref, slot, coarse_ref, fine_ref, t_ref, row0):
    half, low = owner(ids_ref, slot)
    first = pl.multiple_of(half * 16, 16)
    fr = fine_ref[0, pl.ds(first, 16), :]
    fi = fine_ref[1, pl.ds(first, 16), :]
    for t in range(16):
        k = block_of(t, low)
        cr = jnp.concatenate([coarse_ref[0, pl.ds(k, 1), :]] * 4, 1)
        ci = jnp.concatenate([coarse_ref[1, pl.ds(k, 1), :]] * 4, 1)
        row = row0 + t * 16
        t_ref[row : row + 16, :] = (cr * fr - ci * fi).astype(BF16)
        t_ref[row + 256 : row + 272, :] = (cr * fi + ci * fr).astype(BF16)


def prep_kernel(ids_ref, own_ref, xs_ref, perm_ref, t_ref, coarse_ref, fine_ref, outer_ref):
    core, half = ids_ref[0], ids_ref[1]
    row, lane = iota((32, 128), 0), iota((32, 128), 1)
    coarse_ref[0], coarse_ref[1] = root(row * lane, 32)
    br, bi = root((row + 1) * lane, 1024)
    for part in range(4):
        u = 2 * core + part if part < 2 else 2 * (1 - core) + part - 2
        er, ei = eighth((row + 1) * u)
        cols = slice(part * 128, part * 128 + 128)
        fine_ref[0, :, cols] = br * er - bi * ei
        fine_ref[1, :, cols] = br * ei + bi * er
    outer_ref[0], outer_ref[1] = root(row * 32, SAMPLES)
    outer_ref[2], outer_ref[3] = root(row + 1, SAMPLES)
    scale = 1.0 / math.sqrt(SAMPLES)
    outer_ref[4] = jnp.where((((row + 1) * half) & 1) != 0, -scale, scale)
    make_twiddles(ids_ref, 0, coarse_ref, fine_ref, t_ref, 0)
    same = jnp.where(iota((1024, 128), 0) // STRIDE == iota((1024, 128), 1), 1.0, 0.0).astype(BF16)
    phase = iota((16, 128), 0) & (STRIDE - 1)
    for s in range(STRIDE):
        keep = jnp.where(phase == s, 1.0, 0.0).astype(BF16)
        perm_ref[:, s * 128 : (s + 1) * 128] = (same.reshape(64, 16, 128) * keep[None]).reshape(1024, 128)
    for s, rows in enumerate(deinterleave(own_ref[...], perm_ref[...])):
        xs_ref[s * 128 : (s + 1) * 128, :] = rows


def prep(ids, signals):
    full = lambda *shape: pl.BlockSpec(shape, lambda i, ids: (0,) * len(shape))
    return pl.pallas_call(
        prep_kernel,
        grid_spec=pltpu.PrefetchScalarGridSpec(
            num_scalar_prefetch=1,
            grid=(1,),
            in_specs=[pl.BlockSpec((128, 2048), lambda i, ids: (ids[0], 0))],
            out_specs=[
                full(1024, 256),
                full(1024, 1024),
                full(512, 512),
                full(2, 32, 128),
                full(2, 32, 512),
                full(5, 32, 128),
            ],
        ),
        out_shape=[
            jax.ShapeDtypeStruct((1024, 256), BF16),
            jax.ShapeDtypeStruct((1024, 1024), BF16),
            jax.ShapeDtypeStruct((512, 512), BF16),
            jax.ShapeDtypeStruct((2, 32, 128), F32),
            jax.ShapeDtypeStruct((2, 32, 512), F32),
            jax.ShapeDtypeStruct((5, 32, 128), F32),
        ],
        compiler_params=pltpu.CompilerParams(vmem_limit_bytes=LIMIT),
        name="prep",
    )(ids, signals)


def times(w, x):
    return w[0] * x[0] - w[1] * x[1], w[0] * x[1] + w[1] * x[0]


def plus(x, y):
    return x[0] + y[0], x[1] + y[1]


def minus(x, y):
    return x[0] - y[0], x[1] - y[1]


def turned(x, y):
    return x[0] + y[1], x[1] - y[0]


def combine(ids_ref, slot, f_ref, outer_ref, out_ref):
    half, low = owner(ids_ref, slot)
    first = pl.multiple_of(half * 16, 16)
    fine = outer_ref[2, pl.ds(first, 16), :], outer_ref[3, pl.ds(first, 16), :]
    scale = outer_ref[4, pl.ds(first, 16), :]
    eighth_root = math.sqrt(0.5)

    def step(t, carry):
        row0 = pl.multiple_of(t * 16, 16)
        k = block_of(t, low)
        w = times((outer_ref[0, pl.ds(k, 1), :], outer_ref[1, pl.ds(k, 1), :]), fine)
        w2 = times(w, w)
        w4 = times(w2, w2)
        wt = eighth_root * (w[0] + w[1]), eighth_root * (w[1] - w[0])
        term = lambda s: (
            f_ref[pl.ds(row0, 16), s * 128 : (s + 1) * 128],
            f_ref[pl.ds(row0 + 256, 16), s * 128 : (s + 1) * 128],
        )
        sums = []
        for s in range(2):
            near, far = term(s), times(w4, term(s + 4))
            up, down = plus(near, far), minus(near, far)
            near, far = term(s + 2), times(w4, term(s + 6))
            sums.append(
                (plus(up, times(w2, plus(near, far))), turned(down, times(w2, minus(near, far))))
            )
        low_bin = plus(sums[0][0], times(w, sums[1][0]))
        high_bin = plus(sums[0][1], times(wt, sums[1][1]))
        for place, value in enumerate((low_bin[0], high_bin[0], low_bin[1], high_bin[1])):
            rows = pl.ds(row0 + 256 * place, 16)
            out_ref[rows, :] = (value * scale).astype(out_ref.dtype)
        return carry

    lax.fori_loop(0, 16, step, 0, unroll=UNROLL)


def spectrum(t_ref, row0, xs_ref, f_ref):
    f_ref[...] = lax.dot_general(
        t_ref[row0 : row0 + 512, :], xs_ref[...], (((1,), (1,)), ((), ())), preferred_element_type=F32
    )


def first_kernel(
    ids_ref, other_ref, own_ref, perm_ref, t_ref, coarse_ref, fine_ref, outer_ref, out_ref, xs_ref, rest_ref, f_ref
):
    xs_ref[:, 0:256] = own_ref[...]
    other = other_ref[pl.ds(pl.multiple_of(ids_ref[0] * 128, 128), 128), :]
    for s, rows in enumerate(deinterleave(other, perm_ref[...])):
        xs_ref[s * 128 : (s + 1) * 128, 256:512] = rows
    for slot in (1, 2, 3):
        make_twiddles(ids_ref, slot, coarse_ref, fine_ref, rest_ref, (slot - 1) * 512)
    spectrum(t_ref, 0, xs_ref, f_ref)
    combine(ids_ref, 0, f_ref, outer_ref, out_ref)


def next_kernel(ids_ref, xs_ref, rest_ref, outer_ref, out1_ref, out2_ref, f_ref):
    for index, out_ref in enumerate((out1_ref, out2_ref)):
        spectrum(rest_ref, index * 512, xs_ref, f_ref.at[index])
        combine(ids_ref, 1 + index, f_ref.at[index], outer_ref, out_ref)


def last_kernel(ids_ref, xs_ref, rest_ref, outer_ref, bins_ref, out_ref, group_ref, f_ref):
    spectrum(rest_ref, 1024, xs_ref, f_ref)
    half, low = ids_ref[1], ids_ref[2]
    row, lane = iota((512, 128), 0), iota((512, 128), 1)
    line = jnp.where(lane == (row // 128 * 4 + low * 2 + row // 64 % 2), 1.0, 0.0).astype(BF16)[:, :16]
    lines = jnp.dot(line, bins_ref[...].astype(F32).astype(BF16), preferred_element_type=F32)
    place = row // 16 % 4 * 32 + half * 16 + row % 16
    chosen = jnp.where(lane == place, lines, 0.0).astype(BF16)
    group_ref[...] = jnp.dot(chosen, jnp.ones((128, 128), BF16), preferred_element_type=F32)
    combine(ids_ref, 3, f_ref, outer_ref, out_ref)


VM = pl.BlockSpec(memory_space=pltpu.VMEM)


SM = pl.BlockSpec(memory_space=pltpu.SMEM)
PIECE = jax.ShapeDtypeStruct((1024, 128), BF16)


def call(kernel, count, out_shape, scratch, alias={}):
    outs = len(out_shape) if isinstance(out_shape, list) else 0
    return pl.pallas_call(
        kernel,
        in_specs=[SM] + [VM] * count,
        out_specs=[VM] * outs if outs else VM,
        out_shape=out_shape,
        scratch_shapes=scratch,
        input_output_aliases=alias,
        compiler_params=pltpu.CompilerParams(vmem_limit_bytes=LIMIT),
    )


def dft_first(*args):
    outs = [PIECE, jax.ShapeDtypeStruct((1024, 512), BF16), jax.ShapeDtypeStruct((1536, 512), BF16)]
    return call(first_kernel, 7, outs, [pltpu.VMEM((512, 1024), F32)])(*args)


def dft_next(*args):
    return call(next_kernel, 3, [PIECE, PIECE], [pltpu.VMEM((2, 512, 1024), F32)])(*args)


def dft_last(*args):
    outs = [jax.ShapeDtypeStruct((1024, 128), F32), jax.ShapeDtypeStruct((512, 128), F32)]
    return call(last_kernel, 4, outs, [pltpu.VMEM((512, 1024), F32)])(*args)


def product(lhs, weights):
    return lax.dot_general(lhs, weights, (((1,), (1,)), ((), ())), preferred_element_type=F32)


def store_beams(side, acc, group_ref, out_ref):
    acc = acc.reshape(2, 512, 384)
    group = group_ref[...][None]
    total = jnp.where(group == 0, acc[:, :, 0:128], jnp.where(group == 1, acc[:, :, 128:256], acc[:, :, 256:384]))
    re = total[0].reshape(4, 8, 16, 128)
    im = total[1].reshape(4, 8, 16, 128)
    both = jnp.concatenate([re, im], 2).astype(BF16)
    out_ref[:, pl.ds(side, 1)] = both[:, None]


def place_rows(l_ref, xl, src):
    for r in range(0, 512, 64):
        sr, si = src[r : r + 64, :], src[512 + r : 576 + r, :]
        c0, c1 = slice(xl * 256, xl * 256 + 128), slice(xl * 256 + 128, xl * 256 + 256)
        l_ref[r : r + 64, c0] = sr
        l_ref[r : r + 64, c1] = -si
        l_ref[512 + r : 576 + r, c0] = si
        l_ref[512 + r : 576 + r, c1] = sr


def place_weights(core, w_ref, col, blocks):
    for which in range(2):
        lane0 = pl.multiple_of((core if which == 0 else 1 - core) * 128, 128)
        for i in range(6):
            row, at = i // 2 * 128, col + i % 2 * 128
            w_ref[which, row : row + 128, at : at + 128] = blocks[i][:, pl.ds(lane0, 128)]


def pack_near_kernel(ids_ref, w0_ref, w1_ref, p0_ref, p1_ref):
    place_weights(ids_ref[0], p0_ref, 0, [w0_ref.at[i] for i in range(6)])
    place_weights(ids_ref[0], p1_ref, 0, [w1_ref.at[i] for i in range(6)])


def pack_side_kernel(ids_ref, w3_ref, p3_ref):
    place_weights(ids_ref[0], p3_ref, 0, [w3_ref.at[i] for i in range(6)])


def half_sums(which, l_ref, p0_ref, p1_ref, p3_ref):
    both = product(l_ref[:, 256:512], jnp.concatenate([p1_ref[which], p3_ref[which]], 0))
    return product(l_ref[:, 0:256], p0_ref[which]) + both[:, 0:384], both[:, 384:768]


def own_kernel(ids_ref, same_ref, cross_ref, p0_ref, p1_ref, p3_ref, l_ref, near_ref, far_ref):
    place_rows(l_ref, 0, same_ref)
    place_rows(l_ref, 1, cross_ref)
    near_ref[...], far_ref[...] = half_sums(0, l_ref, p0_ref, p1_ref, p3_ref)


def sib_kernel(
    ids_ref, same_ref, cross_ref, p0_ref, p1_ref, p3_ref, near_ref, begun_ref, group_ref, out_ref, l_ref, far_ref
):
    place_rows(l_ref, 0, same_ref)
    place_rows(l_ref, 1, cross_ref)
    near, far = half_sums(1, l_ref, p0_ref, p1_ref, p3_ref)
    store_beams(ids_ref[1], near_ref[...] + near, group_ref, out_ref)
    far_ref[...] = begun_ref[...] + far


def far_kernel(ids_ref, own_ref, sib_ref, acc_ref, group_ref, w2a_ref, w2b_ref, begun_ref, out_ref, w_ref):
    place_weights(ids_ref[0], w_ref, 0, [w2a_ref.at[i] for i in range(3)] + [w2b_ref.at[i] for i in range(3)])
    acc = acc_ref[...] + product(own_ref[:, 0:256], w_ref[0]) + product(sib_ref[:, 0:256], w_ref[1])
    store_beams(1 - ids_ref[1], acc, group_ref, out_ref)


PARTS = jax.ShapeDtypeStruct((4, 2, 8, 32, 128), BF16)
ROWS = jax.ShapeDtypeStruct((1024, 512), BF16)
SUMS = jax.ShapeDtypeStruct((1024, 384), F32)


PACKED = jax.ShapeDtypeStruct((2, 384, 256), BF16)


def pack_near(*args):
    return call(pack_near_kernel, 2, [PACKED, PACKED], [])(*args)


def pack_side(*args):
    return call(pack_side_kernel, 1, PACKED, [])(*args)


def form_own(*args):
    return call(own_kernel, 5, [ROWS, SUMS, SUMS], [])(*args)


def form_sib(*args):
    return call(sib_kernel, 8, [PARTS, ROWS, SUMS], [])(*args)


def form_far(*args):
    return call(far_kernel, 7, PARTS, [pltpu.VMEM((2, 384, 256), BF16)], {7: 0})(*args)


def add_first_kernel(ids_ref, got_ref, out_ref):
    for side in range(2):
        parts = [got_ref[y, side].astype(F32) for y in range(4)]
        out_ref[:, side] = (parts[0] + parts[1]) + (parts[2] + parts[3])


def add_last_kernel(ids_ref, got_ref, out_ref):
    for side in range(2):
        parts = [got_ref[z, side] for z in range(8)]
        total = ((parts[0] + parts[1]) + (parts[2] + parts[3])) + ((parts[4] + parts[5]) + (parts[6] + parts[7]))
        for p in range(2):
            out_ref[side * 16 : side * 16 + 16, p, :] = total[p * 16 : p * 16 + 16]


def add_first(*args):
    return call(add_first_kernel, 1, jax.ShapeDtypeStruct((8, 2, 32, 128), F32), [])(*args)


def add_last(*args):
    return call(add_last_kernel, 1, jax.ShapeDtypeStruct((32, 2, 128), F32), [])(*args)


def shards(signals, weights, bin_group):
    half, core, low = lax.axis_index("xhi"), lax.axis_index("core"), lax.axis_index("xlo")
    ring = ("xlo", "xhi", "core")

    def exchange(value, flip):
        return lax.ppermute(value, ring, [(i, i ^ flip) for i in range(8)])

    ids = jnp.stack([core, half, low])
    blocks = weights.reshape(6, 128, 256)
    w1 = exchange(blocks, 4)
    w3 = exchange(blocks, 6)
    other = exchange(signals, 1)
    own, perm, table, coarse, fine, outer = prep(ids, pltpu.with_memory_space_constraint(signals, pltpu.HBM))

    spec0, xs, rest = dft_first(ids, other, own, perm, table, coarse, fine, outer)
    got0 = exchange(spec0, 2)
    spec1, spec2 = dft_next(ids, xs, rest, outer)
    got1 = exchange(spec1, 4)
    got2 = exchange(spec2, 6)
    mine, group = dft_last(ids, xs, rest, outer, bin_group.reshape(16, 128))
    same = (mine + got0.astype(F32)).astype(BF16)
    same_sib = exchange(same, 1)
    p0, p1 = pack_near(ids, blocks, w1)
    w2a = exchange(w1[:3], 6)
    w2b = exchange(w3[3:], 4)
    p3 = pack_side(ids, w3)
    cross = (got1.astype(F32) + got2.astype(F32)).astype(BF16)
    cross_sib = exchange(cross, 1)
    lhs, near, far = form_own(ids, same, cross, p0, p1, p3)
    begun, lhs_sib, acc_far = form_sib(ids, same_sib, cross_sib, p0, p1, p3, near, far, group)
    parts = form_far(ids, lhs, lhs_sib, acc_far, group, w2a, w2b, begun)
    got = lax.all_to_all(parts.reshape(8, 8, 32, 128), ("y", "xhi"), 0, 0, tiled=True)
    column = add_first(ids, got.reshape(4, 2, 8, 32, 128))
    return add_last(ids, lax.all_to_all(column, "z", 0, 0, tiled=True))


def solution(mesh):
    fine = Mesh(mesh.devices.reshape(4, 2, 8, 2, 2), ("y", "xlo", "z", "xhi", "core"))
    chan, beam = ("y", "xlo", "z"), ("xhi", "core")
    in_specs = (P(chan, beam), P(None, None, beam, chan), P())
    out_specs = P(chan, None, beam)
    return jax.shard_map(shards, mesh=fine, in_specs=in_specs, out_specs=out_specs, check_vma=False)
```

```python
import math

import jax
import jax.numpy as jnp
from jax import lax
from jax.experimental import pallas as pl
from jax.experimental.pallas import tpu as pltpu
from jax.sharding import Mesh, PartitionSpec as P

F32 = jnp.float32
BF16 = jnp.bfloat16
I32 = jnp.int32

STRIDE = 8
SAMPLES = 8192
LIMIT = 16 * 1024 * 1024
UNROLL = 16


def root(numer, denom):
    angle = 2.0 * math.pi / denom * (numer & (denom - 1)).astype(F32)
    return jnp.cos(angle), -jnp.sin(angle)


def iota(shape, dim):
    return lax.broadcasted_iota(I32, shape, dim)


def deinterleave(x, perm):
    out = []
    rows = jnp.concatenate([x[:, :1024], x[:, 1024:]], 0)
    split = jnp.dot(rows, perm, preferred_element_type=F32).astype(BF16)
    for s in range(STRIDE):
        cols = split[:, s * 128 : (s + 1) * 128]
        out.append(jnp.concatenate([cols[:128], cols[128:]], 1))
    return out


def eighth(q):
    q = q & 7
    half = math.sqrt(0.5)
    odd = (q & 1) != 0
    re = jnp.where(odd, half, jnp.where((q & 2) != 0, 0.0, 1.0))
    re = jnp.where((q > 2) & (q < 6), -re, re)
    im = jnp.where(odd, half, jnp.where((q & 2) != 0, 1.0, 0.0))
    im = jnp.where(q < 4, -im, im)
    return re, im


def owner(ids_ref, slot):
    half, low = ids_ref[1], ids_ref[2]
    return (1 - half if slot in (0, 2) else half), (1 - low if slot in (1, 2) else low)


def block_of(t, low):
    return t // 8 * 16 + low * 8 + t % 8


def make_twiddles(ids_ref, slot, coarse_ref, fine_ref, t_ref, row0):
    half, low = owner(ids_ref, slot)
    first = pl.multiple_of(half * 16, 16)
    fr = fine_ref[0, pl.ds(first, 16), :]
    fi = fine_ref[1, pl.ds(first, 16), :]
    for t in range(16):
        k = block_of(t, low)
        cr = jnp.concatenate([coarse_ref[0, pl.ds(k, 1), :]] * 4, 1)
        ci = jnp.concatenate([coarse_ref[1, pl.ds(k, 1), :]] * 4, 1)
        row = row0 + t * 16
        t_ref[row : row + 16, :] = (cr * fr - ci * fi).astype(BF16)
        t_ref[row + 256 : row + 272, :] = (cr * fi + ci * fr).astype(BF16)


def prep_kernel(ids_ref, own_ref, xs_ref, perm_ref, t_ref, coarse_ref, fine_ref, outer_ref):
    core, half = ids_ref[0], ids_ref[1]
    row, lane = iota((32, 128), 0), iota((32, 128), 1)
    coarse_ref[0], coarse_ref[1] = root(row * lane, 32)
    br, bi = root((row + 1) * lane, 1024)
    for part in range(4):
        u = 2 * core + part if part < 2 else 2 * (1 - core) + part - 2
        er, ei = eighth((row + 1) * u)
        cols = slice(part * 128, part * 128 + 128)
        fine_ref[0, :, cols] = br * er - bi * ei
        fine_ref[1, :, cols] = br * ei + bi * er
    outer_ref[0], outer_ref[1] = root(row * 32, SAMPLES)
    outer_ref[2], outer_ref[3] = root(row + 1, SAMPLES)
    scale = 1.0 / math.sqrt(SAMPLES)
    outer_ref[4] = jnp.where((((row + 1) * half) & 1) != 0, -scale, scale)
    make_twiddles(ids_ref, 0, coarse_ref, fine_ref, t_ref, 0)
    same = jnp.where(iota((1024, 128), 0) // STRIDE == iota((1024, 128), 1), 1.0, 0.0).astype(BF16)
    phase = iota((16, 128), 0) & (STRIDE - 1)
    for s in range(STRIDE):
        keep = jnp.where(phase == s, 1.0, 0.0).astype(BF16)
        perm_ref[:, s * 128 : (s + 1) * 128] = (same.reshape(64, 16, 128) * keep[None]).reshape(1024, 128)
    for s, rows in enumerate(deinterleave(own_ref[...], perm_ref[...])):
        xs_ref[s * 128 : (s + 1) * 128, :] = rows


def prep(ids, signals):
    full = lambda *shape: pl.BlockSpec(shape, lambda i, ids: (0,) * len(shape))
    return pl.pallas_call(
        prep_kernel,
        grid_spec=pltpu.PrefetchScalarGridSpec(
            num_scalar_prefetch=1,
            grid=(1,),
            in_specs=[pl.BlockSpec((128, 2048), lambda i, ids: (ids[0], 0))],
            out_specs=[
                full(1024, 256),
                full(1024, 1024),
                full(512, 512),
                full(2, 32, 128),
                full(2, 32, 512),
                full(5, 32, 128),
            ],
        ),
        out_shape=[
            jax.ShapeDtypeStruct((1024, 256), BF16),
            jax.ShapeDtypeStruct((1024, 1024), BF16),
            jax.ShapeDtypeStruct((512, 512), BF16),
            jax.ShapeDtypeStruct((2, 32, 128), F32),
            jax.ShapeDtypeStruct((2, 32, 512), F32),
            jax.ShapeDtypeStruct((5, 32, 128), F32),
        ],
        compiler_params=pltpu.CompilerParams(vmem_limit_bytes=LIMIT),
        name="prep",
    )(ids, signals)


def times(w, x):
    return w[0] * x[0] - w[1] * x[1], w[0] * x[1] + w[1] * x[0]


def plus(x, y):
    return x[0] + y[0], x[1] + y[1]


def minus(x, y):
    return x[0] - y[0], x[1] - y[1]


def turned(x, y):
    return x[0] + y[1], x[1] - y[0]


def combine(ids_ref, slot, f_ref, outer_ref, out_ref):
    half, low = owner(ids_ref, slot)
    first = pl.multiple_of(half * 16, 16)
    fine = outer_ref[2, pl.ds(first, 16), :], outer_ref[3, pl.ds(first, 16), :]
    scale = outer_ref[4, pl.ds(first, 16), :]
    eighth_root = math.sqrt(0.5)

    def step(t, carry):
        row0 = pl.multiple_of(t * 16, 16)
        k = block_of(t, low)
        w = times((outer_ref[0, pl.ds(k, 1), :], outer_ref[1, pl.ds(k, 1), :]), fine)
        w2 = times(w, w)
        w4 = times(w2, w2)
        wt = eighth_root * (w[0] + w[1]), eighth_root * (w[1] - w[0])
        term = lambda s: (
            f_ref[pl.ds(row0, 16), s * 128 : (s + 1) * 128],
            f_ref[pl.ds(row0 + 256, 16), s * 128 : (s + 1) * 128],
        )
        sums = []
        for s in range(2):
            near, far = term(s), times(w4, term(s + 4))
            up, down = plus(near, far), minus(near, far)
            near, far = term(s + 2), times(w4, term(s + 6))
            sums.append(
                (plus(up, times(w2, plus(near, far))), turned(down, times(w2, minus(near, far))))
            )
        low_bin = plus(sums[0][0], times(w, sums[1][0]))
        high_bin = plus(sums[0][1], times(wt, sums[1][1]))
        for place, value in enumerate((low_bin[0], high_bin[0], low_bin[1], high_bin[1])):
            rows = pl.ds(row0 + 256 * place, 16)
            out_ref[rows, :] = (value * scale).astype(out_ref.dtype)
        return carry

    lax.fori_loop(0, 16, step, 0, unroll=UNROLL)


def spectrum(t_ref, row0, xs_ref, f_ref):
    f_ref[...] = lax.dot_general(
        t_ref[row0 : row0 + 512, :], xs_ref[...], (((1,), (1,)), ((), ())), preferred_element_type=F32
    )


def first_kernel(
    ids_ref, other_ref, own_ref, perm_ref, t_ref, coarse_ref, fine_ref, outer_ref, out_ref, xs_ref, rest_ref, f_ref
):
    xs_ref[:, 0:256] = own_ref[...]
    other = other_ref[pl.ds(pl.multiple_of(ids_ref[0] * 128, 128), 128), :]
    for s, rows in enumerate(deinterleave(other, perm_ref[...])):
        xs_ref[s * 128 : (s + 1) * 128, 256:512] = rows
    for slot in (1, 2, 3):
        make_twiddles(ids_ref, slot, coarse_ref, fine_ref, rest_ref, (slot - 1) * 512)
    spectrum(t_ref, 0, xs_ref, f_ref)
    combine(ids_ref, 0, f_ref, outer_ref, out_ref)


def next_kernel(ids_ref, xs_ref, rest_ref, outer_ref, out1_ref, out2_ref, f_ref):
    for index, out_ref in enumerate((out1_ref, out2_ref)):
        spectrum(rest_ref, index * 512, xs_ref, f_ref.at[index])
        combine(ids_ref, 1 + index, f_ref.at[index], outer_ref, out_ref)


def last_kernel(ids_ref, xs_ref, rest_ref, outer_ref, bins_ref, out_ref, group_ref, f_ref):
    spectrum(rest_ref, 1024, xs_ref, f_ref)
    half, low = ids_ref[1], ids_ref[2]
    row, lane = iota((512, 128), 0), iota((512, 128), 1)
    line = jnp.where(lane == (row // 128 * 4 + low * 2 + row // 64 % 2), 1.0, 0.0).astype(BF16)[:, :16]
    lines = jnp.dot(line, bins_ref[...].astype(F32).astype(BF16), preferred_element_type=F32)
    place = row // 16 % 4 * 32 + half * 16 + row % 16
    chosen = jnp.where(lane == place, lines, 0.0).astype(BF16)
    group_ref[...] = jnp.dot(chosen, jnp.ones((128, 128), BF16), preferred_element_type=F32)
    combine(ids_ref, 3, f_ref, outer_ref, out_ref)


VM = pl.BlockSpec(memory_space=pltpu.VMEM)


SM = pl.BlockSpec(memory_space=pltpu.SMEM)
PIECE = jax.ShapeDtypeStruct((1024, 128), BF16)


def call(kernel, count, out_shape, scratch, alias={}):
    outs = len(out_shape) if isinstance(out_shape, list) else 0
    return pl.pallas_call(
        kernel,
        in_specs=[SM] + [VM] * count,
        out_specs=[VM] * outs if outs else VM,
        out_shape=out_shape,
        scratch_shapes=scratch,
        input_output_aliases=alias,
        compiler_params=pltpu.CompilerParams(vmem_limit_bytes=LIMIT),
    )


def dft_first(*args):
    outs = [PIECE, jax.ShapeDtypeStruct((1024, 512), BF16), jax.ShapeDtypeStruct((1536, 512), BF16)]
    return call(first_kernel, 7, outs, [pltpu.VMEM((512, 1024), F32)])(*args)


def dft_next(*args):
    return call(next_kernel, 3, [PIECE, PIECE], [pltpu.VMEM((2, 512, 1024), F32)])(*args)


def dft_last(*args):
    outs = [jax.ShapeDtypeStruct((1024, 128), F32), jax.ShapeDtypeStruct((512, 128), F32)]
    return call(last_kernel, 4, outs, [pltpu.VMEM((512, 1024), F32)])(*args)


def product(lhs, weights):
    return lax.dot_general(lhs, weights, (((1,), (1,)), ((), ())), preferred_element_type=F32)


def store_beams(side, acc, group_ref, out_ref):
    acc = acc.reshape(2, 512, 384)
    group = group_ref[...][None]
    total = jnp.where(group == 0, acc[:, :, 0:128], jnp.where(group == 1, acc[:, :, 128:256], acc[:, :, 256:384]))
    re = total[0].reshape(4, 8, 16, 128)
    im = total[1].reshape(4, 8, 16, 128)
    both = jnp.concatenate([re, im], 2).astype(BF16)
    for y in range(4):
        out_ref[:, pl.ds(side, 1), y] = both[y][:, None]


def place_rows(l_ref, src):
    for r in range(0, 512, 64):
        sr, si = src[r : r + 64, :], src[512 + r : 576 + r, :]
        l_ref[r : r + 64, 0:128] = sr
        l_ref[r : r + 64, 128:256] = -si
        l_ref[512 + r : 576 + r, 0:128] = si
        l_ref[512 + r : 576 + r, 128:256] = sr


def place_weights(core, w_ref, col, blocks):
    for which in range(2):
        lane0 = pl.multiple_of((core if which == 0 else 1 - core) * 128, 128)
        for i in range(6):
            row, at = i // 2 * 128, col + i % 2 * 128
            w_ref[which, row : row + 128, at : at + 128] = blocks[i][:, pl.ds(lane0, 128)]


def pack_near_kernel(ids_ref, w0_ref, w1_ref, p0_ref, p1_ref):
    place_weights(ids_ref[0], p0_ref, 0, [w0_ref.at[i] for i in range(6)])
    place_weights(ids_ref[0], p1_ref, 0, [w1_ref.at[i] for i in range(6)])


def pack_side_kernel(ids_ref, w3_ref, p3_ref):
    place_weights(ids_ref[0], p3_ref, 0, [w3_ref.at[i] for i in range(6)])


def early_kernel(ids_ref, own_ref, sib_ref, p0_ref, l_ref, near_ref):
    place_rows(l_ref.at[0], own_ref)
    place_rows(l_ref.at[1], sib_ref)
    near_ref[...] = product(l_ref[0], p0_ref[0]) + product(l_ref[1], p0_ref[1])


def cross_sums(which, l_ref, p1_ref, p3_ref):
    both = product(l_ref[...], jnp.concatenate([p1_ref[which], p3_ref[which]], 0))
    return both[:, 0:384], both[:, 384:768]


def own_kernel(ids_ref, cross_ref, p1_ref, p3_ref, begun_ref, near_ref, far_ref, l_ref):
    place_rows(l_ref, cross_ref)
    near, far_ref[...] = cross_sums(0, l_ref, p1_ref, p3_ref)
    near_ref[...] = begun_ref[...] + near


def sib_kernel(ids_ref, cross_ref, p1_ref, p3_ref, near_ref, begun_ref, group_ref, out_ref, far_ref, l_ref):
    place_rows(l_ref, cross_ref)
    near, far = cross_sums(1, l_ref, p1_ref, p3_ref)
    store_beams(ids_ref[1], near_ref[...] + near, group_ref, out_ref)
    far_ref[...] = begun_ref[...] + far


def far_kernel(ids_ref, l_ref, acc_ref, group_ref, w2a_ref, w2b_ref, begun_ref, out_ref, w_ref):
    place_weights(ids_ref[0], w_ref, 0, [w2a_ref.at[i] for i in range(3)] + [w2b_ref.at[i] for i in range(3)])
    acc = acc_ref[...] + product(l_ref[0], w_ref[0]) + product(l_ref[1], w_ref[1])
    store_beams(1 - ids_ref[1], acc, group_ref, out_ref)


PARTS = jax.ShapeDtypeStruct((8, 2, 4, 32, 128), BF16)
SUMS = jax.ShapeDtypeStruct((1024, 384), F32)


PACKED = jax.ShapeDtypeStruct((2, 384, 256), BF16)


def pack_near(*args):
    return call(pack_near_kernel, 2, [PACKED, PACKED], [])(*args)


def pack_side(*args):
    return call(pack_side_kernel, 1, PACKED, [])(*args)


LHS = pltpu.VMEM((1024, 256), BF16)


def form_early(*args):
    return call(early_kernel, 3, [jax.ShapeDtypeStruct((2, 1024, 256), BF16), SUMS], [])(*args)


def form_own(*args):
    return call(own_kernel, 4, [SUMS, SUMS], [LHS])(*args)


def form_sib(*args):
    return call(sib_kernel, 6, [PARTS, SUMS], [LHS])(*args)


def form_far(*args):
    return call(far_kernel, 6, PARTS, [pltpu.VMEM((2, 384, 256), BF16)], {6: 0})(*args)


def add_kernel(got_ref, out_ref):
    for side in range(2):
        sources = [(z * 2 + side) * 4 + y for z in range(8) for y in range(4)]
        parts = [got_ref[src].astype(F32) for src in sources[:4]]
        for place, src in enumerate(sources[4:]):
            parts[place % 4] = parts[place % 4] + got_ref[src].astype(F32)
        total = (parts[0] + parts[1]) + (parts[2] + parts[3])
        for p in range(2):
            out_ref[side * 16 : side * 16 + 16, p, :] = total[p * 16 : p * 16 + 16]


def add(got):
    return pl.pallas_call(
        add_kernel,
        in_specs=[VM],
        out_specs=VM,
        out_shape=jax.ShapeDtypeStruct((32, 2, 128), F32),
        compiler_params=pltpu.CompilerParams(vmem_limit_bytes=LIMIT),
        name="add",
    )(got)


def shards(signals, weights, bin_group):
    half, core, low = lax.axis_index("xhi"), lax.axis_index("core"), lax.axis_index("xlo")
    ring = ("xlo", "xhi", "core")

    def exchange(value, flip):
        return lax.ppermute(value, ring, [(i, i ^ flip) for i in range(8)])

    ids = jnp.stack([core, half, low])
    blocks = weights.reshape(6, 128, 256)
    w1 = exchange(blocks, 4)
    w3 = exchange(blocks, 6)
    other = exchange(signals, 1)
    own, perm, table, coarse, fine, outer = prep(ids, pltpu.with_memory_space_constraint(signals, pltpu.HBM))

    spec0, xs, rest = dft_first(ids, other, own, perm, table, coarse, fine, outer)
    got0 = exchange(spec0, 2)
    spec1, spec2 = dft_next(ids, xs, rest, outer)
    got1 = exchange(spec1, 4)
    got2 = exchange(spec2, 6)
    mine, group = dft_last(ids, xs, rest, outer, bin_group.reshape(16, 128))
    same = (mine + got0.astype(F32)).astype(BF16)
    same_sib = exchange(same, 1)
    p0, p1 = pack_near(ids, blocks, w1)
    w2a = exchange(w1[:3], 6)
    w2b = exchange(w3[3:], 4)
    p3 = pack_side(ids, w3)
    lhs, near = form_early(ids, same, same_sib, p0)
    cross = (got1.astype(F32) + got2.astype(F32)).astype(BF16)
    cross_sib = exchange(cross, 1)
    near, far = form_own(ids, cross, p1, p3, near)
    begun, far = form_sib(ids, cross_sib, p1, p3, near, far, group)
    parts = form_far(ids, lhs, far, group, w2a, w2b, begun)
    got = lax.all_to_all(parts.reshape(64, 32, 128), ("z", "xhi", "y"), 0, 0, tiled=True)
    return add(got)


def solution(mesh):
    fine = Mesh(mesh.devices.reshape(4, 2, 8, 2, 2), ("y", "xlo", "z", "xhi", "core"))
    chan, beam = ("y", "xlo", "z"), ("xhi", "core")
    in_specs = (P(chan, beam), P(None, None, beam, chan), P())
    out_specs = P(chan, None, beam)
    return jax.shard_map(shards, mesh=fine, in_specs=in_specs, out_specs=out_specs, check_vma=False)
```

```python
import math

import jax
import jax.numpy as jnp
from jax import lax
from jax.experimental import pallas as pl
from jax.experimental.pallas import tpu as pltpu
from jax.sharding import Mesh, PartitionSpec as P

F32 = jnp.float32
BF16 = jnp.bfloat16
I32 = jnp.int32

STRIDE = 8
SAMPLES = 8192
LIMIT = 16 * 1024 * 1024
UNROLL = 16


def root(numer, denom):
    angle = 2.0 * math.pi / denom * (numer & (denom - 1)).astype(F32)
    return jnp.cos(angle), -jnp.sin(angle)


def iota(shape, dim):
    return lax.broadcasted_iota(I32, shape, dim)


def deinterleave(x, perm):
    out = []
    rows = jnp.concatenate([x[:, :1024], x[:, 1024:]], 0)
    split = jnp.dot(rows, perm, preferred_element_type=F32).astype(BF16)
    for s in range(STRIDE):
        cols = split[:, s * 128 : (s + 1) * 128]
        out.append(jnp.concatenate([cols[:128], cols[128:]], 1))
    return out


def eighth(q):
    q = q & 7
    half = math.sqrt(0.5)
    odd = (q & 1) != 0
    re = jnp.where(odd, half, jnp.where((q & 2) != 0, 0.0, 1.0))
    re = jnp.where((q > 2) & (q < 6), -re, re)
    im = jnp.where(odd, half, jnp.where((q & 2) != 0, 1.0, 0.0))
    im = jnp.where(q < 4, -im, im)
    return re, im


def owner(ids_ref, slot):
    half, low = ids_ref[1], ids_ref[2]
    return (1 - half if slot in (0, 2) else half), (1 - low if slot in (1, 2) else low)


def block_of(t, low):
    return t // 8 * 16 + low * 8 + t % 8


def make_twiddles(ids_ref, slot, coarse_ref, fine_ref, t_ref, row0):
    half, low = owner(ids_ref, slot)
    first = pl.multiple_of(half * 16, 16)
    fr = fine_ref[0, pl.ds(first, 16), :]
    fi = fine_ref[1, pl.ds(first, 16), :]
    for t in range(16):
        k = block_of(t, low)
        cr = jnp.concatenate([coarse_ref[0, pl.ds(k, 1), :]] * 4, 1)
        ci = jnp.concatenate([coarse_ref[1, pl.ds(k, 1), :]] * 4, 1)
        row = row0 + t * 16
        t_ref[row : row + 16, :] = (cr * fr - ci * fi).astype(BF16)
        t_ref[row + 256 : row + 272, :] = (cr * fi + ci * fr).astype(BF16)


def prep_kernel(ids_ref, own_ref, xs_ref, perm_ref, t_ref, coarse_ref, fine_ref, outer_ref):
    core, half = ids_ref[0], ids_ref[1]
    row, lane = iota((32, 128), 0), iota((32, 128), 1)
    coarse_ref[0], coarse_ref[1] = root(row * lane, 32)
    br, bi = root((row + 1) * lane, 1024)
    for part in range(4):
        u = 2 * core + part if part < 2 else 2 * (1 - core) + part - 2
        er, ei = eighth((row + 1) * u)
        cols = slice(part * 128, part * 128 + 128)
        fine_ref[0, :, cols] = br * er - bi * ei
        fine_ref[1, :, cols] = br * ei + bi * er
    outer_ref[0], outer_ref[1] = root(row * 32, SAMPLES)
    outer_ref[2], outer_ref[3] = root(row + 1, SAMPLES)
    scale = 1.0 / math.sqrt(SAMPLES)
    outer_ref[4] = jnp.where((((row + 1) * half) & 1) != 0, -scale, scale)
    make_twiddles(ids_ref, 0, coarse_ref, fine_ref, t_ref, 0)
    same = jnp.where(iota((1024, 128), 0) // STRIDE == iota((1024, 128), 1), 1.0, 0.0).astype(BF16)
    phase = iota((16, 128), 0) & (STRIDE - 1)
    for s in range(STRIDE):
        keep = jnp.where(phase == s, 1.0, 0.0).astype(BF16)
        perm_ref[:, s * 128 : (s + 1) * 128] = (same.reshape(64, 16, 128) * keep[None]).reshape(1024, 128)
    for s, rows in enumerate(deinterleave(own_ref[...], perm_ref[...])):
        xs_ref[s * 128 : (s + 1) * 128, :] = rows


def prep(ids, signals):
    full = lambda *shape: pl.BlockSpec(shape, lambda i, ids: (0,) * len(shape))
    return pl.pallas_call(
        prep_kernel,
        grid_spec=pltpu.PrefetchScalarGridSpec(
            num_scalar_prefetch=1,
            grid=(1,),
            in_specs=[pl.BlockSpec((128, 2048), lambda i, ids: (ids[0], 0))],
            out_specs=[
                full(1024, 256),
                full(1024, 1024),
                full(512, 512),
                full(2, 32, 128),
                full(2, 32, 512),
                full(5, 32, 128),
            ],
        ),
        out_shape=[
            jax.ShapeDtypeStruct((1024, 256), BF16),
            jax.ShapeDtypeStruct((1024, 1024), BF16),
            jax.ShapeDtypeStruct((512, 512), BF16),
            jax.ShapeDtypeStruct((2, 32, 128), F32),
            jax.ShapeDtypeStruct((2, 32, 512), F32),
            jax.ShapeDtypeStruct((5, 32, 128), F32),
        ],
        compiler_params=pltpu.CompilerParams(vmem_limit_bytes=LIMIT),
        name="prep",
    )(ids, signals)


def times(w, x):
    return w[0] * x[0] - w[1] * x[1], w[0] * x[1] + w[1] * x[0]


def plus(x, y):
    return x[0] + y[0], x[1] + y[1]


def minus(x, y):
    return x[0] - y[0], x[1] - y[1]


def turned(x, y):
    return x[0] + y[1], x[1] - y[0]


def combine(ids_ref, slot, f_ref, outer_ref, out_ref):
    half, low = owner(ids_ref, slot)
    first = pl.multiple_of(half * 16, 16)
    fine = outer_ref[2, pl.ds(first, 16), :], outer_ref[3, pl.ds(first, 16), :]
    scale = outer_ref[4, pl.ds(first, 16), :]
    eighth_root = math.sqrt(0.5)

    def step(t, carry):
        row0 = pl.multiple_of(t * 16, 16)
        k = block_of(t, low)
        w = times((outer_ref[0, pl.ds(k, 1), :], outer_ref[1, pl.ds(k, 1), :]), fine)
        w2 = times(w, w)
        w4 = times(w2, w2)
        wt = eighth_root * (w[0] + w[1]), eighth_root * (w[1] - w[0])
        term = lambda s: (
            f_ref[pl.ds(row0, 16), s * 128 : (s + 1) * 128],
            f_ref[pl.ds(row0 + 256, 16), s * 128 : (s + 1) * 128],
        )
        sums = []
        for s in range(2):
            near, far = term(s), times(w4, term(s + 4))
            up, down = plus(near, far), minus(near, far)
            near, far = term(s + 2), times(w4, term(s + 6))
            sums.append(
                (plus(up, times(w2, plus(near, far))), turned(down, times(w2, minus(near, far))))
            )
        low_bin = plus(sums[0][0], times(w, sums[1][0]))
        high_bin = plus(sums[0][1], times(wt, sums[1][1]))
        for place, value in enumerate((low_bin[0], high_bin[0], low_bin[1], high_bin[1])):
            rows = pl.ds(row0 + 256 * place, 16)
            out_ref[rows, :] = (value * scale).astype(out_ref.dtype)
        return carry

    lax.fori_loop(0, 16, step, 0, unroll=UNROLL)


def spectrum(t_ref, row0, xs_ref, f_ref):
    f_ref[...] = lax.dot_general(
        t_ref[row0 : row0 + 512, :], xs_ref[...], (((1,), (1,)), ((), ())), preferred_element_type=F32
    )


def first_kernel(
    ids_ref, other_ref, own_ref, perm_ref, t_ref, coarse_ref, fine_ref, outer_ref, out_ref, xs_ref, rest_ref, f_ref
):
    xs_ref[:, 0:256] = own_ref[...]
    other = other_ref[pl.ds(pl.multiple_of(ids_ref[0] * 128, 128), 128), :]
    for s, rows in enumerate(deinterleave(other, perm_ref[...])):
        xs_ref[s * 128 : (s + 1) * 128, 256:512] = rows
    for slot in (1, 2, 3):
        make_twiddles(ids_ref, slot, coarse_ref, fine_ref, rest_ref, (slot - 1) * 512)
    spectrum(t_ref, 0, xs_ref, f_ref)
    combine(ids_ref, 0, f_ref, outer_ref, out_ref)


def next_kernel(ids_ref, xs_ref, rest_ref, outer_ref, out1_ref, out2_ref, f_ref):
    for index, out_ref in enumerate((out1_ref, out2_ref)):
        spectrum(rest_ref, index * 512, xs_ref, f_ref.at[index])
        combine(ids_ref, 1 + index, f_ref.at[index], outer_ref, out_ref)


def last_kernel(ids_ref, xs_ref, rest_ref, outer_ref, bins_ref, out_ref, group_ref, f_ref):
    spectrum(rest_ref, 1024, xs_ref, f_ref)
    half, low = ids_ref[1], ids_ref[2]
    row, lane = iota((512, 128), 0), iota((512, 128), 1)
    line = jnp.where(lane == (row // 128 * 4 + low * 2 + row // 64 % 2), 1.0, 0.0).astype(BF16)[:, :16]
    lines = jnp.dot(line, bins_ref[...].astype(F32).astype(BF16), preferred_element_type=F32)
    place = row // 16 % 4 * 32 + half * 16 + row % 16
    chosen = jnp.where(lane == place, lines, 0.0).astype(BF16)
    group_ref[...] = jnp.dot(chosen, jnp.ones((128, 128), BF16), preferred_element_type=F32)
    combine(ids_ref, 3, f_ref, outer_ref, out_ref)


VM = pl.BlockSpec(memory_space=pltpu.VMEM)


SM = pl.BlockSpec(memory_space=pltpu.SMEM)
PIECE = jax.ShapeDtypeStruct((1024, 128), BF16)


def call(kernel, count, out_shape, scratch, alias={}):
    outs = len(out_shape) if isinstance(out_shape, list) else 0
    return pl.pallas_call(
        kernel,
        in_specs=[SM] + [VM] * count,
        out_specs=[VM] * outs if outs else VM,
        out_shape=out_shape,
        scratch_shapes=scratch,
        input_output_aliases=alias,
        compiler_params=pltpu.CompilerParams(vmem_limit_bytes=LIMIT),
    )


def dft_first(*args):
    outs = [PIECE, jax.ShapeDtypeStruct((1024, 512), BF16), jax.ShapeDtypeStruct((1536, 512), BF16)]
    return call(first_kernel, 7, outs, [pltpu.VMEM((512, 1024), F32)])(*args)


def dft_next(*args):
    return call(next_kernel, 3, [PIECE, PIECE], [pltpu.VMEM((2, 512, 1024), F32)])(*args)


def dft_last(*args):
    outs = [jax.ShapeDtypeStruct((1024, 128), F32), jax.ShapeDtypeStruct((512, 128), F32)]
    return call(last_kernel, 4, outs, [pltpu.VMEM((512, 1024), F32)])(*args)


def product(lhs, weights):
    return lax.dot_general(lhs, weights, (((1,), (1,)), ((), ())), preferred_element_type=F32)


def store_beams(side, acc, group_ref, out_ref):
    acc = acc.reshape(2, 512, 384)
    group = group_ref[...][None]
    total = jnp.where(group == 0, acc[:, :, 0:128], jnp.where(group == 1, acc[:, :, 128:256], acc[:, :, 256:384]))
    re = total[0].reshape(4, 8, 16, 128)
    im = total[1].reshape(4, 8, 16, 128)
    both = jnp.concatenate([re, im], 2).astype(BF16)
    for y in range(4):
        out_ref[:, pl.ds(side, 1), y] = both[y][:, None]


def place_rows(l_ref, src):
    for r in range(0, 512, 64):
        sr, si = src[r : r + 64, :], src[512 + r : 576 + r, :]
        l_ref[r : r + 64, 0:128] = sr
        l_ref[r : r + 64, 128:256] = -si
        l_ref[512 + r : 576 + r, 0:128] = si
        l_ref[512 + r : 576 + r, 128:256] = sr


def place_weights(core, w_ref, col, blocks):
    for which in range(2):
        lane0 = pl.multiple_of((core if which == 0 else 1 - core) * 128, 128)
        for i in range(6):
            row, at = i // 2 * 128, col + i % 2 * 128
            w_ref[which, row : row + 128, at : at + 128] = blocks[i][:, pl.ds(lane0, 128)]


def pack_near_kernel(ids_ref, w0_ref, w1_ref, p0_ref, p1_ref):
    place_weights(ids_ref[0], p0_ref, 0, [w0_ref.at[i] for i in range(6)])
    place_weights(ids_ref[0], p1_ref, 0, [w1_ref.at[i] for i in range(6)])


def pack_side_kernel(ids_ref, w3_ref, p3_ref):
    place_weights(ids_ref[0], p3_ref, 0, [w3_ref.at[i] for i in range(6)])


def early_kernel(ids_ref, own_ref, sib_ref, p0_ref, l_ref, near_ref):
    place_rows(l_ref.at[0], own_ref)
    place_rows(l_ref.at[1], sib_ref)
    near_ref[...] = product(l_ref[0], p0_ref[0]) + product(l_ref[1], p0_ref[1])


def cross_sums(which, l_ref, p1_ref, p3_ref):
    both = product(l_ref[...], jnp.concatenate([p1_ref[which], p3_ref[which]], 0))
    return both[:, 0:384], both[:, 384:768]


def own_kernel(ids_ref, cross_ref, p1_ref, p3_ref, begun_ref, near_ref, far_ref, l_ref):
    place_rows(l_ref, cross_ref)
    near, far_ref[...] = cross_sums(0, l_ref, p1_ref, p3_ref)
    near_ref[...] = begun_ref[...] + near


def sib_kernel(ids_ref, cross_ref, p1_ref, p3_ref, near_ref, begun_ref, group_ref, out_ref, far_ref, l_ref):
    place_rows(l_ref, cross_ref)
    near, far = cross_sums(1, l_ref, p1_ref, p3_ref)
    store_beams(ids_ref[1], near_ref[...] + near, group_ref, out_ref)
    far_ref[...] = begun_ref[...] + far


def far_kernel(ids_ref, l_ref, acc_ref, group_ref, w2a_ref, w2b_ref, begun_ref, out_ref, w_ref):
    place_weights(ids_ref[0], w_ref, 0, [w2a_ref.at[i] for i in range(2)] + [w2b_ref.at[i] for i in range(4)])
    acc = acc_ref[...] + product(l_ref[0], w_ref[0]) + product(l_ref[1], w_ref[1])
    store_beams(1 - ids_ref[1], acc, group_ref, out_ref)


PARTS = jax.ShapeDtypeStruct((8, 2, 4, 32, 128), BF16)
SUMS = jax.ShapeDtypeStruct((1024, 384), F32)


PACKED = jax.ShapeDtypeStruct((2, 384, 256), BF16)


def pack_near(*args):
    return call(pack_near_kernel, 2, [PACKED, PACKED], [])(*args)


def pack_side(*args):
    return call(pack_side_kernel, 1, PACKED, [])(*args)


LHS = pltpu.VMEM((1024, 256), BF16)


def form_early(*args):
    return call(early_kernel, 3, [jax.ShapeDtypeStruct((2, 1024, 256), BF16), SUMS], [])(*args)


def form_own(*args):
    return call(own_kernel, 4, [SUMS, SUMS], [LHS])(*args)


def form_sib(*args):
    return call(sib_kernel, 6, [PARTS, SUMS], [LHS])(*args)


def form_far(*args):
    return call(far_kernel, 6, PARTS, [pltpu.VMEM((2, 384, 256), BF16)], {6: 0})(*args)


def add_kernel(got_ref, out_ref):
    for side in range(2):
        sources = [(z * 2 + side) * 4 + y for z in range(8) for y in range(4)]
        parts = [got_ref[src].astype(F32) for src in sources[:4]]
        for place, src in enumerate(sources[4:]):
            parts[place % 4] = parts[place % 4] + got_ref[src].astype(F32)
        total = (parts[0] + parts[1]) + (parts[2] + parts[3])
        for p in range(2):
            out_ref[side * 16 : side * 16 + 16, p, :] = total[p * 16 : p * 16 + 16]


def add(got):
    return pl.pallas_call(
        add_kernel,
        in_specs=[VM],
        out_specs=VM,
        out_shape=jax.ShapeDtypeStruct((32, 2, 128), F32),
        compiler_params=pltpu.CompilerParams(vmem_limit_bytes=LIMIT),
        name="add",
    )(got)


def shards(signals, weights, bin_group):
    half, core, low = lax.axis_index("xhi"), lax.axis_index("core"), lax.axis_index("xlo")
    ring = ("xlo", "xhi", "core")

    def exchange(value, flip):
        return lax.ppermute(value, ring, [(i, i ^ flip) for i in range(8)])

    ids = jnp.stack([core, half, low])
    blocks = weights.reshape(6, 128, 256)
    w1 = exchange(blocks, 4)
    w3 = exchange(blocks, 6)
    other = exchange(signals, 1)
    own, perm, table, coarse, fine, outer = prep(ids, pltpu.with_memory_space_constraint(signals, pltpu.HBM))

    spec0, xs, rest = dft_first(ids, other, own, perm, table, coarse, fine, outer)
    got0 = exchange(spec0, 2)
    spec1, spec2 = dft_next(ids, xs, rest, outer)
    got1 = exchange(spec1, 4)
    got2 = exchange(spec2, 6)
    mine, group = dft_last(ids, xs, rest, outer, bin_group.reshape(16, 128))
    same = (mine + got0.astype(F32)).astype(BF16)
    same_sib = exchange(same, 1)
    p0, p1 = pack_near(ids, blocks, w1)
    w2a = exchange(w1[:2], 6)
    w2b = exchange(w3[2:], 4)
    p3 = pack_side(ids, w3)
    lhs, near = form_early(ids, same, same_sib, p0)
    cross = (got1.astype(F32) + got2.astype(F32)).astype(BF16)
    cross_sib = exchange(cross, 1)
    near, far = form_own(ids, cross, p1, p3, near)
    begun, far = form_sib(ids, cross_sib, p1, p3, near, far, group)
    parts = form_far(ids, lhs, far, group, w2a, w2b, begun)
    got = lax.all_to_all(parts.reshape(64, 32, 128), ("z", "xhi", "y"), 0, 0, tiled=True)
    return add(got)


def solution(mesh):
    fine = Mesh(mesh.devices.reshape(4, 2, 8, 2, 2), ("y", "xlo", "z", "xhi", "core"))
    chan, beam = ("y", "xlo", "z"), ("xhi", "core")
    in_specs = (P(chan, beam), P(None, None, beam, chan), P())
    out_specs = P(chan, None, beam)
    return jax.shard_map(shards, mesh=fine, in_specs=in_specs, out_specs=out_specs, check_vma=False)
```

```python
import math

import jax
import jax.numpy as jnp
from jax import lax
from jax.experimental import pallas as pl
from jax.experimental.pallas import tpu as pltpu
from jax.sharding import Mesh, PartitionSpec as P

F32 = jnp.float32
BF16 = jnp.bfloat16
I32 = jnp.int32

STRIDE = 8
SAMPLES = 8192
LIMIT = 16 * 1024 * 1024
UNROLL = 16


def root(numer, denom):
    angle = 2.0 * math.pi / denom * (numer & (denom - 1)).astype(F32)
    return jnp.cos(angle), -jnp.sin(angle)


def iota(shape, dim):
    return lax.broadcasted_iota(I32, shape, dim)


def deinterleave(x, perm):
    out = []
    rows = jnp.concatenate([x[:, :1024], x[:, 1024:]], 0)
    split = jnp.dot(rows, perm, preferred_element_type=F32).astype(BF16)
    for s in range(STRIDE):
        cols = split[:, s * 128 : (s + 1) * 128]
        out.append(jnp.concatenate([cols[:128], cols[128:]], 1))
    return out


def eighth(q):
    q = q & 7
    half = math.sqrt(0.5)
    odd = (q & 1) != 0
    re = jnp.where(odd, half, jnp.where((q & 2) != 0, 0.0, 1.0))
    re = jnp.where((q > 2) & (q < 6), -re, re)
    im = jnp.where(odd, half, jnp.where((q & 2) != 0, 1.0, 0.0))
    im = jnp.where(q < 4, -im, im)
    return re, im


def owner(ids_ref, slot):
    half, low = ids_ref[1], ids_ref[2]
    return (1 - half if slot in (0, 2) else half), (1 - low if slot in (1, 2) else low)


def block_of(t, low):
    return t // 8 * 16 + low * 8 + t % 8


def make_twiddles(ids_ref, slot, coarse_ref, fine_ref, t_ref, row0):
    half, low = owner(ids_ref, slot)
    first = pl.multiple_of(half * 16, 16)
    fr = fine_ref[0, pl.ds(first, 16), :]
    fi = fine_ref[1, pl.ds(first, 16), :]
    for t in range(16):
        k = block_of(t, low)
        cr = jnp.concatenate([coarse_ref[0, pl.ds(k, 1), :]] * 4, 1)
        ci = jnp.concatenate([coarse_ref[1, pl.ds(k, 1), :]] * 4, 1)
        row = row0 + t * 16
        t_ref[row : row + 16, :] = (cr * fr - ci * fi).astype(BF16)
        t_ref[row + 256 : row + 272, :] = (cr * fi + ci * fr).astype(BF16)


def prep_kernel(ids_ref, own_ref, xs_ref, perm_ref, t_ref, coarse_ref, fine_ref, outer_ref):
    core, half = ids_ref[0], ids_ref[1]
    row, lane = iota((32, 128), 0), iota((32, 128), 1)
    coarse_ref[0], coarse_ref[1] = root(row * lane, 32)
    br, bi = root((row + 1) * lane, 1024)
    for part in range(4):
        u = 2 * core + part if part < 2 else 2 * (1 - core) + part - 2
        er, ei = eighth((row + 1) * u)
        cols = slice(part * 128, part * 128 + 128)
        fine_ref[0, :, cols] = br * er - bi * ei
        fine_ref[1, :, cols] = br * ei + bi * er
    outer_ref[0], outer_ref[1] = root(row * 32, SAMPLES)
    outer_ref[2], outer_ref[3] = root(row + 1, SAMPLES)
    scale = 1.0 / math.sqrt(SAMPLES)
    outer_ref[4] = jnp.where((((row + 1) * half) & 1) != 0, -scale, scale)
    make_twiddles(ids_ref, 0, coarse_ref, fine_ref, t_ref, 0)
    same = jnp.where(iota((1024, 128), 0) // STRIDE == iota((1024, 128), 1), 1.0, 0.0).astype(BF16)
    phase = iota((16, 128), 0) & (STRIDE - 1)
    for s in range(STRIDE):
        keep = jnp.where(phase == s, 1.0, 0.0).astype(BF16)
        perm_ref[:, s * 128 : (s + 1) * 128] = (same.reshape(64, 16, 128) * keep[None]).reshape(1024, 128)
    for s, rows in enumerate(deinterleave(own_ref[...], perm_ref[...])):
        xs_ref[s * 128 : (s + 1) * 128, :] = rows


def prep(ids, signals):
    full = lambda *shape: pl.BlockSpec(shape, lambda i, ids: (0,) * len(shape))
    return pl.pallas_call(
        prep_kernel,
        grid_spec=pltpu.PrefetchScalarGridSpec(
            num_scalar_prefetch=1,
            grid=(1,),
            in_specs=[pl.BlockSpec((128, 2048), lambda i, ids: (ids[0], 0))],
            out_specs=[
                full(1024, 256),
                full(1024, 1024),
                full(512, 512),
                full(2, 32, 128),
                full(2, 32, 512),
                full(5, 32, 128),
            ],
        ),
        out_shape=[
            jax.ShapeDtypeStruct((1024, 256), BF16),
            jax.ShapeDtypeStruct((1024, 1024), BF16),
            jax.ShapeDtypeStruct((512, 512), BF16),
            jax.ShapeDtypeStruct((2, 32, 128), F32),
            jax.ShapeDtypeStruct((2, 32, 512), F32),
            jax.ShapeDtypeStruct((5, 32, 128), F32),
        ],
        compiler_params=pltpu.CompilerParams(vmem_limit_bytes=LIMIT),
        name="prep",
    )(ids, signals)


def times(w, x):
    return w[0] * x[0] - w[1] * x[1], w[0] * x[1] + w[1] * x[0]


def plus(x, y):
    return x[0] + y[0], x[1] + y[1]


def minus(x, y):
    return x[0] - y[0], x[1] - y[1]


def turned(x, y):
    return x[0] + y[1], x[1] - y[0]


def combine(ids_ref, slot, f_ref, outer_ref, out_ref):
    half, low = owner(ids_ref, slot)
    first = pl.multiple_of(half * 16, 16)
    fine = outer_ref[2, pl.ds(first, 16), :], outer_ref[3, pl.ds(first, 16), :]
    scale = outer_ref[4, pl.ds(first, 16), :]
    eighth_root = math.sqrt(0.5)

    def step(t, carry):
        row0 = pl.multiple_of(t * 16, 16)
        k = block_of(t, low)
        w = times((outer_ref[0, pl.ds(k, 1), :], outer_ref[1, pl.ds(k, 1), :]), fine)
        w2 = times(w, w)
        w4 = times(w2, w2)
        wt = eighth_root * (w[0] + w[1]), eighth_root * (w[1] - w[0])
        term = lambda s: (
            f_ref[pl.ds(row0, 16), s * 128 : (s + 1) * 128],
            f_ref[pl.ds(row0 + 256, 16), s * 128 : (s + 1) * 128],
        )
        sums = []
        for s in range(2):
            near, far = term(s), times(w4, term(s + 4))
            up, down = plus(near, far), minus(near, far)
            near, far = term(s + 2), times(w4, term(s + 6))
            sums.append(
                (plus(up, times(w2, plus(near, far))), turned(down, times(w2, minus(near, far))))
            )
        low_bin = plus(sums[0][0], times(w, sums[1][0]))
        high_bin = plus(sums[0][1], times(wt, sums[1][1]))
        for place, value in enumerate((low_bin[0], high_bin[0], low_bin[1], high_bin[1])):
            rows = pl.ds(row0 + 256 * place, 16)
            out_ref[rows, :] = (value * scale).astype(out_ref.dtype)
        return carry

    lax.fori_loop(0, 16, step, 0, unroll=UNROLL)


def spectrum(t_ref, row0, xs_ref, f_ref):
    f_ref[...] = lax.dot_general(
        t_ref[row0 : row0 + 512, :], xs_ref[...], (((1,), (1,)), ((), ())), preferred_element_type=F32
    )


def first_kernel(
    ids_ref, other_ref, own_ref, perm_ref, t_ref, coarse_ref, fine_ref, outer_ref, out_ref, xs_ref, rest_ref, f_ref
):
    xs_ref[:, 0:256] = own_ref[...]
    other = other_ref[pl.ds(pl.multiple_of(ids_ref[0] * 128, 128), 128), :]
    for s, rows in enumerate(deinterleave(other, perm_ref[...])):
        xs_ref[s * 128 : (s + 1) * 128, 256:512] = rows
    for slot in (1, 2, 3):
        make_twiddles(ids_ref, slot, coarse_ref, fine_ref, rest_ref, (slot - 1) * 512)
    spectrum(t_ref, 0, xs_ref, f_ref)
    combine(ids_ref, 0, f_ref, outer_ref, out_ref)


def next_kernel(ids_ref, xs_ref, rest_ref, outer_ref, out1_ref, out2_ref, f_ref):
    for index, out_ref in enumerate((out1_ref, out2_ref)):
        spectrum(rest_ref, index * 512, xs_ref, f_ref.at[index])
        combine(ids_ref, 1 + index, f_ref.at[index], outer_ref, out_ref)


def last_kernel(ids_ref, xs_ref, rest_ref, outer_ref, bins_ref, out_ref, group_ref, f_ref):
    spectrum(rest_ref, 1024, xs_ref, f_ref)
    half, low = ids_ref[1], ids_ref[2]
    row, lane = iota((512, 128), 0), iota((512, 128), 1)
    line = jnp.where(lane == (row // 128 * 4 + low * 2 + row // 64 % 2), 1.0, 0.0).astype(BF16)[:, :16]
    lines = jnp.dot(line, bins_ref[...].astype(F32).astype(BF16), preferred_element_type=F32)
    place = row // 16 % 4 * 32 + half * 16 + row % 16
    chosen = jnp.where(lane == place, lines, 0.0).astype(BF16)
    group_ref[...] = jnp.dot(chosen, jnp.ones((128, 128), BF16), preferred_element_type=F32)
    combine(ids_ref, 3, f_ref, outer_ref, out_ref)


VM = pl.BlockSpec(memory_space=pltpu.VMEM)


SM = pl.BlockSpec(memory_space=pltpu.SMEM)
PIECE = jax.ShapeDtypeStruct((1024, 128), BF16)


def call(kernel, count, out_shape, scratch, alias={}):
    outs = len(out_shape) if isinstance(out_shape, list) else 0
    return pl.pallas_call(
        kernel,
        in_specs=[SM] + [VM] * count,
        out_specs=[VM] * outs if outs else VM,
        out_shape=out_shape,
        scratch_shapes=scratch,
        input_output_aliases=alias,
        compiler_params=pltpu.CompilerParams(vmem_limit_bytes=LIMIT),
    )


def dft_first(*args):
    outs = [PIECE, jax.ShapeDtypeStruct((1024, 512), BF16), jax.ShapeDtypeStruct((1536, 512), BF16)]
    return call(first_kernel, 7, outs, [pltpu.VMEM((512, 1024), F32)])(*args)


def dft_next(*args):
    return call(next_kernel, 3, [PIECE, PIECE], [pltpu.VMEM((2, 512, 1024), F32)])(*args)


def dft_last(*args):
    outs = [jax.ShapeDtypeStruct((1024, 128), F32), jax.ShapeDtypeStruct((512, 128), F32)]
    return call(last_kernel, 4, outs, [pltpu.VMEM((512, 1024), F32)])(*args)


def product(lhs, weights):
    return lax.dot_general(lhs, weights, (((1,), (1,)), ((), ())), preferred_element_type=F32)


def store_beams(side, acc, group_ref, out_ref):
    acc = acc.reshape(2, 512, 384)
    group = group_ref[...][None]
    total = jnp.where(group == 0, acc[:, :, 0:128], jnp.where(group == 1, acc[:, :, 128:256], acc[:, :, 256:384]))
    re = total[0].reshape(4, 8, 16, 128)
    im = total[1].reshape(4, 8, 16, 128)
    both = jnp.concatenate([re, im], 2).astype(BF16)
    for y in range(4):
        out_ref[:, pl.ds(side, 1), y] = both[y][:, None]


def place_rows(l_ref, src):
    for r in range(0, 512, 64):
        sr, si = src[r : r + 64, :], src[512 + r : 576 + r, :]
        l_ref[r : r + 64, 0:128] = sr
        l_ref[r : r + 64, 128:256] = -si
        l_ref[512 + r : 576 + r, 0:128] = si
        l_ref[512 + r : 576 + r, 128:256] = sr


def place_weights(core, w_ref, col, blocks):
    for which in range(2):
        lane0 = pl.multiple_of((core if which == 0 else 1 - core) * 128, 128)
        for i in range(6):
            row, at = i // 2 * 128, col + i % 2 * 128
            w_ref[which, row : row + 128, at : at + 128] = blocks[i][:, pl.ds(lane0, 128)]


def pack_near_kernel(ids_ref, w0_ref, w1_ref, p0_ref, p1_ref):
    place_weights(ids_ref[0], p0_ref, 0, [w0_ref.at[i] for i in range(6)])
    place_weights(ids_ref[0], p1_ref, 0, [w1_ref.at[i] for i in range(6)])


def pack_side_kernel(ids_ref, w3_ref, p3_ref):
    place_weights(ids_ref[0], p3_ref, 0, [w3_ref.at[i] for i in range(6)])


def early_kernel(ids_ref, own_ref, sib_ref, p0_ref, l_ref, near_ref):
    place_rows(l_ref.at[0], own_ref)
    place_rows(l_ref.at[1], sib_ref)
    near_ref[...] = product(l_ref[0], p0_ref[0]) + product(l_ref[1], p0_ref[1])


def cross_sums(which, l_ref, p1_ref, p3_ref):
    both = product(l_ref[...], jnp.concatenate([p1_ref[which], p3_ref[which]], 0))
    return both[:, 0:384], both[:, 384:768]


def own_kernel(ids_ref, cross_ref, p1_ref, p3_ref, begun_ref, near_ref, far_ref, l_ref):
    place_rows(l_ref, cross_ref)
    near, far_ref[...] = cross_sums(0, l_ref, p1_ref, p3_ref)
    near_ref[...] = begun_ref[...] + near


def sib_kernel(ids_ref, cross_ref, p1_ref, p3_ref, near_ref, begun_ref, group_ref, out_ref, far_ref, l_ref):
    place_rows(l_ref, cross_ref)
    near, far = cross_sums(1, l_ref, p1_ref, p3_ref)
    store_beams(ids_ref[1], near_ref[...] + near, group_ref, out_ref)
    far_ref[...] = begun_ref[...] + far


def far_kernel(ids_ref, l_ref, acc_ref, group_ref, w2a_ref, w2b_ref, begun_ref, out_ref, w_ref):
    place_weights(ids_ref[0], w_ref, 0, [w2a_ref.at[i] for i in range(1)] + [w2b_ref.at[i] for i in range(5)])
    acc = acc_ref[...] + product(l_ref[0], w_ref[0]) + product(l_ref[1], w_ref[1])
    store_beams(1 - ids_ref[1], acc, group_ref, out_ref)


PARTS = jax.ShapeDtypeStruct((8, 2, 4, 32, 128), BF16)
SUMS = jax.ShapeDtypeStruct((1024, 384), F32)


PACKED = jax.ShapeDtypeStruct((2, 384, 256), BF16)


def pack_near(*args):
    return call(pack_near_kernel, 2, [PACKED, PACKED], [])(*args)


def pack_side(*args):
    return call(pack_side_kernel, 1, PACKED, [])(*args)


LHS = pltpu.VMEM((1024, 256), BF16)


def form_early(*args):
    return call(early_kernel, 3, [jax.ShapeDtypeStruct((2, 1024, 256), BF16), SUMS], [])(*args)


def form_own(*args):
    return call(own_kernel, 4, [SUMS, SUMS], [LHS])(*args)


def form_sib(*args):
    return call(sib_kernel, 6, [PARTS, SUMS], [LHS])(*args)


def form_far(*args):
    return call(far_kernel, 6, PARTS, [pltpu.VMEM((2, 384, 256), BF16)], {6: 0})(*args)


def add_kernel(got_ref, out_ref):
    for side in range(2):
        sources = [(z * 2 + side) * 4 + y for z in range(8) for y in range(4)]
        parts = [got_ref[src].astype(F32) for src in sources[:4]]
        for place, src in enumerate(sources[4:]):
            parts[place % 4] = parts[place % 4] + got_ref[src].astype(F32)
        total = (parts[0] + parts[1]) + (parts[2] + parts[3])
        for p in range(2):
            out_ref[side * 16 : side * 16 + 16, p, :] = total[p * 16 : p * 16 + 16]


def add(got):
    return pl.pallas_call(
        add_kernel,
        in_specs=[VM],
        out_specs=VM,
        out_shape=jax.ShapeDtypeStruct((32, 2, 128), F32),
        compiler_params=pltpu.CompilerParams(vmem_limit_bytes=LIMIT),
        name="add",
    )(got)


def shards(signals, weights, bin_group):
    half, core, low = lax.axis_index("xhi"), lax.axis_index("core"), lax.axis_index("xlo")
    ring = ("xlo", "xhi", "core")

    def exchange(value, flip):
        return lax.ppermute(value, ring, [(i, i ^ flip) for i in range(8)])

    ids = jnp.stack([core, half, low])
    blocks = weights.reshape(6, 128, 256)
    w1 = exchange(blocks, 4)
    w3 = exchange(blocks, 6)
    other = exchange(signals, 1)
    own, perm, table, coarse, fine, outer = prep(ids, pltpu.with_memory_space_constraint(signals, pltpu.HBM))

    spec0, xs, rest = dft_first(ids, other, own, perm, table, coarse, fine, outer)
    got0 = exchange(spec0, 2)
    spec1, spec2 = dft_next(ids, xs, rest, outer)
    got1 = exchange(spec1, 4)
    got2 = exchange(spec2, 6)
    mine, group = dft_last(ids, xs, rest, outer, bin_group.reshape(16, 128))
    same = (mine + got0.astype(F32)).astype(BF16)
    same_sib = exchange(same, 1)
    p0, p1 = pack_near(ids, blocks, w1)
    w2a = exchange(w1[:1], 6)
    w2b = exchange(w3[1:], 4)
    p3 = pack_side(ids, w3)
    lhs, near = form_early(ids, same, same_sib, p0)
    cross = (got1.astype(F32) + got2.astype(F32)).astype(BF16)
    cross_sib = exchange(cross, 1)
    near, far = form_own(ids, cross, p1, p3, near)
    begun, far = form_sib(ids, cross_sib, p1, p3, near, far, group)
    parts = form_far(ids, lhs, far, group, w2a, w2b, begun)
    got = lax.all_to_all(parts.reshape(64, 32, 128), ("z", "xhi", "y"), 0, 0, tiled=True)
    return add(got)


def solution(mesh):
    fine = Mesh(mesh.devices.reshape(4, 2, 8, 2, 2), ("y", "xlo", "z", "xhi", "core"))
    chan, beam = ("y", "xlo", "z"), ("xhi", "core")
    in_specs = (P(chan, beam), P(None, None, beam, chan), P())
    out_specs = P(chan, None, beam)
    return jax.shard_map(shards, mesh=fine, in_specs=in_specs, out_specs=out_specs, check_vma=False)
```
